32 devices in a mesh: branch: 4 (over z), row: 4 (over y, x), col: 2 (over core).
Axes of the slice: x: 2, y: 2, z: 4, core: 2. Of those that a mesh axis runs over, the one named last changes fastest.
Arguments:
- section_in: bfloat16 [4, 4, 2, 48, 4096], P('branch', 'row', 'col'), may hold values from -6 to 6
- conv_weight: bfloat16 [4, 2, 3, 3, 384, 384], P('branch'), may hold values from -1 to 1, as said below
- conv_bias: float32 [4, 2, 384], P('branch'), may hold values from -3 to 3
- join_weight: bfloat16 [720, 720], replicated, may hold values from -0.4375 to 0.4375
- join_bias: float32 [720], replicated, may hold values from -3 to 3
Outputs:
- joined_first: bfloat16 [48, 128, 256], P(None, ('branch', 'row'), 'col')
- joined_second: bfloat16 [96, 64, 128], P(None, ('branch', 'row'), 'col')
- joined_third: bfloat16 [192, 32, 64], P(None, ('branch', 'row'), 'col')
- joined_fourth: bfloat16 [384, 16, 32], P(None, ('branch', 'row'), 'col')
The draws below stay inside these ranges and needn't reach their ends.
Inputs may be any that keep to these rules, and one draw needn't show every extreme that they name: `conv_weight`: entries of branch b's kernels have standard deviation (9 * 2^b * 48) ** -0.5; entries outside the C_b x C_b corner are drawn too and unused.
All inputs are finite; a program needn't handle non-finite values.
Results may differ from the reference program's by a relative error of at most 0.0075.
Values may be sent and summed in bfloat16 or wider, within the bound.
A program may use at most 128 MiB of HBM per device.

```python
import jax
import jax.numpy as jnp
from jax import lax

WIDTH = 48
TH = 32
TW = 128
N_BRANCH = 4
N_ROW = 4
N_COL = 2


def draw_conv_weight(key, part):
    array_dims = (4, 2, 3, 3, 8 * WIDTH, 8 * WIDTH)
    fan_scale = (9.0 * WIDTH * 2.0 ** jnp.arange(4, dtype=jnp.float32)) ** (-0.5)
    values = jax.random.normal(key, array_dims, jnp.float32)
    values = jnp.clip(values, -6.0, 6.0)
    return (values * fan_scale[:, None, None, None, None, None]).astype(jnp.bfloat16)


def block_scale(rng, shape, pieces, low, largest):
    gain = 1.0
    for position, parts in pieces:
        draws = jax.random.uniform(jax.random.fold_in(jax.random.fold_in(rng, 6), position), (parts,), jnp.float32, low / len(pieces), largest / len(pieces))
        gain = gain * jnp.repeat(jnp.exp(draws), shape[position] // parts).reshape((-1,) + (1,) * (len(shape) - 1 - position))
    return gain


def bell_draw(stream_key, dims, width, limit, split=(), held_as=jnp.bfloat16):
    values = width * jax.random.normal(stream_key, dims, jnp.float32)
    if split:
        values = values * block_scale(stream_key, dims, split, -0.22, 0.18)
    return jnp.clip(values, -limit, limit).astype(held_as)


def setup_inputs(seed: int = 0) -> dict:
    key_list = jax.random.split(jax.random.key(seed), 6)
    section_in = bell_draw(key_list[0], (N_BRANCH, N_ROW, N_COL, WIDTH, TH * TW), 1.0, 6.0, ((0, 4), (1, 4), (2, 2)))
    conv_weight = draw_conv_weight(jax.random.fold_in(key_list[5], 71), 0)
    conv_bias = bell_draw(key_list[2], (N_BRANCH, 2, 8 * WIDTH), 0.5, 3.0, ((0, 4),), jnp.float32)
    join_weight = bell_draw(key_list[3], (15 * WIDTH, 15 * WIDTH), (4 * WIDTH) ** -0.5, 0.4375)
    join_bias = bell_draw(key_list[4], (15 * WIDTH,), 0.5, 3.0, (), jnp.float32)
    return {"section_in": section_in, "conv_weight": conv_weight, "conv_bias": conv_bias, "join_weight": join_weight, "join_bias": join_bias}


def branch_map(section_in, branch_level):
    channels = WIDTH * 2 ** branch_level
    tile_rows = TH // 2 ** branch_level
    tile_cols = TW // 2 ** branch_level
    packed = section_in[branch_level][:, :, :, : (TH * TW) // 2 ** branch_level]
    packed = packed.reshape(N_ROW, N_COL, channels, tile_rows, tile_cols)
    return packed.transpose(2, 0, 3, 1, 4).reshape(channels, N_ROW * tile_rows, N_COL * tile_cols)


def conv_same(field, kernel):
    result = lax.conv_general_dilated(
        field[None].astype(jnp.float32),
        kernel.astype(jnp.float32).transpose(2, 3, 0, 1),
        (1, 1),
        "SAME",
        dimension_numbers=("NCHW", "OIHW", "NCHW"),
        precision=lax.Precision.HIGHEST,
    )
    return result[0]


def pooled(tile_data, factor):
    channels, height, breadth = tile_data.shape
    blocks = tile_data.astype(jnp.float32).reshape(channels, height // factor, factor, breadth // factor, factor)
    return jnp.mean(blocks, axis=(2, 4)).astype(jnp.bfloat16)


def upsample(tile_data, factor):
    channels, height, breadth = tile_data.shape
    spread = jnp.broadcast_to(tile_data[:, :, None, :, None], (channels, height, factor, breadth, factor))
    return spread.reshape(channels, height * factor, breadth * factor)


def mix_block(join_weight, target, source, tile_data):
    target_start = (2 ** target - 1) * WIDTH
    source_start = (2 ** source - 1) * WIDTH
    target_width = WIDTH * 2 ** target
    source_width = WIDTH * 2 ** source
    block = join_weight[target_start:target_start + target_width, source_start:source_start + source_width]
    channels, height, breadth = tile_data.shape
    product = jnp.dot(block, tile_data.reshape(channels, height * breadth), preferred_element_type=jnp.float32)
    return product.astype(jnp.bfloat16).reshape(target_width, height, breadth)


def reference(section_in, conv_weight, conv_bias, join_weight, join_bias):
    settled = []
    for branch_level in range(4):
        channels = WIDTH * 2 ** branch_level
        inputs = branch_map(section_in, branch_level)
        kernel_first = conv_weight[branch_level, 0, :, :, :channels, :channels]
        kernel_second = conv_weight[branch_level, 1, :, :, :channels, :channels]
        hidden = jax.nn.relu(conv_same(inputs, kernel_first) + conv_bias[branch_level, 0, :channels, None, None])
        hidden = hidden.astype(jnp.bfloat16)
        after = conv_same(hidden, kernel_second) + conv_bias[branch_level, 1, :channels, None, None]
        settled.append(jax.nn.relu(after + inputs.astype(jnp.float32)).astype(jnp.bfloat16))
    outputs = []
    for target in range(4):
        target_start = (2 ** target - 1) * WIDTH
        target_width = WIDTH * 2 ** target
        total_sum = settled[target].astype(jnp.float32) + join_bias[target_start:target_start + target_width, None, None]
        for source in range(4):
            if source < target:
                term = mix_block(join_weight, target, source, pooled(settled[source], 2 ** (target - source)))
                total_sum = total_sum + term.astype(jnp.float32)
            elif source > target:
                term = mix_block(join_weight, target, source, settled[source])
                total_sum = total_sum + upsample(term, 2 ** (source - target)).astype(jnp.float32)
        outputs.append(jax.nn.relu(total_sum).astype(jnp.bfloat16))
    return (outputs[0], outputs[1], outputs[2], outputs[3])
```

```python
from functools import partial

import jax
import jax.numpy as jnp
from jax import lax
from jax.experimental import pallas as pl
from jax.experimental.pallas import tpu as pltpu
from jax.sharding import PartitionSpec as P

WIDTH = 48
TH = 32
TW = 128
LANES = 128
STRIPS = 4
MESH = pl.DeviceIdType.MESH
WAYS = [(dr, dc) for dr in (-1, 0, 1) for dc in (-1, 0, 1) if dr or dc]
F32 = jnp.float32
BF16 = jnp.bfloat16

OWN_TILES = (32, 8, 2, 1)
BEFORE = (2, 1, 1, 0)
FIELD_TILES = (36, 10, 4, 1)
HIDDEN_TILES = (34, 10, 4, 1)


def lane_index(width=LANES):
    return lax.broadcasted_iota(jnp.int32, (1, width), 1)


def turned(group, shift):
    shift = shift % LANES
    return pltpu.roll(group, shift, 1) if shift else group


def tiles_turned(field, shift):
    if shift % LANES == 0:
        return field
    tiles = [turned(field[:, t : t + LANES], shift) for t in range(0, field.shape[1], LANES)]
    return tiles[0] if len(tiles) == 1 else jnp.concatenate(tiles, axis=1)


def natural_tile(branch_level, container_ref):
    pixels = TH * TW >> 2 * branch_level
    channels = WIDTH << branch_level
    parts = []
    for part in range(1 << branch_level):
        at = part * pixels
        low = at // LANES * LANES
        piece = container_ref[:, low : low + max(pixels, LANES)]
        if at > low:
            piece = pltpu.roll(piece.astype(F32), LANES - at + low, 1).astype(BF16)
        parts.append(piece)
    held = lax.broadcasted_iota(jnp.int32, (1, channels), 1)
    part = sum((held >= WIDTH * turn).astype(jnp.int32) for turn in range(1, 1 << branch_level))
    home = ((held - WIDTH * part) << branch_level) + part
    order = jnp.where(lax.broadcasted_iota(jnp.int32, (channels, channels), 0) == home, 1.0, 0.0)
    return jnp.dot(
        order.astype(BF16), jnp.concatenate(parts, axis=0), preferred_element_type=F32
    ).astype(BF16)


def column_stack(branch_level, own, west, east):
    cols = TW >> branch_level
    col = lane_index(own.shape[1]) & (cols - 1)
    own32 = own.astype(F32)
    minus = tiles_turned(
        jnp.where(col == cols - 1, tiles_turned(west.astype(F32), -cols), own32), 1
    ).astype(BF16)
    plus = tiles_turned(
        jnp.where(col == 0, tiles_turned(east.astype(F32), cols), own32), -1
    ).astype(BF16)

    def zeros(rows):
        return jnp.zeros((rows, own.shape[1]), BF16)

    if branch_level == 0:
        pieces = [minus, own, zeros(32), plus, zeros(80)]
    elif branch_level == 3:
        pieces = [minus, own, plus]
    else:
        pad = zeros(-own.shape[0] % LANES)
        pieces = [minus, pad, own, pad, plus, pad]
    return jnp.concatenate(pieces, axis=0)


def taps(branch_level, weights, layer):
    channels = WIDTH << branch_level
    width = -(-channels // LANES) * LANES
    lines = []
    for dy in range(3):
        if branch_level == 0:
            first, middle, last = (weights[layer, dy, dx, 0:channels, 0:width] for dx in range(3))
            pair = jnp.where(
                lane_index() < channels,
                first.astype(F32),
                pltpu.roll(middle.astype(F32), channels, 1),
            )
            lines.append(jnp.concatenate([pair.astype(BF16), last], axis=1))
        else:
            lines.append(
                jnp.concatenate(
                    [weights[layer, dy, dx, 0:channels, 0:width] for dx in range(3)], axis=1
                )
            )
    return jnp.concatenate(lines, axis=0)


def row_sum(branch_level, products, first, count):
    channels = products.shape[0] // 3
    cols = TW >> branch_level
    above, here, below = (products[d * channels : (d + 1) * channels] for d in range(3))
    span = slice(first * LANES, (first + count) * LANES)
    if cols == LANES:
        return (
            above[:, (first - 1) * LANES : (first - 1 + count) * LANES]
            + here[:, span]
            + below[:, (first + 1) * LANES : (first + 1 + count) * LANES]
        )
    last = products.shape[1] // LANES - 1
    above, below = tiles_turned(above, cols), tiles_turned(below, -cols)
    lane = lane_index()

    def tile(field, t):
        t = min(max(t, 0), last)
        return field[:, t * LANES : (t + 1) * LANES]

    tiles = [
        jnp.where(lane < cols, tile(above, t - 1), tile(above, t))
        + tile(here, t)
        + jnp.where(lane >= LANES - cols, tile(below, t + 1), tile(below, t))
        for t in range(first, first + count)
    ]
    return tiles[0] if count == 1 else jnp.concatenate(tiles, axis=1)


def front_kernel(
    section, kernels, biases, held0, held1, held2, held3,
    container, weights, bias, own0, own1, own2, own3, side0, side1, side2, side3,
    pack_send, pack_recv, hide0, hide1, hide2, hide3, hid0, hid1, hid2, hid3,
    settled0, settled1, settled2, settled3, load_sem,
    halo_send, halo_recv, hidden_send, hidden_recv, strip_send, strip_recv, own_sem,
):
    level = lax.axis_index("branch")
    place = lax.axis_index("row")
    col = lax.axis_index("col")
    row_count = lax.axis_size("row")
    col_count = lax.axis_size("col")

    def reach(dr, dc):
        there = jnp.bool_(True)
        if dr:
            there = (place + dr >= 0) & (place + dr < row_count)
        if dc:
            sideways = (col + dc >= 0) & (col + dc < col_count)
            there = there & sideways if dr else sideways
        device = (
            level,
            lax.rem(place + dr + row_count, row_count),
            lax.rem(col + dc + col_count, col_count),
        )
        return there, device

    barrier = pltpu.get_barrier_semaphore()
    expected = 0
    for dr, dc in WAYS:
        there, device = reach(dr, dc)
        expected = expected + there.astype(jnp.int32)

        @pl.when(there)
        def _():
            pl.semaphore_signal(barrier, inc=1, device_id=device, device_id_type=MESH)

    at_home = level == place
    for source in range(STRIPS):

        @pl.when(jnp.logical_not(at_home & (level == source)))
        def _():
            pl.semaphore_signal(
                barrier, inc=1, device_id=(source, level, col), device_id_type=MESH
            )

    expected = expected + STRIPS - at_home.astype(jnp.int32)

    helds = (held0, held1, held2, held3)
    owns = (own0, own1, own2, own3)
    sides = (side0, side1, side2, side3)
    hides = (hide0, hide1, hide2, hide3)
    hids = (hid0, hid1, hid2, hid3)
    settleds = (settled0, settled1, settled2, settled3)

    def run(b):
        channels = WIDTH << b
        width = -(-channels // LANES) * LANES
        cols, rows = TW >> b, TH >> b
        own, side, hide, hid = owns[b], sides[b], hides[b], hids[b]
        settled, held = settleds[b], helds[b]
        before, tiles = BEFORE[b], OWN_TILES[b]
        middle = slice(before * LANES, (before + tiles) * LANES)

        if b == 0:
            load = pltpu.make_async_copy(section, own.at[:, middle], load_sem.at[0])
        else:
            load = pltpu.make_async_copy(
                section.at[:, 0 : TH * TW >> b], container.at[:, 0 : TH * TW >> b], load_sem.at[0]
            )
        load.start()
        bias_load = pltpu.make_async_copy(biases, bias, load_sem.at[1])
        bias_load.start()
        weight_loads = [
            pltpu.make_async_copy(
                kernels.at[layer, :, :, 0:channels, 0:width],
                weights.at[layer, :, :, 0:channels, 0:width],
                load_sem.at[2 + layer],
            )
            for layer in range(2)
        ]
        for copy in weight_loads:
            copy.start()
        load.wait()
        if b:
            own[:, middle] = natural_tile(b, container)
        packed = b == 3
        lane = lane_index()
        if packed:
            whole = own[...].astype(F32)
            for end in range(2):
                out = None
                for g in range(4):
                    part = turned(whole[g * 96 : (g + 1) * 96], 32 * g - 32 * end)
                    out = part if g == 0 else jnp.where(lane < 32 * g, out, part)
                pack_send[end] = out.astype(BF16)

        def halo_region(dr, dc):
            if packed and dr:
                return pack_recv.at[WAYS.index((dr, dc))]
            target = own if dc == 0 else side.at[0 if dc == 1 else 1]
            if dr == 0:
                return target.at[:, middle]
            if dr == 1:
                return target.at[:, 0 : before * LANES]
            return target.at[:, (before + tiles) * LANES : (before + tiles + before) * LANES]

        def halo_source(dr):
            if dr == 0:
                return own.at[:, middle]
            if packed:
                return pack_send.at[0 if dr == -1 else 1]
            first = before if dr == -1 else tiles
            return own.at[:, first * LANES : (first + before) * LANES]

        def halo_copy(dr, dc):
            way = WAYS.index((dr, dc))
            return pltpu.make_async_remote_copy(
                src_ref=halo_source(dr),
                dst_ref=halo_region(dr, dc),
                send_sem=halo_send.at[way],
                recv_sem=halo_recv.at[way],
                device_id=reach(dr, dc)[1],
                device_id_type=MESH,
            )

        order = [way for way in WAYS if way[0]] + [way for way in WAYS if not way[0]]
        pl.semaphore_wait(barrier, expected)
        for dr, dc in order:
            pl.when(reach(dr, dc)[0])(halo_copy(dr, dc).start)
        for dr, dc in order:

            @pl.when(jnp.logical_not(reach(-dr, -dc)[0]))
            def _():
                region = halo_region(dr, dc)
                region[...] = jnp.zeros(region.shape, BF16)

        bias_load.wait()
        offsets = [
            jnp.broadcast_to(bias[layer : layer + 1, :], (8, bias.shape[1])).T[:channels, 0:1]
            for layer in range(2)
        ]
        weight_loads[0].wait()
        for dr, dc in order:
            pl.when(reach(-dr, -dc)[0])(halo_copy(dr, dc).wait_recv)

        fields = [own[...], side[0], side[1]]
        if packed:
            for at, dc in enumerate((0, 1, -1)):
                upper = pack_recv[WAYS.index((1, dc))].astype(F32)
                lower = pack_recv[WAYS.index((-1, dc))].astype(F32)
                lines = []
                for g in range(4):
                    here = fields[at][g * 96 : (g + 1) * 96].astype(F32)
                    ring = jnp.where(
                        lane < 96, turned(lower, 64 - 32 * g), turned(upper, 96 - 32 * g)
                    )
                    lines.append(jnp.where(lane < 64, here, ring).astype(BF16))
                fields[at] = jnp.concatenate(lines, axis=0)

        products = jnp.dot(
            taps(b, weights, 0),
            column_stack(b, *fields),
            preferred_element_type=F32,
        )
        first = 1 if b == 0 else 0
        hidden = row_sum(b, products, first, HIDDEN_TILES[b])
        hidden = jnp.maximum(hidden + offsets[0], 0.0)
        row = lax.shift_right_logical(lane_index(HIDDEN_TILES[b] * LANES), cols.bit_length() - 1)
        if b == 3:
            row = jnp.where(row >= 6, row - 8, row)
        else:
            row = row - (before - first) * (LANES // cols)
        low = jnp.where(place == 0, 0, -LANES)
        high = jnp.where(place == row_count - 1, rows, 2 * LANES)
        hidden = jnp.where((row >= low) & (row < high), hidden, 0.0)
        hid[...] = hidden.astype(BF16)

        def hidden_copy(dc):
            at = 0 if dc == 1 else 1
            return pltpu.make_async_remote_copy(
                src_ref=hid,
                dst_ref=hide.at[at],
                send_sem=hidden_send.at[at],
                recv_sem=hidden_recv.at[at],
                device_id=reach(0, dc)[1],
                device_id_type=MESH,
            )

        for dc in (1, -1):
            pl.when(reach(0, dc)[0])(hidden_copy(dc).start)
        for dc in (1, -1):

            @pl.when(jnp.logical_not(reach(0, -dc)[0]))
            def _():
                at = 0 if dc == 1 else 1
                hide[at] = jnp.zeros(hid.shape, BF16)

        weight_loads[1].wait()
        for dc in (1, -1):
            pl.when(reach(0, -dc)[0])(hidden_copy(dc).wait_recv)
        products = jnp.dot(
            taps(b, weights, 1),
            column_stack(b, hid[...], hide[0], hide[1]),
            preferred_element_type=F32,
        )
        after = row_sum(b, products, 1 if b == 0 else before, tiles)
        final = jnp.maximum(after + offsets[1] + own[:, middle].astype(F32), 0.0)
        if b < 3:
            settled[...] = final.astype(BF16)
        else:
            for strip in range(STRIPS):
                out = None
                for g in range(8):
                    part = turned(final[g * WIDTH : (g + 1) * WIDTH], 16 * g - 16 * strip)
                    out = part if g == 0 else jnp.where(lane < 16 * g, out, part)
                settled[strip] = out.astype(BF16)

        def strip_source(strip):
            if b == 3:
                return settled.at[strip]
            if b == 2:
                return settled.at[:, pl.ds(pl.multiple_of(strip // 2 * LANES, LANES), LANES)]
            size = tiles * LANES // STRIPS
            return settled.at[:, pl.ds(pl.multiple_of(strip * size, LANES), size)]

        def strip_copies(turn):
            strip = lax.rem(place + turn, STRIPS)
            source = strip_source(strip)
            remote = pltpu.make_async_remote_copy(
                src_ref=source,
                dst_ref=held,
                send_sem=strip_send.at[turn],
                recv_sem=strip_recv.at[b],
                device_id=(place, strip, col),
                device_id_type=MESH,
            )
            return remote, pltpu.make_async_copy(source, held, own_sem)

        for turn in range(STRIPS):
            remote, local_copy = strip_copies(turn)
            if turn == 0:
                pl.when(jnp.logical_not(at_home))(remote.start)
                pl.when(at_home)(local_copy.start)
            else:
                remote.start()

        for dr, dc in order:
            pl.when(reach(dr, dc)[0])(halo_copy(dr, dc).wait_send)
        for dc in (1, -1):
            pl.when(reach(0, dc)[0])(hidden_copy(dc).wait_send)
        for turn in range(STRIPS):
            remote, local_copy = strip_copies(turn)
            if turn == 0:
                pl.when(jnp.logical_not(at_home))(remote.wait_send)
                pl.when(at_home)(local_copy.wait)
            else:
                remote.wait_send()

    for b in range(STRIPS):
        pl.when(level == b)(partial(run, b))

    for source in range(STRIPS):
        arrival = pltpu.make_async_remote_copy(
            src_ref=helds[source],
            dst_ref=helds[source],
            send_sem=strip_send.at[0],
            recv_sem=strip_recv.at[source],
            device_id=(source, level, col),
            device_id_type=MESH,
        )
        pl.when(jnp.logical_not(at_home & (level == source)))(arrival.wait_recv)


HELD_SHAPES = ((48, 1024), (96, 256), (192, 128), (48, 128))


def front(section, kernels, biases):
    anywhere = pl.BlockSpec(memory_space=pl.ANY)
    vmem = pl.BlockSpec(memory_space=pltpu.VMEM)

    def field(b, tiles):
        return (WIDTH << b, tiles[b] * LANES)

    scratch = [
        pltpu.VMEM((WIDTH, TH * TW // 2), BF16),
        pltpu.VMEM(kernels.shape, BF16),
        pltpu.VMEM(biases.shape, F32),
    ]
    scratch += [pltpu.VMEM(field(b, FIELD_TILES), BF16) for b in range(4)]
    scratch += [pltpu.VMEM((2, *field(b, FIELD_TILES)), BF16) for b in range(4)]
    scratch += [pltpu.VMEM((2, 96, LANES), BF16), pltpu.VMEM((8, 96, LANES), BF16)]
    scratch += [pltpu.VMEM((2, *field(b, HIDDEN_TILES)), BF16) for b in range(4)]
    scratch += [pltpu.VMEM(field(b, HIDDEN_TILES), BF16) for b in range(4)]
    scratch += [pltpu.VMEM(field(b, OWN_TILES), BF16) for b in range(3)]
    scratch += [pltpu.VMEM((STRIPS, WIDTH, LANES), BF16)]
    dma = pltpu.SemaphoreType.DMA
    scratch += [dma((4,)), dma((8,)), dma((8,)), dma((2,)), dma((2,)), dma((4,)), dma((4,)), dma]
    return pl.pallas_call(
        front_kernel,
        out_shape=[jax.ShapeDtypeStruct(shape, BF16) for shape in HELD_SHAPES],
        in_specs=[anywhere] * 3,
        out_specs=[vmem] * 4,
        scratch_shapes=scratch,
        compiler_params=pltpu.CompilerParams(
            collective_id=0, has_side_effects=True, vmem_limit_bytes=56 << 20
        ),
        name="front",
    )(section, kernels, biases)


def block_mask(fine_level, coarse_level):
    fine_cols = TW >> fine_level
    coarse_cols = TW >> coarse_level
    fine = TH * TW // STRIPS >> 2 * fine_level
    coarse = TH * TW // STRIPS >> 2 * coarse_level
    shift = coarse_level - fine_level
    pixel = lax.broadcasted_iota(jnp.int32, (fine, 1), 0)
    row = lax.shift_right_logical(pixel, fine_cols.bit_length() - 1 + shift)
    col = lax.shift_right_logical(pixel & (fine_cols - 1), shift)
    home = row * coarse_cols + col
    target = lax.broadcasted_iota(jnp.int32, (fine, coarse), 1)
    return jnp.where(home == target, 1.0, 0.0).astype(BF16)


def mixed(weight_ref, target, source, tile_data):
    start = ((1 << source) - 1) * WIDTH
    low = start // LANES * LANES
    high = min(-(-(start + tile_data.shape[0]) // LANES) * LANES, weight_ref.shape[1])
    pieces = []
    if start > low:
        pieces.append(jnp.zeros((start - low, tile_data.shape[1]), tile_data.dtype))
    pieces.append(tile_data)
    if high > start + tile_data.shape[0]:
        pieces.append(
            jnp.zeros((high - start - tile_data.shape[0], tile_data.shape[1]), tile_data.dtype)
        )
    rows = ((1 << target) - 1) * WIDTH
    return jnp.dot(
        weight_ref[rows : rows + (WIDTH << target), low:high],
        jnp.concatenate(pieces, axis=0),
        preferred_element_type=F32,
    ).astype(BF16)


def join_strip(maps, masks, weight_ref, offset, out_refs):
    for target in range(4):
        start = ((1 << target) - 1) * WIDTH
        total = maps[target].astype(F32) + offset[start : start + (WIDTH << target), :]
        for source in range(4):
            if source < target:
                share = 0.25 ** (target - source)
                shrunk = jnp.dot(maps[source], masks[source, target], preferred_element_type=F32)
                term = mixed(weight_ref, target, source, (shrunk * share).astype(BF16))
                total = total + term.astype(F32)
            elif source > target:
                term = mixed(weight_ref, target, source, maps[source])
                total = total + lax.dot_general(
                    term,
                    masks[target, source],
                    (((1,), (1,)), ((), ())),
                    preferred_element_type=F32,
                )
        total = jnp.maximum(total, 0.0)
        out_ref = out_refs[target]
        if len(out_ref.shape) == 2:
            out_ref[...] = total.T.astype(BF16)
        else:
            lines = [total[:, at : at + LANES] for at in range(0, total.shape[1], LANES)]
            out_ref[...] = jnp.stack(lines, axis=1).astype(BF16)


def join_kernel(held0, held1, held2, held3, weight_ref, bias_ref, *out_refs):
    masks = {
        (fine, coarse): block_mask(fine, coarse)
        for fine in range(3)
        for coarse in range(fine + 1, 4)
    }
    total = bias_ref.shape[1]
    line = jnp.concatenate([bias_ref[...], jnp.zeros((1, -total % LANES), F32)], axis=1)
    offset = jnp.broadcast_to(line, (8, line.shape[1])).T[:total, 0:1]
    third = held2[...].astype(F32)
    odd = lax.rem(lax.axis_index("row"), 2) == 1
    third = jnp.where(odd, turned(third, 64), third).astype(BF16)[:, :64]
    last = held3[...].astype(F32)
    last = jnp.concatenate([turned(last, -16 * g) for g in range(8)], axis=0)
    maps = [held0[...], held1[...], third, last.astype(BF16)[:, :16]]
    join_strip(maps, masks, weight_ref, offset, out_refs)


def joined(helds, join_weight, join_bias):
    vmem = pl.BlockSpec(memory_space=pltpu.VMEM)
    shapes = [(WIDTH << b, (TH >> b) // STRIPS, TW >> b) for b in range(4)]
    outs = pl.pallas_call(
        join_kernel,
        out_shape=[
            jax.ShapeDtypeStruct(
                shape if shape[2] == LANES else (shape[1] * shape[2], shape[0]), BF16
            )
            for shape in shapes
        ],
        in_specs=[vmem] * 6,
        out_specs=[vmem] * 4,
        name="join",
    )(*helds, join_weight, join_bias[None, :])
    return tuple(
        out if out.ndim == 3 else out.reshape(*shape[1:], shape[0]).transpose(2, 0, 1)
        for out, shape in zip(outs, shapes)
    )


def local(section_in, conv_weight, conv_bias, join_weight, join_bias):
    helds = front(section_in[0, 0, 0], conv_weight[0], conv_bias[0])
    return joined(helds, join_weight, join_bias)


def solution(mesh):
    in_specs = (
        P("branch", "row", "col", None, None),
        P("branch", None, None, None, None, None),
        P("branch", None, None),
        P(),
        P(),
    )
    out_specs = (P(None, ("branch", "row"), "col"),) * 4
    return jax.shard_map(local, mesh=mesh, in_specs=in_specs, out_specs=out_specs, check_vma=False)
```

```python
from functools import partial

import jax
import jax.numpy as jnp
from jax import lax
from jax.experimental import pallas as pl
from jax.experimental.pallas import tpu as pltpu
from jax.sharding import PartitionSpec as P

WIDTH = 48
TH = 32
TW = 128
LANES = 128
STRIPS = 4
MESH = pl.DeviceIdType.MESH
WAYS = [(dr, dc) for dr in (-1, 0, 1) for dc in (-1, 0, 1) if dr or dc]
F32 = jnp.float32
BF16 = jnp.bfloat16

OWN_TILES = (32, 8, 2, 1)
BEFORE = (2, 1, 1, 0)
FIELD_TILES = (36, 10, 4, 1)
HIDDEN_TILES = (34, 10, 4, 1)


CHUNKS = (4, 2, 2, 1)
RELAYS = 12


def route(source, tile, strip, chunk):
    if tile == source or strip == tile:
        return None
    if source == 0 and strip == 3 - tile and chunk % 2 == 0:
        return None
    return strip


def relayed(source, place):
    pieces = [
        (tile, strip, chunk)
        for chunk in range(CHUNKS[source])
        for tile in range(STRIPS)
        for strip in range(STRIPS)
        if tile != place and route(source, tile, strip, chunk) == place
    ]
    return sorted(pieces, key=lambda p: (p[2], (p[0] ^ place).bit_count(), -abs(p[0] - source)))


def own_pieces(source, place):
    chunks = range(CHUNKS[source])
    if source == place:
        return [(place ^ turn, chunk) for turn in (0, 1, 2, 3) for chunk in chunks]
    return [(place ^ turn, chunk) for chunk in chunks for turn in (1, 2, 0, 3)]


def lane_index(width=LANES):
    return lax.broadcasted_iota(jnp.int32, (1, width), 1)


def turned(group, shift):
    shift = shift % LANES
    return pltpu.roll(group, shift, 1) if shift else group


def tiles_turned(field, shift):
    if shift % LANES == 0:
        return field
    tiles = [turned(field[:, t : t + LANES], shift) for t in range(0, field.shape[1], LANES)]
    return tiles[0] if len(tiles) == 1 else jnp.concatenate(tiles, axis=1)


def natural_tile(branch_level, container_ref):
    pixels = TH * TW >> 2 * branch_level
    channels = WIDTH << branch_level
    parts = []
    for part in range(1 << branch_level):
        at = part * pixels
        low = at // LANES * LANES
        piece = container_ref[:, low : low + max(pixels, LANES)]
        if at > low:
            piece = pltpu.roll(piece.astype(F32), LANES - at + low, 1).astype(BF16)
        parts.append(piece)
    held = lax.broadcasted_iota(jnp.int32, (1, channels), 1)
    part = sum((held >= WIDTH * turn).astype(jnp.int32) for turn in range(1, 1 << branch_level))
    home = ((held - WIDTH * part) << branch_level) + part
    order = jnp.where(lax.broadcasted_iota(jnp.int32, (channels, channels), 0) == home, 1.0, 0.0)
    return jnp.dot(
        order.astype(BF16), jnp.concatenate(parts, axis=0), preferred_element_type=F32
    ).astype(BF16)


def column_stack(branch_level, own, west, east):
    cols = TW >> branch_level
    col = lane_index(own.shape[1]) & (cols - 1)
    own32 = own.astype(F32)
    minus = tiles_turned(
        jnp.where(col == cols - 1, tiles_turned(west.astype(F32), -cols), own32), 1
    ).astype(BF16)
    plus = tiles_turned(
        jnp.where(col == 0, tiles_turned(east.astype(F32), cols), own32), -1
    ).astype(BF16)

    def zeros(rows):
        return jnp.zeros((rows, own.shape[1]), BF16)

    if branch_level == 0:
        pieces = [minus, own, zeros(32), plus, zeros(80)]
    elif branch_level == 3:
        pieces = [minus, own, plus]
    else:
        pad = zeros(-own.shape[0] % LANES)
        pieces = [minus, pad, own, pad, plus, pad]
    return jnp.concatenate(pieces, axis=0)


def taps(branch_level, weights, layer):
    channels = WIDTH << branch_level
    width = -(-channels // LANES) * LANES
    lines = []
    for dy in range(3):
        if branch_level == 0:
            first, middle, last = (weights[layer, dy, dx, 0:channels, 0:width] for dx in range(3))
            pair = jnp.where(
                lane_index() < channels,
                first.astype(F32),
                pltpu.roll(middle.astype(F32), channels, 1),
            )
            lines.append(jnp.concatenate([pair.astype(BF16), last], axis=1))
        else:
            lines.append(
                jnp.concatenate(
                    [weights[layer, dy, dx, 0:channels, 0:width] for dx in range(3)], axis=1
                )
            )
    return jnp.concatenate(lines, axis=0)


def row_sum(branch_level, products, first, count):
    channels = products.shape[0] // 3
    cols = TW >> branch_level
    above, here, below = (products[d * channels : (d + 1) * channels] for d in range(3))
    span = slice(first * LANES, (first + count) * LANES)
    if cols == LANES:
        return (
            above[:, (first - 1) * LANES : (first - 1 + count) * LANES]
            + here[:, span]
            + below[:, (first + 1) * LANES : (first + 1 + count) * LANES]
        )
    last = products.shape[1] // LANES - 1
    above, below = tiles_turned(above, cols), tiles_turned(below, -cols)
    lane = lane_index()

    def tile(field, t):
        t = min(max(t, 0), last)
        return field[:, t * LANES : (t + 1) * LANES]

    tiles = [
        jnp.where(lane < cols, tile(above, t - 1), tile(above, t))
        + tile(here, t)
        + jnp.where(lane >= LANES - cols, tile(below, t + 1), tile(below, t))
        for t in range(first, first + count)
    ]
    return tiles[0] if count == 1 else jnp.concatenate(tiles, axis=1)


def front_kernel(
    section, kernels, biases, held0, held1, held2, held3,
    container, weights, bias, own0, own1, own2, own3, side0, side1, side2, side3,
    pack_send, pack_recv, hide0, hide1, hide2, hide3, hid0, hid1, hid2, hid3,
    settled0, settled1, settled2, settled3, relay0, relay1, relay2, relay3, load_sem,
    halo_send, halo_recv, hidden_send, hidden_recv, strip_send, strip_recv, relay_recv, own_sem,
):
    level = lax.axis_index("branch")
    place = lax.axis_index("row")
    col = lax.axis_index("col")
    row_count = lax.axis_size("row")
    col_count = lax.axis_size("col")

    def reach(dr, dc):
        there = jnp.bool_(True)
        if dr:
            there = (place + dr >= 0) & (place + dr < row_count)
        if dc:
            sideways = (col + dc >= 0) & (col + dc < col_count)
            there = there & sideways if dr else sideways
        device = (
            level,
            lax.rem(place + dr + row_count, row_count),
            lax.rem(col + dc + col_count, col_count),
        )
        return there, device

    barrier = pltpu.get_barrier_semaphore()
    expected = 0
    for dr, dc in WAYS:
        there, device = reach(dr, dc)
        expected = expected + there.astype(jnp.int32)

        @pl.when(there)
        def _():
            pl.semaphore_signal(barrier, inc=1, device_id=device, device_id_type=MESH)

    at_home = level == place
    for step in range(1, STRIPS):
        for device in (
            (level, lax.rem(place + step, STRIPS), col),
            (lax.rem(level + step, STRIPS), place, col),
        ):
            pl.semaphore_signal(barrier, inc=1, device_id=device, device_id_type=MESH)

    @pl.when((level > 0) & (place == STRIPS - 1 - level))
    def _():
        pl.semaphore_signal(barrier, inc=1, device_id=(0, level, col), device_id_type=MESH)

    expected = expected + 2 * (STRIPS - 1) + ((level == 0) & (place > 0)).astype(jnp.int32)

    helds = (held0, held1, held2, held3)
    owns = (own0, own1, own2, own3)
    sides = (side0, side1, side2, side3)
    hides = (hide0, hide1, hide2, hide3)
    hids = (hid0, hid1, hid2, hid3)
    settleds = (settled0, settled1, settled2, settled3)
    relays = (relay0, relay1, relay2, relay3)

    def run(b):
        channels = WIDTH << b
        width = -(-channels // LANES) * LANES
        cols, rows = TW >> b, TH >> b
        own, side, hide, hid = owns[b], sides[b], hides[b], hids[b]
        settled, held, relay = settleds[b], helds[b], relays[b]
        before, tiles = BEFORE[b], OWN_TILES[b]
        middle = slice(before * LANES, (before + tiles) * LANES)

        if b == 0:
            load = pltpu.make_async_copy(section, own.at[:, middle], load_sem.at[0])
        else:
            load = pltpu.make_async_copy(
                section.at[:, 0 : TH * TW >> b], container.at[:, 0 : TH * TW >> b], load_sem.at[0]
            )
        load.start()
        bias_load = pltpu.make_async_copy(biases, bias, load_sem.at[1])
        bias_load.start()
        weight_loads = [
            pltpu.make_async_copy(
                kernels.at[layer, :, :, 0:channels, 0:width],
                weights.at[layer, :, :, 0:channels, 0:width],
                load_sem.at[2 + layer],
            )
            for layer in range(2)
        ]
        for copy in weight_loads:
            copy.start()
        load.wait()
        if b:
            own[:, middle] = natural_tile(b, container)
        packed = b >= 2
        lane = lane_index()
        folds = (WIDTH << b) // 96
        pair = 2 * cols
        if packed:
            for end in range(2):
                tile = before if end == 0 else before + tiles - 1
                at = 0 if end == 0 else (rows - 2) * cols % LANES
                edge = own[:, tile * LANES : (tile + 1) * LANES].astype(F32)
                out = None
                for g in range(folds):
                    part = turned(edge[g * 96 : (g + 1) * 96], pair * g - at)
                    out = part if g == 0 else jnp.where(lane < pair * g, out, part)
                pack_send[end] = out.astype(BF16)

        def halo_region(dr, dc):
            if packed and dr:
                return pack_recv.at[WAYS.index((dr, dc))]
            target = own if dc == 0 else side.at[0 if dc == 1 else 1]
            if dr == 0:
                return target.at[:, middle]
            if dr == 1:
                return target.at[:, 0 : before * LANES]
            return target.at[:, (before + tiles) * LANES : (before + tiles + before) * LANES]

        def halo_source(dr):
            if dr == 0:
                return own.at[:, middle]
            if packed:
                return pack_send.at[0 if dr == -1 else 1]
            first = before if dr == -1 else tiles
            return own.at[:, first * LANES : (first + before) * LANES]

        def halo_copy(dr, dc):
            way = WAYS.index((dr, dc))
            return pltpu.make_async_remote_copy(
                src_ref=halo_source(dr),
                dst_ref=halo_region(dr, dc),
                send_sem=halo_send.at[way],
                recv_sem=halo_recv.at[way],
                device_id=reach(dr, dc)[1],
                device_id_type=MESH,
            )

        order = [way for way in WAYS if way[0]] + [way for way in WAYS if not way[0]]
        pl.semaphore_wait(barrier, expected)
        for dr, dc in order:
            pl.when(reach(dr, dc)[0])(halo_copy(dr, dc).start)
        for dr, dc in order:

            @pl.when(jnp.logical_not(reach(-dr, -dc)[0]))
            def _():
                region = halo_region(dr, dc)
                region[...] = jnp.zeros(region.shape, BF16)

        bias_load.wait()
        offsets = [
            jnp.broadcast_to(bias[layer : layer + 1, :], (8, bias.shape[1])).T[:channels, 0:1]
            for layer in range(2)
        ]
        weight_loads[0].wait()
        for dr, dc in order:
            pl.when(reach(-dr, -dc)[0])(halo_copy(dr, dc).wait_recv)

        fields = [own, side.at[0], side.at[1]]
        if packed:
            for at, dc in enumerate((0, 1, -1)):
                upper = pack_recv[WAYS.index((1, dc))].astype(F32)
                lower = pack_recv[WAYS.index((-1, dc))].astype(F32)
                lines = []
                for g in range(folds):
                    span = slice(g * 96, (g + 1) * 96)
                    here = fields[at][span, middle]
                    above = turned(upper, LANES - pair - pair * g)
                    if b == 3:
                        ring = jnp.where(lane < 96, turned(lower, 64 - pair * g), above)
                        lines.append(jnp.where(lane < 64, here.astype(F32), ring).astype(BF16))
                    else:
                        below = turned(lower, -pair * g)
                        lines.append(
                            jnp.concatenate([above.astype(BF16), here, below.astype(BF16)], axis=1)
                        )
                fields[at] = jnp.concatenate(lines, axis=0)
        else:
            fields = [field[...] for field in fields]

        products = jnp.dot(
            taps(b, weights, 0),
            column_stack(b, *fields),
            preferred_element_type=F32,
        )
        first = 1 if b == 0 else 0
        hidden = row_sum(b, products, first, HIDDEN_TILES[b])
        hidden = jnp.maximum(hidden + offsets[0], 0.0)
        row = lax.shift_right_logical(lane_index(HIDDEN_TILES[b] * LANES), cols.bit_length() - 1)
        if b == 3:
            row = jnp.where(row >= 6, row - 8, row)
        else:
            row = row - (before - first) * (LANES // cols)
        low = jnp.where(place == 0, 0, -LANES)
        high = jnp.where(place == row_count - 1, rows, 2 * LANES)
        hidden = jnp.where((row >= low) & (row < high), hidden, 0.0)
        hid[...] = hidden.astype(BF16)

        def hidden_copy(dc):
            at = 0 if dc == 1 else 1
            return pltpu.make_async_remote_copy(
                src_ref=hid,
                dst_ref=hide.at[at],
                send_sem=hidden_send.at[at],
                recv_sem=hidden_recv.at[at],
                device_id=reach(0, dc)[1],
                device_id_type=MESH,
            )

        for dc in (1, -1):
            pl.when(reach(0, dc)[0])(hidden_copy(dc).start)
        for dc in (1, -1):

            @pl.when(jnp.logical_not(reach(0, -dc)[0]))
            def _():
                at = 0 if dc == 1 else 1
                hide[at] = jnp.zeros(hid.shape, BF16)

        weight_loads[1].wait()
        for dc in (1, -1):
            pl.when(reach(0, -dc)[0])(hidden_copy(dc).wait_recv)
        products = jnp.dot(
            taps(b, weights, 1),
            column_stack(b, hid[...], hide[0], hide[1]),
            preferred_element_type=F32,
        )
        after = row_sum(b, products, 1 if b == 0 else before, tiles)
        final = jnp.maximum(after + offsets[1] + own[:, middle].astype(F32), 0.0)
        if b < 3:
            settled[...] = final.astype(BF16)
        else:
            for strip in range(STRIPS):
                out = None
                for g in range(8):
                    part = turned(final[g * WIDTH : (g + 1) * WIDTH], 16 * g - 16 * strip)
                    out = part if g == 0 else jnp.where(lane < 16 * g, out, part)
                settled[strip] = out.astype(BF16)

        chunks = CHUNKS[b]

        def ends(strip, chunk):
            if b == 3:
                return settled.at[strip], held
            if b == 2:
                size = channels // chunks
                span = slice(chunk * size, (chunk + 1) * size)
                tile = strip // 2
                return settled.at[span, tile * LANES : (tile + 1) * LANES], held.at[span]
            size = tiles * LANES // STRIPS // chunks
            at = (strip * chunks + chunk) * size
            return settled.at[:, at : at + size], held.at[:, chunk * size : (chunk + 1) * size]

        def send(source, target, semaphore, arrived, device):
            copy = pltpu.make_async_remote_copy(
                src_ref=source,
                dst_ref=target,
                send_sem=strip_send.at[semaphore],
                recv_sem=arrived,
                device_id=device,
                device_id_type=MESH,
            )
            copy.start()
            return copy.wait_send

        def exchange(here):
            waits = []
            for strip, chunk in own_pieces(b, here):
                source, target = ends(strip, chunk)
                if here == b and strip == here:
                    copy = pltpu.make_async_copy(source, target, own_sem.at[chunk])
                    copy.start()
                    waits.append(copy.wait)
                    continue
                via = route(b, here, strip, chunk)
                if via is None:
                    arrived, device = strip_recv.at[b], (here, strip, col)
                else:
                    slot = relayed(b, via).index((here, strip, chunk))
                    target = relay.at[slot]
                    arrived, device = relay_recv.at[slot], (b, via, col)
                waits.append(send(source, target, len(waits), arrived, device))
            for slot, (tile, strip, chunk) in enumerate(relayed(b, here)):
                piece = relay.at[slot]
                pltpu.make_async_remote_copy(
                    src_ref=piece,
                    dst_ref=piece,
                    send_sem=strip_send.at[0],
                    recv_sem=relay_recv.at[slot],
                    device_id=(b, tile, col),
                    device_id_type=MESH,
                ).wait_recv()
                target = ends(strip, chunk)[1]
                waits.append(
                    send(piece, target, len(waits), strip_recv.at[b], (tile, strip, col))
                )
            for wait in waits:
                wait()

        for here in range(STRIPS):
            pl.when(place == here)(partial(exchange, here))

        for dr, dc in order:
            pl.when(reach(dr, dc)[0])(halo_copy(dr, dc).wait_send)
        for dc in (1, -1):
            pl.when(reach(0, dc)[0])(hidden_copy(dc).wait_send)

    for b in range(STRIPS):
        pl.when(level == b)(partial(run, b))

    for source in range(STRIPS):
        arrival = pltpu.make_async_remote_copy(
            src_ref=helds[source],
            dst_ref=helds[source],
            send_sem=strip_send.at[0],
            recv_sem=strip_recv.at[source],
            device_id=(source, level, col),
            device_id_type=MESH,
        )
        pl.when(jnp.logical_not(at_home & (level == source)))(arrival.wait_recv)


HELD_SHAPES = ((48, 1024), (96, 256), (192, 128), (48, 128))


def front(section, kernels, biases):
    anywhere = pl.BlockSpec(memory_space=pl.ANY)
    vmem = pl.BlockSpec(memory_space=pltpu.VMEM)

    def field(b, tiles):
        return (WIDTH << b, tiles[b] * LANES)

    scratch = [
        pltpu.VMEM((WIDTH, TH * TW // 2), BF16),
        pltpu.VMEM(kernels.shape, BF16),
        pltpu.VMEM(biases.shape, F32),
    ]
    scratch += [pltpu.VMEM(field(b, FIELD_TILES), BF16) for b in range(4)]
    scratch += [pltpu.VMEM((2, *field(b, FIELD_TILES)), BF16) for b in range(4)]
    scratch += [pltpu.VMEM((2, 96, LANES), BF16), pltpu.VMEM((8, 96, LANES), BF16)]
    scratch += [pltpu.VMEM((2, *field(b, HIDDEN_TILES)), BF16) for b in range(4)]
    scratch += [pltpu.VMEM(field(b, HIDDEN_TILES), BF16) for b in range(4)]
    scratch += [pltpu.VMEM(field(b, OWN_TILES), BF16) for b in range(3)]
    scratch += [pltpu.VMEM((STRIPS, WIDTH, LANES), BF16)]
    pieces = ((48, 256), (96, 128), (96, 128), (48, 128))
    scratch += [pltpu.VMEM((RELAYS, *piece), BF16) for piece in pieces]
    counts = (4, 8, 8, 2, 2, 16 + RELAYS, 4, RELAYS, 4)
    scratch += [pltpu.SemaphoreType.DMA((count,)) for count in counts]
    return pl.pallas_call(
        front_kernel,
        out_shape=[jax.ShapeDtypeStruct(shape, BF16) for shape in HELD_SHAPES],
        in_specs=[anywhere] * 3,
        out_specs=[vmem] * 4,
        scratch_shapes=scratch,
        compiler_params=pltpu.CompilerParams(
            collective_id=0, has_side_effects=True, vmem_limit_bytes=56 << 20
        ),
        name="front",
    )(section, kernels, biases)


def block_mask(fine_level, coarse_level):
    fine_cols = TW >> fine_level
    coarse_cols = TW >> coarse_level
    fine = TH * TW // STRIPS >> 2 * fine_level
    coarse = TH * TW // STRIPS >> 2 * coarse_level
    shift = coarse_level - fine_level
    pixel = lax.broadcasted_iota(jnp.int32, (fine, 1), 0)
    row = lax.shift_right_logical(pixel, fine_cols.bit_length() - 1 + shift)
    col = lax.shift_right_logical(pixel & (fine_cols - 1), shift)
    home = row * coarse_cols + col
    target = lax.broadcasted_iota(jnp.int32, (fine, coarse), 1)
    return jnp.where(home == target, 1.0, 0.0).astype(BF16)


def mixed(weight_ref, target, source, tile_data):
    start = ((1 << source) - 1) * WIDTH
    low = start // LANES * LANES
    high = min(-(-(start + tile_data.shape[0]) // LANES) * LANES, weight_ref.shape[1])
    pieces = []
    if start > low:
        pieces.append(jnp.zeros((start - low, tile_data.shape[1]), tile_data.dtype))
    pieces.append(tile_data)
    if high > start + tile_data.shape[0]:
        pieces.append(
            jnp.zeros((high - start - tile_data.shape[0], tile_data.shape[1]), tile_data.dtype)
        )
    rows = ((1 << target) - 1) * WIDTH
    return jnp.dot(
        weight_ref[rows : rows + (WIDTH << target), low:high],
        jnp.concatenate(pieces, axis=0),
        preferred_element_type=F32,
    ).astype(BF16)


def join_strip(maps, masks, weight_ref, offset, out_refs):
    for target in range(4):
        start = ((1 << target) - 1) * WIDTH
        total = maps[target].astype(F32) + offset[start : start + (WIDTH << target), :]
        for source in range(4):
            if source < target:
                share = 0.25 ** (target - source)
                shrunk = jnp.dot(maps[source], masks[source, target], preferred_element_type=F32)
                term = mixed(weight_ref, target, source, (shrunk * share).astype(BF16))
                total = total + term.astype(F32)
            elif source > target:
                term = mixed(weight_ref, target, source, maps[source])
                total = total + lax.dot_general(
                    term,
                    masks[target, source],
                    (((1,), (1,)), ((), ())),
                    preferred_element_type=F32,
                )
        total = jnp.maximum(total, 0.0)
        out_ref = out_refs[target]
        if len(out_ref.shape) == 2:
            out_ref[...] = total.T.astype(BF16)
        else:
            lines = [total[:, at : at + LANES] for at in range(0, total.shape[1], LANES)]
            out_ref[...] = jnp.stack(lines, axis=1).astype(BF16)


def join_kernel(held0, held1, held2, held3, weight_ref, bias_ref, *out_refs):
    masks = {
        (fine, coarse): block_mask(fine, coarse)
        for fine in range(3)
        for coarse in range(fine + 1, 4)
    }
    total = bias_ref.shape[0]
    line = jnp.concatenate([bias_ref[...][None, :], jnp.zeros((1, -total % LANES), F32)], axis=1)
    offset = jnp.broadcast_to(line, (8, line.shape[1])).T[:total, 0:1]
    third = held2[...].astype(F32)
    odd = lax.rem(lax.axis_index("row"), 2) == 1
    third = jnp.where(odd, turned(third, 64), third).astype(BF16)[:, :64]
    last = held3[...].astype(F32)
    last = jnp.concatenate([turned(last, -16 * g) for g in range(8)], axis=0)
    maps = [held0[...], held1[...], third, last.astype(BF16)[:, :16]]
    join_strip(maps, masks, weight_ref, offset, out_refs)


def joined(helds, join_weight, join_bias):
    vmem = pl.BlockSpec(memory_space=pltpu.VMEM)
    shapes = [(WIDTH << b, (TH >> b) // STRIPS, TW >> b) for b in range(4)]
    outs = pl.pallas_call(
        join_kernel,
        out_shape=[
            jax.ShapeDtypeStruct(
                shape if shape[2] == LANES else (shape[1] * shape[2], shape[0]), BF16
            )
            for shape in shapes
        ],
        in_specs=[vmem] * 6,
        out_specs=[vmem] * 4,
        name="join",
    )(*helds, join_weight, join_bias)
    return tuple(
        out if out.ndim == 3 else out.reshape(*shape[1:], shape[0]).transpose(2, 0, 1)
        for out, shape in zip(outs, shapes)
    )


def local(section_in, conv_weight, conv_bias, join_weight, join_bias):
    helds = front(section_in[0, 0, 0], conv_weight[0], conv_bias[0])
    return joined(helds, join_weight, join_bias)


def solution(mesh):
    in_specs = (
        P("branch", "row", "col", None, None),
        P("branch", None, None, None, None, None),
        P("branch", None, None),
        P(),
        P(),
    )
    out_specs = (P(None, ("branch", "row"), "col"),) * 4
    return jax.shard_map(local, mesh=mesh, in_specs=in_specs, out_specs=out_specs, check_vma=False)
```

```python
from functools import partial

import jax
import jax.numpy as jnp
from jax import lax
from jax.experimental import pallas as pl
from jax.experimental.pallas import tpu as pltpu
from jax.sharding import PartitionSpec as P

WIDTH = 48
TH = 32
TW = 128
LANES = 128
STRIPS = 4
MESH = pl.DeviceIdType.MESH
WAYS = [(dr, dc) for dr in (-1, 0, 1) for dc in (-1, 0, 1) if dr or dc]
F32 = jnp.float32
BF16 = jnp.bfloat16

OWN_TILES = (32, 8, 2, 1)
BEFORE = (2, 1, 1, 0)
FIELD_TILES = (36, 10, 4, 1)
HIDDEN_TILES = (34, 10, 4, 1)


CHUNKS = (4, 2, 2, 1)
RELAYS = 12


def route(source, tile, strip, chunk):
    if tile == source or strip == tile:
        return None
    if source == 0 and strip == 3 - tile and chunk % 2 == 0:
        return None
    return strip


def relayed(source, place):
    pieces = [
        (tile, strip, chunk)
        for chunk in range(CHUNKS[source])
        for tile in range(STRIPS)
        for strip in range(STRIPS)
        if tile != place and route(source, tile, strip, chunk) == place
    ]
    return sorted(pieces, key=lambda p: (p[2], (p[0] ^ place).bit_count(), -abs(p[0] - source)))


def own_pieces(source, place):
    chunks = range(CHUNKS[source])
    if source == place:
        return [(place ^ turn, chunk) for turn in (0, 1, 2, 3) for chunk in chunks]
    return [(place ^ turn, chunk) for chunk in chunks for turn in (1, 2, 0, 3)]


def lane_index(width=LANES):
    return lax.broadcasted_iota(jnp.int32, (1, width), 1)


def turned(group, shift):
    shift = shift % LANES
    return pltpu.roll(group, shift, 1) if shift else group


def tiles_turned(field, shift):
    if shift % LANES == 0:
        return field
    tiles = [turned(field[:, t : t + LANES], shift) for t in range(0, field.shape[1], LANES)]
    return tiles[0] if len(tiles) == 1 else jnp.concatenate(tiles, axis=1)


def natural_tile(branch_level, container_ref):
    pixels = TH * TW >> 2 * branch_level
    channels = WIDTH << branch_level
    parts = []
    for part in range(1 << branch_level):
        at = part * pixels
        low = at // LANES * LANES
        piece = container_ref[:, low : low + max(pixels, LANES)]
        if at > low:
            piece = pltpu.roll(piece.astype(F32), LANES - at + low, 1).astype(BF16)
        parts.append(piece)
    held = lax.broadcasted_iota(jnp.int32, (1, channels), 1)
    part = sum((held >= WIDTH * turn).astype(jnp.int32) for turn in range(1, 1 << branch_level))
    home = ((held - WIDTH * part) << branch_level) + part
    order = jnp.where(lax.broadcasted_iota(jnp.int32, (channels, channels), 0) == home, 1.0, 0.0)
    return jnp.dot(
        order.astype(BF16), jnp.concatenate(parts, axis=0), preferred_element_type=F32
    ).astype(BF16)


def column_stack(branch_level, own, west, east):
    cols = TW >> branch_level
    col = lane_index(own.shape[1]) & (cols - 1)
    own32 = own.astype(F32)
    minus = tiles_turned(
        jnp.where(col == cols - 1, tiles_turned(west.astype(F32), -cols), own32), 1
    ).astype(BF16)
    plus = tiles_turned(
        jnp.where(col == 0, tiles_turned(east.astype(F32), cols), own32), -1
    ).astype(BF16)

    def zeros(rows):
        return jnp.zeros((rows, own.shape[1]), BF16)

    if branch_level == 0:
        pieces = [minus, own, zeros(32), plus, zeros(80)]
    elif branch_level == 3:
        pieces = [minus, own, plus]
    else:
        pad = zeros(-own.shape[0] % LANES)
        pieces = [minus, pad, own, pad, plus, pad]
    return jnp.concatenate(pieces, axis=0)


def taps(branch_level, weights, layer):
    channels = WIDTH << branch_level
    width = -(-channels // LANES) * LANES
    lines = []
    for dy in range(3):
        if branch_level == 0:
            first, middle, last = (weights[layer, dy, dx, 0:channels, 0:width] for dx in range(3))
            pair = jnp.where(
                lane_index() < channels,
                first.astype(F32),
                pltpu.roll(middle.astype(F32), channels, 1),
            )
            lines.append(jnp.concatenate([pair.astype(BF16), last], axis=1))
        else:
            lines.append(
                jnp.concatenate(
                    [weights[layer, dy, dx, 0:channels, 0:width] for dx in range(3)], axis=1
                )
            )
    return jnp.concatenate(lines, axis=0)


def row_sum(branch_level, products, first, count):
    channels = products.shape[0] // 3
    cols = TW >> branch_level
    above, here, below = (products[d * channels : (d + 1) * channels] for d in range(3))
    span = slice(first * LANES, (first + count) * LANES)
    if cols == LANES:
        return (
            above[:, (first - 1) * LANES : (first - 1 + count) * LANES]
            + here[:, span]
            + below[:, (first + 1) * LANES : (first + 1 + count) * LANES]
        )
    last = products.shape[1] // LANES - 1
    above, below = tiles_turned(above, cols), tiles_turned(below, -cols)
    lane = lane_index()

    def tile(field, t):
        t = min(max(t, 0), last)
        return field[:, t * LANES : (t + 1) * LANES]

    tiles = [
        jnp.where(lane < cols, tile(above, t - 1), tile(above, t))
        + tile(here, t)
        + jnp.where(lane >= LANES - cols, tile(below, t + 1), tile(below, t))
        for t in range(first, first + count)
    ]
    return tiles[0] if count == 1 else jnp.concatenate(tiles, axis=1)


def front_kernel(
    section, kernels, biases, join_weight, join_bias, out0, out1, out2, out3,
    held0, held1, held2, held3, mix, mix_bias, pool0, pool1, pool2,
    container, weights, bias, own0, own1, own2, own3, side0, side1, side2, side3,
    pack_send, pack_recv, hide0, hide1, hide2, hide3, hid0, hid1, hid2, hid3,
    settled0, settled1, settled2, settled3, relay0, relay1, relay2, relay3, load_sem,
    halo_send, halo_recv, hidden_send, hidden_recv, strip_send, strip_recv, relay_recv, own_sem,
):
    level = lax.axis_index("branch")
    place = lax.axis_index("row")
    col = lax.axis_index("col")
    row_count = lax.axis_size("row")
    col_count = lax.axis_size("col")

    def reach(dr, dc):
        there = jnp.bool_(True)
        if dr:
            there = (place + dr >= 0) & (place + dr < row_count)
        if dc:
            sideways = (col + dc >= 0) & (col + dc < col_count)
            there = there & sideways if dr else sideways
        device = (
            level,
            lax.rem(place + dr + row_count, row_count),
            lax.rem(col + dc + col_count, col_count),
        )
        return there, device

    barrier = pltpu.get_barrier_semaphore()
    expected = 0
    for dr, dc in WAYS:
        there, device = reach(dr, dc)
        expected = expected + there.astype(jnp.int32)

        @pl.when(there)
        def _():
            pl.semaphore_signal(barrier, inc=1, device_id=device, device_id_type=MESH)

    at_home = level == place
    for step in range(1, STRIPS):
        for device in (
            (level, lax.rem(place + step, STRIPS), col),
            (lax.rem(level + step, STRIPS), place, col),
        ):
            pl.semaphore_signal(barrier, inc=1, device_id=device, device_id_type=MESH)

    @pl.when((level > 0) & (place == STRIPS - 1 - level))
    def _():
        pl.semaphore_signal(barrier, inc=1, device_id=(0, level, col), device_id_type=MESH)

    expected = expected + 2 * (STRIPS - 1) + ((level == 0) & (place > 0)).astype(jnp.int32)

    helds = (held0, held1, held2, held3)
    owns = (own0, own1, own2, own3)
    sides = (side0, side1, side2, side3)
    hides = (hide0, hide1, hide2, hide3)
    hids = (hid0, hid1, hid2, hid3)
    settleds = (settled0, settled1, settled2, settled3)
    relays = (relay0, relay1, relay2, relay3)

    mix_loads = [
        pltpu.make_async_copy(join_weight, mix, load_sem.at[4]),
        pltpu.make_async_copy(join_bias, mix_bias, load_sem.at[5]),
    ]

    def branch(b):
        channels = WIDTH << b
        width = -(-channels // LANES) * LANES
        pixels = TH * TW >> b
        cols, rows = TW >> b, TH >> b
        own, side, hide, hid = owns[b], sides[b], hides[b], hids[b]
        settled, held, relay = settleds[b], helds[b], relays[b]
        before, tiles = BEFORE[b], OWN_TILES[b]
        middle = slice(before * LANES, (before + tiles) * LANES)
        packed = b >= 2
        folds = channels // 96
        pair = 2 * cols
        chunks = CHUNKS[b]
        lane = lane_index()
        order = [way for way in WAYS if way[0]] + [way for way in WAYS if not way[0]]

        load = pltpu.make_async_copy(
            section.at[:, 0:pixels],
            own.at[:, middle] if b == 0 else container.at[:, 0:pixels],
            load_sem.at[0],
        )
        bias_load = pltpu.make_async_copy(biases, bias, load_sem.at[1])
        weight_loads = [
            pltpu.make_async_copy(
                kernels.at[layer, :, :, 0:channels, 0:width],
                weights.at[layer, :, :, 0:channels, 0:width],
                load_sem.at[2 + layer],
            )
            for layer in range(2)
        ]

        def begin():
            for copy in (load, bias_load, *weight_loads, *mix_loads):
                copy.start()

        def halo_region(dr, dc):
            if packed and dr:
                return pack_recv.at[WAYS.index((dr, dc))]
            target = own if dc == 0 else side.at[0 if dc == 1 else 1]
            if dr == 0:
                return target.at[:, middle]
            if dr == 1:
                return target.at[:, 0 : before * LANES]
            return target.at[:, (before + tiles) * LANES : (before + tiles + before) * LANES]

        def halo_source(dr):
            if dr == 0:
                return own.at[:, middle]
            if packed:
                return pack_send.at[0 if dr == -1 else 1]
            first = before if dr == -1 else tiles
            return own.at[:, first * LANES : (first + before) * LANES]

        def halo_copy(dr, dc):
            way = WAYS.index((dr, dc))
            return pltpu.make_async_remote_copy(
                src_ref=halo_source(dr),
                dst_ref=halo_region(dr, dc),
                send_sem=halo_send.at[way],
                recv_sem=halo_recv.at[way],
                device_id=reach(dr, dc)[1],
                device_id_type=MESH,
            )

        def hidden_copy(dc):
            at = 0 if dc == 1 else 1
            return pltpu.make_async_remote_copy(
                src_ref=hid,
                dst_ref=hide.at[at],
                send_sem=hidden_send.at[at],
                recv_sem=hidden_recv.at[at],
                device_id=reach(0, dc)[1],
                device_id_type=MESH,
            )

        def ends(strip, chunk):
            if b == 3:
                return settled.at[strip], held
            if b == 2:
                size = channels // chunks
                span = slice(chunk * size, (chunk + 1) * size)
                tile = strip // 2
                return settled.at[span, tile * LANES : (tile + 1) * LANES], held.at[span]
            size = tiles * LANES // STRIPS // chunks
            at = (strip * chunks + chunk) * size
            return settled.at[:, at : at + size], held.at[:, chunk * size : (chunk + 1) * size]

        def exchange(here, closing=False):
            count = 0

            def send(source, target, arrived, device):
                nonlocal count
                copy = pltpu.make_async_remote_copy(
                    src_ref=source,
                    dst_ref=target,
                    send_sem=strip_send.at[count],
                    recv_sem=arrived,
                    device_id=device,
                    device_id_type=MESH,
                )
                count += 1
                if closing:
                    copy.wait_send()
                else:
                    copy.start()

            at_once = []
            for strip, chunk in own_pieces(b, here):
                source, target = ends(strip, chunk)
                if here == b and strip == here:
                    if not closing:
                        copy = pltpu.make_async_copy(source, target, own_sem.at[chunk])
                        copy.start()
                        at_once.append(copy)
                    continue
                via = route(b, here, strip, chunk)
                if via is None:
                    send(source, target, strip_recv.at[b], (here, strip, col))
                else:
                    slot = relayed(b, via).index((here, strip, chunk))
                    send(source, relay.at[slot], relay_recv.at[slot], (b, via, col))
            for slot, (tile, strip, chunk) in enumerate(relayed(b, here)):
                piece = relay.at[slot]
                if not closing:
                    pltpu.make_async_remote_copy(
                        src_ref=piece,
                        dst_ref=piece,
                        send_sem=strip_send.at[0],
                        recv_sem=relay_recv.at[slot],
                        device_id=(b, tile, col),
                        device_id_type=MESH,
                    ).wait_recv()
                send(piece, ends(strip, chunk)[1], strip_recv.at[b], (tile, strip, col))
            for copy in at_once:
                copy.wait()

        def run():
            load.wait()
            if b:
                own[:, middle] = natural_tile(b, container)
            if packed:
                for end in range(2):
                    tile = before if end == 0 else before + tiles - 1
                    at = 0 if end == 0 else (rows - 2) * cols % LANES
                    edge = own[:, tile * LANES : (tile + 1) * LANES].astype(F32)
                    out = None
                    for g in range(folds):
                        part = turned(edge[g * 96 : (g + 1) * 96], pair * g - at)
                        out = part if g == 0 else jnp.where(lane < pair * g, out, part)
                    pack_send[end] = out.astype(BF16)

            pl.semaphore_wait(barrier, expected)
            for dr, dc in order:
                pl.when(reach(dr, dc)[0])(halo_copy(dr, dc).start)
            for dr, dc in order:

                @pl.when(jnp.logical_not(reach(-dr, -dc)[0]))
                def _():
                    region = halo_region(dr, dc)
                    region[...] = jnp.zeros(region.shape, BF16)

            bias_load.wait()
            offsets = [
                jnp.broadcast_to(bias[layer : layer + 1, :], (8, bias.shape[1])).T[:channels, 0:1]
                for layer in range(2)
            ]
            weight_loads[0].wait()
            for dr, dc in order:
                pl.when(reach(-dr, -dc)[0])(halo_copy(dr, dc).wait_recv)

            fields = [own, side.at[0], side.at[1]]
            if packed:
                for at, dc in enumerate((0, 1, -1)):
                    upper = pack_recv[WAYS.index((1, dc))].astype(F32)
                    lower = pack_recv[WAYS.index((-1, dc))].astype(F32)
                    lines = []
                    for g in range(folds):
                        span = slice(g * 96, (g + 1) * 96)
                        here = fields[at][span, middle]
                        above = turned(upper, LANES - pair - pair * g)
                        if b == 3:
                            ring = jnp.where(lane < 96, turned(lower, 64 - pair * g), above)
                            lines.append(jnp.where(lane < 64, here.astype(F32), ring).astype(BF16))
                        else:
                            below = turned(lower, -pair * g)
                            lines.append(
                                jnp.concatenate([above.astype(BF16), here, below.astype(BF16)], axis=1)
                            )
                    fields[at] = jnp.concatenate(lines, axis=0)
            else:
                fields = [field[...] for field in fields]

            products = jnp.dot(
                taps(b, weights, 0),
                column_stack(b, *fields),
                preferred_element_type=F32,
            )
            first = 1 if b == 0 else 0
            hidden = row_sum(b, products, first, HIDDEN_TILES[b])
            hidden = jnp.maximum(hidden + offsets[0], 0.0)
            row = lax.shift_right_logical(lane_index(HIDDEN_TILES[b] * LANES), cols.bit_length() - 1)
            if b == 3:
                row = jnp.where(row >= 6, row - 8, row)
            else:
                row = row - (before - first) * (LANES // cols)
            low = jnp.where(place == 0, 0, -LANES)
            high = jnp.where(place == row_count - 1, rows, 2 * LANES)
            hidden = jnp.where((row >= low) & (row < high), hidden, 0.0)
            hid[...] = hidden.astype(BF16)

            for dc in (1, -1):
                pl.when(reach(0, dc)[0])(hidden_copy(dc).start)
            for dc in (1, -1):

                @pl.when(jnp.logical_not(reach(0, -dc)[0]))
                def _():
                    at = 0 if dc == 1 else 1
                    hide[at] = jnp.zeros(hid.shape, BF16)

            weight_loads[1].wait()
            for dc in (1, -1):
                pl.when(reach(0, -dc)[0])(hidden_copy(dc).wait_recv)
            products = jnp.dot(
                taps(b, weights, 1),
                column_stack(b, hid[...], hide[0], hide[1]),
                preferred_element_type=F32,
            )
            after = row_sum(b, products, 1 if b == 0 else before, tiles)
            final = jnp.maximum(after + offsets[1] + own[:, middle].astype(F32), 0.0)
            if b < 3:
                settled[...] = final.astype(BF16)
            else:
                for strip in range(STRIPS):
                    out = None
                    for g in range(8):
                        part = turned(final[g * WIDTH : (g + 1) * WIDTH], 16 * g - 16 * strip)
                        out = part if g == 0 else jnp.where(lane < 16 * g, out, part)
                    settled[strip] = out.astype(BF16)

            for here in range(STRIPS):
                pl.when(place == here)(partial(exchange, here))

        def close():
            for here in range(STRIPS):
                pl.when(place == here)(partial(exchange, here, True))
            for dr, dc in order:
                pl.when(reach(dr, dc)[0])(halo_copy(dr, dc).wait_send)
            for dc in (1, -1):
                pl.when(reach(0, dc)[0])(hidden_copy(dc).wait_send)

        return begin, run, close

    branches = [branch(b) for b in range(STRIPS)]
    for b, (begin, _, _) in enumerate(branches):
        pl.when(level == b)(begin)

    pool_refs = (pool0, pool1, pool2)
    for fine, pool in enumerate(pool_refs):
        pool[...] = pool_table(fine)

    for b, (_, run, _) in enumerate(branches):
        pl.when(level == b)(run)

    for copy in mix_loads:
        copy.wait()

    def arrived(source):
        arrival = pltpu.make_async_remote_copy(
            src_ref=helds[source],
            dst_ref=helds[source],
            send_sem=strip_send.at[0],
            recv_sem=strip_recv.at[source],
            device_id=(source, level, col),
            device_id_type=MESH,
        )
        pl.when(jnp.logical_not(at_home & (level == source)))(arrival.wait_recv)

    join(place, arrived, helds, mix, mix_bias, pool_refs, (out0, out1, out2, out3))

    for b, (_, _, close) in enumerate(branches):
        pl.when(level == b)(close)


def coarse_home(fine_level, coarse_level):
    fine_cols, coarse_cols = TW >> fine_level, TW >> coarse_level
    shift = coarse_level - fine_level
    pixel = lax.broadcasted_iota(jnp.int32, (strip_pixels(fine_level), 1), 0)
    row = lax.shift_right_logical(pixel, fine_cols.bit_length() - 1 + shift)
    return row * coarse_cols + lax.shift_right_logical(pixel & (fine_cols - 1), shift)


def strip_pixels(branch_level):
    return TH * TW // STRIPS >> 2 * branch_level


def pool_table(fine_level):
    at = 0
    hits = []
    for coarse_level in range(fine_level + 1, STRIPS):
        hits.append((at, at + coarse_home(fine_level, coarse_level)))
        at += strip_pixels(coarse_level)
    tiles = []
    for tile in range(-(-at // LANES)):
        target = lane_index() + tile * LANES
        hit = None
        for first, home in hits:
            same = home == target
            hit = same if hit is None else hit | same
        tiles.append(jnp.where(hit, 1.0, 0.0).astype(BF16))
    table = tiles[0] if len(tiles) == 1 else jnp.concatenate(tiles, axis=1)
    short = max(LANES - table.shape[0], 0)
    if short:
        table = jnp.concatenate([table, jnp.zeros((short, table.shape[1]), BF16)], axis=0)
    return table


def product(mix, rows, source, data):
    start = ((1 << source) - 1) * WIDTH
    stop = start + data.shape[0]
    low = start // LANES * LANES
    high = min(-(-stop // LANES) * LANES, mix.shape[1])
    pieces = [data]
    if start > low:
        pieces.insert(0, jnp.zeros((start - low, data.shape[1]), BF16))
    if high > stop:
        pieces.append(jnp.zeros((high - stop, data.shape[1]), BF16))
    stacked = jnp.concatenate(pieces, axis=0)
    return jnp.dot(
        mix[rows, low:high], stacked, preferred_element_type=F32
    ).astype(BF16).astype(F32)


def spread(term, pool):
    return lax.dot_general(
        term.astype(BF16), pool, (((1,), (1,)), ((), ())), preferred_element_type=F32
    )


def join(place, arrived, helds, mix, mix_bias, pools, outs):
    lane = lane_index()
    total = mix_bias.shape[0]
    line = jnp.concatenate([mix_bias[...][None, :], jnp.zeros((1, -total % LANES), F32)], axis=1)
    offset = jnp.broadcast_to(line, (8, line.shape[1])).T
    starts = [((1 << b) - 1) * WIDTH for b in range(STRIPS + 1)]
    offsets = [offset[starts[b] : starts[b + 1], 0:1] for b in range(STRIPS)]
    one, two, three = (slice(starts[b], starts[b + 1]) for b in range(1, STRIPS))

    arrived(3)
    folded = helds[3][...].astype(F32)
    last = jnp.concatenate([turned(folded, -16 * g) for g in range(8)], axis=0)
    from3 = product(mix, slice(0, starts[3]), 3, last.astype(BF16))

    arrived(2)
    pieces = helds[2][...].astype(F32)
    third = jnp.where(lax.rem(place, 2) == 1, turned(pieces, 64), pieces)
    third16 = third.astype(BF16)
    from2 = product(mix, slice(0, starts[2]), 2, third16)
    shrunk = jnp.dot(third16, pools[2][...], preferred_element_type=F32)
    total3 = last + offsets[3] + product(mix, three, 2, (shrunk * 0.25).astype(BF16))
    total2 = third + offsets[2] + spread(from3[two], pools[2][...])

    def side_by_side(near, far):
        return jnp.where(lane < 64, near, jnp.where(lane < 80, turned(far, 64), 0.0))

    arrived(1)
    second = helds[1][...]
    from1 = product(mix, slice(0, starts[1]), 1, second)
    shrunk = jnp.dot(second, pools[1][...], preferred_element_type=F32)
    shrunk = shrunk * jnp.where(lane < 64, 0.25, 0.0625)
    down1 = product(mix, slice(starts[2], total), 1, shrunk.astype(BF16))
    total2 = total2 + down1[: starts[3] - starts[2]]
    tail3 = down1[starts[3] - starts[2] :]
    total1 = second.astype(F32) + offsets[1]
    total1 = total1 + spread(side_by_side(from2[one], from3[one]), pools[1][...])
    first = slice(0, starts[1])
    total0 = offsets[0] + spread(
        jnp.concatenate([from1, side_by_side(from2[first], from3[first])], axis=1), pools[0][...]
    )

    arrived(0)
    maps = helds[0][...]
    shrunk = jnp.dot(maps, pools[0][...], preferred_element_type=F32)
    near = (shrunk[:, :256] * 0.25).astype(BF16)
    far = (shrunk[:, 256:] * jnp.where(lane < 64, 0.0625, 0.015625)).astype(BF16)
    total1 = total1 + product(mix, one, 0, near)
    down0 = product(mix, slice(starts[2], total), 0, far)
    total2 = total2 + down0[: starts[3] - starts[2]]
    total3 = total3 + turned(tail3 + down0[starts[3] - starts[2] :], -64)
    total0 = jnp.maximum(total0 + maps.astype(F32), 0.0)
    lines = [total0[:, at : at + LANES] for at in range(0, total0.shape[1], LANES)]
    outs[0][...] = jnp.stack(lines, axis=1).astype(BF16)
    for out, value in zip(outs[1:], (total1, total2, total3)):
        out[...] = jnp.maximum(value, 0.0).T[: out.shape[0]].astype(BF16)


HELD_SHAPES = ((48, 1024), (96, 256), (192, 128), (48, 128))


def front(section, kernels, biases, join_weight, join_bias):
    anywhere = pl.BlockSpec(memory_space=pl.ANY)
    vmem = pl.BlockSpec(memory_space=pltpu.VMEM)

    def field(b, tiles):
        return (WIDTH << b, tiles[b] * LANES)

    scratch = [pltpu.VMEM(shape, BF16) for shape in HELD_SHAPES]
    scratch += [pltpu.VMEM(join_weight.shape, BF16), pltpu.VMEM(join_bias.shape, F32)]
    scratch += [pltpu.VMEM(shape, BF16) for shape in ((1024, 384), (256, 128), (128, 128))]
    scratch += [
        pltpu.VMEM((WIDTH, TH * TW // 2), BF16),
        pltpu.VMEM(kernels.shape, BF16),
        pltpu.VMEM(biases.shape, F32),
    ]
    scratch += [pltpu.VMEM(field(b, FIELD_TILES), BF16) for b in range(4)]
    scratch += [pltpu.VMEM((2, *field(b, FIELD_TILES)), BF16) for b in range(4)]
    scratch += [pltpu.VMEM((2, 96, LANES), BF16), pltpu.VMEM((8, 96, LANES), BF16)]
    scratch += [pltpu.VMEM((2, *field(b, HIDDEN_TILES)), BF16) for b in range(4)]
    scratch += [pltpu.VMEM(field(b, HIDDEN_TILES), BF16) for b in range(4)]
    scratch += [pltpu.VMEM(field(b, OWN_TILES), BF16) for b in range(3)]
    scratch += [pltpu.VMEM((STRIPS, WIDTH, LANES), BF16)]
    pieces = ((48, 256), (96, 128), (96, 128), (48, 128))
    scratch += [pltpu.VMEM((RELAYS, *piece), BF16) for piece in pieces]
    counts = (6, 8, 8, 2, 2, 16 + RELAYS, 4, RELAYS, 4)
    scratch += [pltpu.SemaphoreType.DMA((count,)) for count in counts]
    return pl.pallas_call(
        front_kernel,
        out_shape=[pltpu.VMEM(shape, BF16) for shape in OUT_SHAPES],
        in_specs=[anywhere] * 5,
        out_specs=[vmem] * 4,
        scratch_shapes=scratch,
        compiler_params=pltpu.CompilerParams(
            collective_id=0, has_side_effects=True, vmem_limit_bytes=VMEM_LIMIT
        ),
        name="front",
    )(
        *(
            pltpu.with_memory_space_constraint(array, pltpu.HBM)
            for array in (section, kernels, biases, join_weight, join_bias)
        )
    )


OUT_SHAPES = ((48, 8, 128), (256, 96), (64, 192), (16, 384))
VMEM_LIMIT = 48 << 20


def finish_kernel(*refs):
    sources, targets, sem = refs[:4], refs[4:8], refs[8]
    copies = [
        pltpu.make_async_copy(source, target, sem.at[at])
        for at, (source, target) in enumerate(zip(sources, targets))
    ]
    for copy in copies:
        copy.start()
    for copy in copies:
        copy.wait()


def finished(outs):
    return pl.pallas_call(
        finish_kernel,
        out_shape=[jax.ShapeDtypeStruct(out.shape, out.dtype) for out in outs],
        in_specs=[pl.BlockSpec(memory_space=pltpu.VMEM)] * 4,
        out_specs=[pl.BlockSpec(memory_space=pl.ANY)] * 4,
        scratch_shapes=[pltpu.SemaphoreType.DMA((4,))],
        compiler_params=pltpu.CompilerParams(vmem_limit_bytes=1 << 20),
        name="finish",
    )(*outs)


def local(section_in, conv_weight, conv_bias, join_weight, join_bias):
    outs = finished(
        front(section_in[0, 0, 0], conv_weight[0], conv_bias[0], join_weight, join_bias)
    )
    shapes = [(WIDTH << b, (TH >> b) // STRIPS, TW >> b) for b in range(4)]
    return tuple(
        out if out.ndim == 3 else out.reshape(*shape[1:], shape[0]).transpose(2, 0, 1)
        for out, shape in zip(outs, shapes)
    )


def solution(mesh):
    in_specs = (
        P("branch", "row", "col", None, None),
        P("branch", None, None, None, None, None),
        P("branch", None, None),
        P(),
        P(),
    )
    out_specs = (P(None, ("branch", "row"), "col"),) * 4
    return jax.shard_map(local, mesh=mesh, in_specs=in_specs, out_specs=out_specs, check_vma=False)
```

```python
from functools import partial

import jax
import jax.numpy as jnp
from jax import lax
from jax.experimental import pallas as pl
from jax.experimental.pallas import tpu as pltpu
from jax.sharding import PartitionSpec as P

WIDTH = 48
TH = 32
TW = 128
LANES = 128
STRIPS = 4
MESH = pl.DeviceIdType.MESH
WAYS = [(dr, dc) for dr in (-1, 0, 1) for dc in (-1, 0, 1) if dr or dc]
F32 = jnp.float32
BF16 = jnp.bfloat16

OWN_TILES = (32, 8, 2, 1)
BEFORE = (2, 1, 1, 0)
FIELD_TILES = (36, 10, 4, 1)
HIDDEN_TILES = (34, 10, 4, 1)
HIDDEN_START = (1, 0, 0, 0)


CHUNKS = (4, 2, 2, 1)
RELAYS = 12


def route(source, tile, strip, chunk):
    if tile == source or strip == tile:
        return None
    if source == 0 and strip == 3 - tile and chunk % 2 == 0:
        return None
    return strip


def relayed(source, place):
    pieces = [
        (tile, strip, chunk)
        for chunk in range(CHUNKS[source])
        for tile in range(STRIPS)
        for strip in range(STRIPS)
        if tile != place and route(source, tile, strip, chunk) == place
    ]
    return sorted(pieces, key=lambda p: (p[2], (p[0] ^ place).bit_count(), -abs(p[0] - source)))


def own_pieces(source, place):
    chunks = range(CHUNKS[source])
    if source == place:
        return [(place ^ turn, chunk) for turn in (0, 1, 2, 3) for chunk in chunks]
    return [(place ^ turn, chunk) for chunk in chunks for turn in (1, 2, 0, 3)]


def lane_index(width=LANES):
    return lax.broadcasted_iota(jnp.int32, (1, width), 1)


def turned(group, shift):
    shift = shift % LANES
    return pltpu.roll(group, shift, 1) if shift else group


def tiles_turned(field, shift):
    if shift % LANES == 0:
        return field
    tiles = [turned(field[:, t : t + LANES], shift) for t in range(0, field.shape[1], LANES)]
    return tiles[0] if len(tiles) == 1 else jnp.concatenate(tiles, axis=1)


def natural_tile(branch_level, container_ref):
    pixels = TH * TW >> 2 * branch_level
    channels = WIDTH << branch_level
    parts = []
    for part in range(1 << branch_level):
        at = part * pixels
        low = at // LANES * LANES
        piece = container_ref[:, low : low + max(pixels, LANES)]
        if at > low:
            piece = pltpu.roll(piece.astype(F32), LANES - at + low, 1).astype(BF16)
        parts.append(piece)
    held = lax.broadcasted_iota(jnp.int32, (1, channels), 1)
    part = sum((held >= WIDTH * turn).astype(jnp.int32) for turn in range(1, 1 << branch_level))
    home = ((held - WIDTH * part) << branch_level) + part
    order = jnp.where(lax.broadcasted_iota(jnp.int32, (channels, channels), 0) == home, 1.0, 0.0)
    return jnp.dot(
        order.astype(BF16), jnp.concatenate(parts, axis=0), preferred_element_type=F32
    ).astype(BF16)


def column_stack(branch_level, own, west, east):
    cols = TW >> branch_level
    col = lane_index(own.shape[1]) & (cols - 1)
    own32 = own.astype(F32)
    minus = tiles_turned(
        jnp.where(col == cols - 1, tiles_turned(west.astype(F32), -cols), own32), 1
    ).astype(BF16)
    plus = tiles_turned(
        jnp.where(col == 0, tiles_turned(east.astype(F32), cols), own32), -1
    ).astype(BF16)

    def zeros(rows):
        return jnp.zeros((rows, own.shape[1]), BF16)

    if branch_level == 0:
        pieces = [minus, own, zeros(32), plus, zeros(80)]
    elif branch_level == 3:
        pieces = [minus, own, plus]
    else:
        pad = zeros(-own.shape[0] % LANES)
        pieces = [minus, pad, own, pad, plus, pad]
    return jnp.concatenate(pieces, axis=0)


def taps(branch_level, weights, layer):
    channels = WIDTH << branch_level
    width = -(-channels // LANES) * LANES
    lines = []
    for dy in range(3):
        if branch_level == 0:
            first, middle, last = (weights[layer, dy, dx, 0:channels, 0:width] for dx in range(3))
            pair = jnp.where(
                lane_index() < channels,
                first.astype(F32),
                pltpu.roll(middle.astype(F32), channels, 1),
            )
            lines.append(jnp.concatenate([pair.astype(BF16), last], axis=1))
        else:
            lines.append(
                jnp.concatenate(
                    [weights[layer, dy, dx, 0:channels, 0:width] for dx in range(3)], axis=1
                )
            )
    return jnp.concatenate(lines, axis=0)


def row_sum(branch_level, products, first, count):
    channels = products.shape[0] // 3
    cols = TW >> branch_level
    above, here, below = (products[d * channels : (d + 1) * channels] for d in range(3))
    span = slice(first * LANES, (first + count) * LANES)
    if cols == LANES:
        return (
            above[:, (first - 1) * LANES : (first - 1 + count) * LANES]
            + here[:, span]
            + below[:, (first + 1) * LANES : (first + 1 + count) * LANES]
        )
    last = products.shape[1] // LANES - 1
    above, below = tiles_turned(above, cols), tiles_turned(below, -cols)
    lane = lane_index()

    def tile(field, t):
        t = min(max(t, 0), last)
        return field[:, t * LANES : (t + 1) * LANES]

    tiles = [
        jnp.where(lane < cols, tile(above, t - 1), tile(above, t))
        + tile(here, t)
        + jnp.where(lane >= LANES - cols, tile(below, t + 1), tile(below, t))
        for t in range(first, first + count)
    ]
    return tiles[0] if count == 1 else jnp.concatenate(tiles, axis=1)


def front_kernel(
    section, kernels, biases, join_weight, join_bias, out0, out1, out2, out3,
    held0, held1, held2, held3, mix, mix_bias, pool0, pool1, pool2,
    container, weights, bias, own0, own1, own2, own3, side0, side1, side2, side3,
    pack_send, pack_recv, hide0, hide1, hide2, hide3, hid0, hid1, hid2, hid3,
    settled0, settled1, settled2, settled3, relay0, relay1, relay2, relay3, load_sem,
    halo_send, halo_recv, hidden_send, hidden_recv, strip_send, strip_recv, relay_recv, own_sem,
):
    level = lax.axis_index("branch")
    place = lax.axis_index("row")
    col = lax.axis_index("col")
    row_count = lax.axis_size("row")
    col_count = lax.axis_size("col")

    def reach(dr, dc):
        there = jnp.bool_(True)
        if dr:
            there = (place + dr >= 0) & (place + dr < row_count)
        if dc:
            sideways = (col + dc >= 0) & (col + dc < col_count)
            there = there & sideways if dr else sideways
        device = (
            level,
            lax.rem(place + dr + row_count, row_count),
            lax.rem(col + dc + col_count, col_count),
        )
        return there, device

    barrier = pltpu.get_barrier_semaphore()
    expected = 0
    for dr, dc in WAYS:
        there, device = reach(dr, dc)
        expected = expected + there.astype(jnp.int32)

        @pl.when(there)
        def _():
            pl.semaphore_signal(barrier, inc=1, device_id=device, device_id_type=MESH)

    at_home = level == place
    for step in range(1, STRIPS):
        for device in (
            (level, lax.rem(place + step, STRIPS), col),
            (lax.rem(level + step, STRIPS), place, col),
        ):
            pl.semaphore_signal(barrier, inc=1, device_id=device, device_id_type=MESH)

    @pl.when((level > 0) & (place == STRIPS - 1 - level))
    def _():
        pl.semaphore_signal(barrier, inc=1, device_id=(0, level, col), device_id_type=MESH)

    expected = expected + 2 * (STRIPS - 1) + ((level == 0) & (place > 0)).astype(jnp.int32)

    helds = (held0, held1, held2, held3)
    owns = (own0, own1, own2, own3)
    sides = (side0, side1, side2, side3)
    hides = (hide0, hide1, hide2, hide3)
    hids = (hid0, hid1, hid2, hid3)
    settleds = (settled0, settled1, settled2, settled3)
    relays = (relay0, relay1, relay2, relay3)

    mix_loads = [
        pltpu.make_async_copy(join_weight, mix, load_sem.at[4]),
        pltpu.make_async_copy(join_bias, mix_bias, load_sem.at[5]),
    ]

    def branch(b):
        channels = WIDTH << b
        width = -(-channels // LANES) * LANES
        pixels = TH * TW >> b
        cols, rows = TW >> b, TH >> b
        own, side, hide, hid = owns[b], sides[b], hides[b], hids[b]
        settled, held, relay = settleds[b], helds[b], relays[b]
        before, tiles = BEFORE[b], OWN_TILES[b]
        middle = slice(before * LANES, (before + tiles) * LANES)
        packed = b >= 2
        folds = channels // 96
        pair = 2 * cols
        chunks = CHUNKS[b]
        lane = lane_index()
        order = [way for way in WAYS if way[0]] + [way for way in WAYS if not way[0]]

        load = pltpu.make_async_copy(
            section.at[:, 0:pixels],
            own.at[:, middle] if b == 0 else container.at[:, 0:pixels],
            load_sem.at[0],
        )
        bias_load = pltpu.make_async_copy(biases, bias, load_sem.at[1])
        weight_loads = [
            pltpu.make_async_copy(
                kernels.at[layer, :, :, 0:channels, 0:width],
                weights.at[layer, :, :, 0:channels, 0:width],
                load_sem.at[2 + layer],
            )
            for layer in range(2)
        ]

        def begin():
            for copy in (load, bias_load, *weight_loads, *mix_loads):
                copy.start()

        def halo_region(dr, dc):
            if packed and dr:
                return pack_recv.at[WAYS.index((dr, dc))]
            target = own if dc == 0 else side.at[0 if dc == 1 else 1]
            if dr == 0:
                return target.at[:, middle]
            if dr == 1:
                return target.at[:, 0 : before * LANES]
            return target.at[:, (before + tiles) * LANES : (before + tiles + before) * LANES]

        def halo_source(dr):
            if dr == 0:
                return own.at[:, middle]
            if packed:
                return pack_send.at[0 if dr == -1 else 1]
            first = before if dr == -1 else tiles
            return own.at[:, first * LANES : (first + before) * LANES]

        def halo_copy(dr, dc):
            way = WAYS.index((dr, dc))
            return pltpu.make_async_remote_copy(
                src_ref=halo_source(dr),
                dst_ref=halo_region(dr, dc),
                send_sem=halo_send.at[way],
                recv_sem=halo_recv.at[way],
                device_id=reach(dr, dc)[1],
                device_id_type=MESH,
            )

        last = HIDDEN_TILES[b]
        if b < 2:
            hidden_parts = ((2, last - 2), (0, 2), (last - 2, last))
        else:
            hidden_parts = ((0, last),)

        def hidden_copy(dc, part):
            at = 0 if dc == 1 else 1
            low, high = hidden_parts[part]
            span = slice(low * LANES, high * LANES)
            return pltpu.make_async_remote_copy(
                src_ref=hid.at[:, span],
                dst_ref=hide.at[at, :, span],
                send_sem=hidden_send.at[at, part],
                recv_sem=hidden_recv.at[at, part],
                device_id=reach(0, dc)[1],
                device_id_type=MESH,
            )

        def hidden_start(*parts):
            for part in parts:
                for dc in (1, -1):
                    pl.when(reach(0, dc)[0])(hidden_copy(dc, part).start)

        def hidden_wait(*parts):
            for part in parts:
                for dc in (1, -1):
                    pl.when(reach(0, -dc)[0])(hidden_copy(dc, part).wait_recv)

        def bias_columns():
            bias_load.wait()
            return [
                jnp.broadcast_to(bias[layer : layer + 1, :], (8, bias.shape[1])).T[:channels, 0:1]
                for layer in range(2)
            ]

        def convolved(layer, fields, first, count):
            products = jnp.dot(
                taps(b, weights, layer), column_stack(b, *fields), preferred_element_type=F32
            )
            return row_sum(b, products, first, count)

        def settle_hidden(raw, offset, first):
            count = raw.shape[1] // LANES
            row = lax.shift_right_logical(lane_index(count * LANES), cols.bit_length() - 1)
            if b == 3:
                row = jnp.where(row >= 6, row - 8, row)
            else:
                row = row + (first + HIDDEN_START[b] - before) * (LANES // cols)
            low = jnp.where(place == 0, 0, -LANES)
            high = jnp.where(place == row_count - 1, rows, 2 * LANES)
            hidden = jnp.where((row >= low) & (row < high), jnp.maximum(raw + offset, 0.0), 0.0)
            hid[:, first * LANES : (first + count) * LANES] = hidden.astype(BF16)

        def hidden_tiles(offset, first, count):
            low = max(first + HIDDEN_START[b] - 1, 0)
            high = min(first + HIDDEN_START[b] + count + 1, FIELD_TILES[b])
            span = slice(low * LANES, high * LANES)
            fields = (own[:, span], side[0, :, span], side[1, :, span])
            start = first + HIDDEN_START[b] - low
            settle_hidden(convolved(0, fields, start, count), offset, first)

        def settled_tiles(offset, first, count):
            span = slice(first * LANES, (first + count + 2) * LANES)
            fields = (hid[:, span], hide[0, :, span], hide[1, :, span])
            after = convolved(1, fields, 1, count)
            kept = own[:, (before + first) * LANES : (before + first + count) * LANES]
            final = jnp.maximum(after + offset + kept.astype(F32), 0.0)
            settled[:, first * LANES : (first + count) * LANES] = final.astype(BF16)

        def ends(strip, chunk):
            if b == 3:
                return settled.at[strip], held
            if b == 2:
                size = channels // chunks
                span = slice(chunk * size, (chunk + 1) * size)
                tile = strip // 2
                return settled.at[span, tile * LANES : (tile + 1) * LANES], held.at[span]
            size = tiles * LANES // STRIPS // chunks
            at = (strip * chunks + chunk) * size
            return settled.at[:, at : at + size], held.at[:, chunk * size : (chunk + 1) * size]

        def exchange(here, strips=(), handing=False, closing=False):
            count = 0

            def send(source, target, arrived, device, act=True):
                nonlocal count
                copy = pltpu.make_async_remote_copy(
                    src_ref=source,
                    dst_ref=target,
                    send_sem=strip_send.at[count],
                    recv_sem=arrived,
                    device_id=device,
                    device_id_type=MESH,
                )
                count += 1
                if closing:
                    copy.wait_send()
                elif act:
                    copy.start()

            at_once = []
            for strip, chunk in own_pieces(b, here):
                source, target = ends(strip, chunk)
                act = strip in strips
                if here == b and strip == here:
                    copy = pltpu.make_async_copy(source, target, own_sem.at[chunk])
                    if act:
                        copy.start()
                    if handing:
                        at_once.append(copy)
                    continue
                via = route(b, here, strip, chunk)
                if via is None:
                    send(source, target, strip_recv.at[b], (here, strip, col), act)
                else:
                    slot = relayed(b, via).index((here, strip, chunk))
                    send(source, relay.at[slot], relay_recv.at[slot], (b, via, col), act)
            if not handing and not closing:
                return
            for slot, (tile, strip, chunk) in enumerate(relayed(b, here)):
                piece = relay.at[slot]
                if not closing:
                    pltpu.make_async_remote_copy(
                        src_ref=piece,
                        dst_ref=piece,
                        send_sem=strip_send.at[0],
                        recv_sem=relay_recv.at[slot],
                        device_id=(b, tile, col),
                        device_id_type=MESH,
                    ).wait_recv()
                send(piece, ends(strip, chunk)[1], strip_recv.at[b], (tile, strip, col))
            for copy in at_once:
                copy.wait()

        def run():
            load.wait()
            if b:
                own[:, middle] = natural_tile(b, container)
            if packed:
                for end in range(2):
                    tile = before if end == 0 else before + tiles - 1
                    at = 0 if end == 0 else (rows - 2) * cols % LANES
                    edge = own[:, tile * LANES : (tile + 1) * LANES].astype(F32)
                    out = None
                    for g in range(folds):
                        part = turned(edge[g * 96 : (g + 1) * 96], pair * g - at)
                        out = part if g == 0 else jnp.where(lane < pair * g, out, part)
                    pack_send[end] = out.astype(BF16)

            pl.semaphore_wait(barrier, expected)
            for dr, dc in order:
                pl.when(reach(dr, dc)[0])(halo_copy(dr, dc).start)
            for dr, dc in order:

                @pl.when(jnp.logical_not(reach(-dr, -dc)[0]))
                def _():
                    region = halo_region(dr, dc)
                    region[...] = jnp.zeros(region.shape, BF16)

            for dc in (1, -1):

                @pl.when(jnp.logical_not(reach(0, -dc)[0]))
                def _():
                    at = 0 if dc == 1 else 1
                    hide[at] = jnp.zeros(hid.shape, BF16)

            def halo_wait(ways):
                for dr, dc in ways:
                    pl.when(reach(-dr, -dc)[0])(halo_copy(dr, dc).wait_recv)

            def leave(**how):
                for here in range(STRIPS):
                    pl.when(place == here)(partial(exchange, here, **how))

            offsets = bias_columns()
            weight_loads[0].wait()
            if not packed:
                size = tiles // STRIPS
                halo_wait([way for way in order if not way[0]])
                hidden_tiles(offsets[0], 2, last - 4)
                hidden_start(0)
                halo_wait([way for way in order if way[0]])
                hidden_tiles(offsets[0], 0, 2)
                hidden_tiles(offsets[0], last - 2, 2)
                hidden_start(1, 2)
                weight_loads[1].wait()
                hidden_wait(0)
                settled_tiles(offsets[1], size, 2 * size)
                leave(strips=(1, 2))
                hidden_wait(1)
                settled_tiles(offsets[1], 0, size)
                hidden_wait(2)
                settled_tiles(offsets[1], 3 * size, size)
                leave(strips=(0, 3), handing=True)
                return

            halo_wait(order)
            fields = []
            for target, dc in ((own, 0), (side.at[0], 1), (side.at[1], -1)):
                upper = pack_recv[WAYS.index((1, dc))].astype(F32)
                lower = pack_recv[WAYS.index((-1, dc))].astype(F32)
                lines = []
                for g in range(folds):
                    here = target[g * 96 : (g + 1) * 96, middle]
                    above = turned(upper, LANES - pair - pair * g)
                    if b == 3:
                        ring = jnp.where(lane < 96, turned(lower, 64 - pair * g), above)
                        lines.append(jnp.where(lane < 64, here.astype(F32), ring).astype(BF16))
                    else:
                        below = turned(lower, -pair * g)
                        lines.append(
                            jnp.concatenate([above.astype(BF16), here, below.astype(BF16)], axis=1)
                        )
                fields.append(jnp.concatenate(lines, axis=0))
            settle_hidden(convolved(0, fields, 0, last), offsets[0], 0)
            hidden_start(0)
            weight_loads[1].wait()
            hidden_wait(0)
            after = convolved(1, (hid[...], hide[0], hide[1]), before, tiles)
            final = jnp.maximum(after + offsets[1] + own[:, middle].astype(F32), 0.0)
            if b < 3:
                settled[...] = final.astype(BF16)
            else:
                for strip in range(STRIPS):
                    out = None
                    for g in range(8):
                        part = turned(final[g * WIDTH : (g + 1) * WIDTH], 16 * g - 16 * strip)
                        out = part if g == 0 else jnp.where(lane < 16 * g, out, part)
                    settled[strip] = out.astype(BF16)

            leave(strips=range(STRIPS), handing=True)

        def close():
            for here in range(STRIPS):
                pl.when(place == here)(partial(exchange, here, closing=True))
            for dr, dc in order:
                pl.when(reach(dr, dc)[0])(halo_copy(dr, dc).wait_send)
            for part in range(len(hidden_parts)):
                for dc in (1, -1):
                    pl.when(reach(0, dc)[0])(hidden_copy(dc, part).wait_send)

        return begin, run, close

    branches = [branch(b) for b in range(STRIPS)]
    for b, (begin, _, _) in enumerate(branches):
        pl.when(level == b)(begin)

    pool_refs = (pool0, pool1, pool2)
    for fine, pool in enumerate(pool_refs):
        pool[...] = pool_table(fine)

    for b, (_, run, _) in enumerate(branches):
        pl.when(level == b)(run)

    for copy in mix_loads:
        copy.wait()

    def arrived(source):
        arrival = pltpu.make_async_remote_copy(
            src_ref=helds[source],
            dst_ref=helds[source],
            send_sem=strip_send.at[0],
            recv_sem=strip_recv.at[source],
            device_id=(source, level, col),
            device_id_type=MESH,
        )
        pl.when(jnp.logical_not(at_home & (level == source)))(arrival.wait_recv)

    join(place, arrived, helds, mix, mix_bias, pool_refs, (out0, out1, out2, out3))

    for b, (_, _, close) in enumerate(branches):
        pl.when(level == b)(close)


def coarse_home(fine_level, coarse_level):
    fine_cols, coarse_cols = TW >> fine_level, TW >> coarse_level
    shift = coarse_level - fine_level
    pixel = lax.broadcasted_iota(jnp.int32, (strip_pixels(fine_level), 1), 0)
    row = lax.shift_right_logical(pixel, fine_cols.bit_length() - 1 + shift)
    return row * coarse_cols + lax.shift_right_logical(pixel & (fine_cols - 1), shift)


def strip_pixels(branch_level):
    return TH * TW // STRIPS >> 2 * branch_level


def pool_table(fine_level):
    at = 0
    hits = []
    for coarse_level in range(fine_level + 1, STRIPS):
        hits.append((at, at + coarse_home(fine_level, coarse_level)))
        at += strip_pixels(coarse_level)
    tiles = []
    for tile in range(-(-at // LANES)):
        target = lane_index() + tile * LANES
        hit = None
        for first, home in hits:
            same = home == target
            hit = same if hit is None else hit | same
        tiles.append(jnp.where(hit, 1.0, 0.0).astype(BF16))
    table = tiles[0] if len(tiles) == 1 else jnp.concatenate(tiles, axis=1)
    short = max(LANES - table.shape[0], 0)
    if short:
        table = jnp.concatenate([table, jnp.zeros((short, table.shape[1]), BF16)], axis=0)
    return table


def product(mix, rows, source, data):
    start = ((1 << source) - 1) * WIDTH
    stop = start + data.shape[0]
    low = start // LANES * LANES
    high = min(-(-stop // LANES) * LANES, mix.shape[1])
    pieces = [data]
    if start > low:
        pieces.insert(0, jnp.zeros((start - low, data.shape[1]), BF16))
    if high > stop:
        pieces.append(jnp.zeros((high - stop, data.shape[1]), BF16))
    stacked = jnp.concatenate(pieces, axis=0)
    return jnp.dot(
        mix[rows, low:high], stacked, preferred_element_type=F32
    ).astype(BF16).astype(F32)


def spread(term, pool):
    return lax.dot_general(
        term.astype(BF16), pool, (((1,), (1,)), ((), ())), preferred_element_type=F32
    )


def join(place, arrived, helds, mix, mix_bias, pools, outs):
    lane = lane_index()
    total = mix_bias.shape[0]
    line = jnp.concatenate([mix_bias[...][None, :], jnp.zeros((1, -total % LANES), F32)], axis=1)
    offset = jnp.broadcast_to(line, (8, line.shape[1])).T
    starts = [((1 << b) - 1) * WIDTH for b in range(STRIPS + 1)]
    offsets = [offset[starts[b] : starts[b + 1], 0:1] for b in range(STRIPS)]
    one, two, three = (slice(starts[b], starts[b + 1]) for b in range(1, STRIPS))

    arrived(3)
    folded = helds[3][...].astype(F32)
    last = jnp.concatenate([turned(folded, -16 * g) for g in range(8)], axis=0)
    from3 = product(mix, slice(0, starts[3]), 3, last.astype(BF16))

    arrived(2)
    pieces = helds[2][...].astype(F32)
    third = jnp.where(lax.rem(place, 2) == 1, turned(pieces, 64), pieces)
    third16 = third.astype(BF16)
    from2 = product(mix, slice(0, starts[2]), 2, third16)
    shrunk = jnp.dot(third16, pools[2][...], preferred_element_type=F32)
    total3 = last + offsets[3] + product(mix, three, 2, (shrunk * 0.25).astype(BF16))
    total2 = third + offsets[2] + spread(from3[two], pools[2][...])

    def side_by_side(near, far):
        return jnp.where(lane < 64, near, jnp.where(lane < 80, turned(far, 64), 0.0))

    arrived(1)
    second = helds[1][...]
    from1 = product(mix, slice(0, starts[1]), 1, second)
    shrunk = jnp.dot(second, pools[1][...], preferred_element_type=F32)
    shrunk = shrunk * jnp.where(lane < 64, 0.25, 0.0625)
    down1 = product(mix, slice(starts[2], total), 1, shrunk.astype(BF16))
    total2 = total2 + down1[: starts[3] - starts[2]]
    tail3 = down1[starts[3] - starts[2] :]
    total1 = second.astype(F32) + offsets[1]
    total1 = total1 + spread(side_by_side(from2[one], from3[one]), pools[1][...])
    first = slice(0, starts[1])
    total0 = offsets[0] + spread(
        jnp.concatenate([from1, side_by_side(from2[first], from3[first])], axis=1), pools[0][...]
    )

    arrived(0)
    maps = helds[0][...]
    shrunk = jnp.dot(maps, pools[0][...], preferred_element_type=F32)
    near = (shrunk[:, :256] * 0.25).astype(BF16)
    far = (shrunk[:, 256:] * jnp.where(lane < 64, 0.0625, 0.015625)).astype(BF16)
    total1 = total1 + product(mix, one, 0, near)
    down0 = product(mix, slice(starts[2], total), 0, far)
    total2 = total2 + down0[: starts[3] - starts[2]]
    total3 = total3 + turned(tail3 + down0[starts[3] - starts[2] :], -64)
    total0 = jnp.maximum(total0 + maps.astype(F32), 0.0)
    lines = [total0[:, at : at + LANES] for at in range(0, total0.shape[1], LANES)]
    outs[0][...] = jnp.stack(lines, axis=1).astype(BF16)
    for out, value in zip(outs[1:], (total1, total2, total3)):
        out[...] = jnp.maximum(value, 0.0).T[: out.shape[0]].astype(BF16)


HELD_SHAPES = ((48, 1024), (96, 256), (192, 128), (48, 128))


def front(section, kernels, biases, join_weight, join_bias):
    anywhere = pl.BlockSpec(memory_space=pl.ANY)
    vmem = pl.BlockSpec(memory_space=pltpu.VMEM)

    def field(b, tiles):
        return (WIDTH << b, tiles[b] * LANES)

    scratch = [pltpu.VMEM(shape, BF16) for shape in HELD_SHAPES]
    scratch += [pltpu.VMEM(join_weight.shape, BF16), pltpu.VMEM(join_bias.shape, F32)]
    scratch += [pltpu.VMEM(shape, BF16) for shape in ((1024, 384), (256, 128), (128, 128))]
    scratch += [
        pltpu.VMEM((WIDTH, TH * TW // 2), BF16),
        pltpu.VMEM(kernels.shape, BF16),
        pltpu.VMEM(biases.shape, F32),
    ]
    scratch += [pltpu.VMEM(field(b, FIELD_TILES), BF16) for b in range(4)]
    scratch += [pltpu.VMEM((2, *field(b, FIELD_TILES)), BF16) for b in range(4)]
    scratch += [pltpu.VMEM((2, 96, LANES), BF16), pltpu.VMEM((8, 96, LANES), BF16)]
    scratch += [pltpu.VMEM((2, *field(b, HIDDEN_TILES)), BF16) for b in range(4)]
    scratch += [pltpu.VMEM(field(b, HIDDEN_TILES), BF16) for b in range(4)]
    scratch += [pltpu.VMEM(field(b, OWN_TILES), BF16) for b in range(3)]
    scratch += [pltpu.VMEM((STRIPS, WIDTH, LANES), BF16)]
    pieces = ((48, 256), (96, 128), (96, 128), (48, 128))
    scratch += [pltpu.VMEM((RELAYS, *piece), BF16) for piece in pieces]
    counts = ((6,), (8,), (8,), (2, 3), (2, 3), (16 + RELAYS,), (4,), (RELAYS,), (4,))
    scratch += [pltpu.SemaphoreType.DMA(count) for count in counts]
    return pl.pallas_call(
        front_kernel,
        out_shape=[pltpu.VMEM(shape, BF16) for shape in OUT_SHAPES],
        in_specs=[anywhere] * 5,
        out_specs=[vmem] * 4,
        scratch_shapes=scratch,
        compiler_params=pltpu.CompilerParams(
            collective_id=0, has_side_effects=True, vmem_limit_bytes=VMEM_LIMIT
        ),
        name="front",
    )(
        *(
            pltpu.with_memory_space_constraint(array, pltpu.HBM)
            for array in (section, kernels, biases, join_weight, join_bias)
        )
    )


OUT_SHAPES = ((48, 8, 128), (256, 96), (64, 192), (16, 384))
VMEM_LIMIT = 48 << 20


def finish_kernel(*refs):
    sources, targets, sem = refs[:4], refs[4:8], refs[8]
    copies = [
        pltpu.make_async_copy(source, target, sem.at[at])
        for at, (source, target) in enumerate(zip(sources, targets))
    ]
    for copy in copies:
        copy.start()
    for copy in copies:
        copy.wait()


def finished(outs):
    return pl.pallas_call(
        finish_kernel,
        out_shape=[jax.ShapeDtypeStruct(out.shape, out.dtype) for out in outs],
        in_specs=[pl.BlockSpec(memory_space=pltpu.VMEM)] * 4,
        out_specs=[pl.BlockSpec(memory_space=pl.ANY)] * 4,
        scratch_shapes=[pltpu.SemaphoreType.DMA((4,))],
        compiler_params=pltpu.CompilerParams(vmem_limit_bytes=1 << 20),
        name="finish",
    )(*outs)


def local(section_in, conv_weight, conv_bias, join_weight, join_bias):
    outs = finished(
        front(section_in[0, 0, 0], conv_weight[0], conv_bias[0], join_weight, join_bias)
    )
    shapes = [(WIDTH << b, (TH >> b) // STRIPS, TW >> b) for b in range(4)]
    return tuple(
        out if out.ndim == 3 else out.reshape(*shape[1:], shape[0]).transpose(2, 0, 1)
        for out, shape in zip(outs, shapes)
    )


def solution(mesh):
    in_specs = (
        P("branch", "row", "col", None, None),
        P("branch", None, None, None, None, None),
        P("branch", None, None),
        P(),
        P(),
    )
    out_specs = (P(None, ("branch", "row"), "col"),) * 4
    return jax.shard_map(local, mesh=mesh, in_specs=in_specs, out_specs=out_specs, check_vma=False)
```

```python
from functools import partial

import jax
import jax.numpy as jnp
from jax import lax
from jax.experimental import pallas as pl
from jax.experimental.pallas import tpu as pltpu
from jax.sharding import PartitionSpec as P

WIDTH = 48
TH = 32
TW = 128
LANES = 128
STRIPS = 4
MESH = pl.DeviceIdType.MESH
WAYS = [(dr, dc) for dr in (-1, 0, 1) for dc in (-1, 0, 1) if dr or dc]
F32 = jnp.float32
BF16 = jnp.bfloat16

OWN_TILES = (32, 8, 2, 1)
BEFORE = (2, 1, 1, 0)
FIELD_TILES = (36, 10, 4, 1)
HIDDEN_TILES = (34, 10, 4, 1)
HIDDEN_START = (1, 0, 0, 0)


CHUNKS = (4, 2, 2, 1)
RELAYS = 12


def route(source, tile, strip, chunk):
    if tile == source or strip == tile or source >= 2:
        return None
    if source == 0 and strip == 3 - tile and chunk % 2 == 0:
        return None
    return strip


def relayed(source, place):
    pieces = [
        (tile, strip, chunk)
        for chunk in range(CHUNKS[source])
        for tile in range(STRIPS)
        for strip in range(STRIPS)
        if tile != place and route(source, tile, strip, chunk) == place
    ]
    return sorted(pieces, key=lambda p: (p[2], (p[0] ^ place).bit_count(), -abs(p[0] - source)))


def own_pieces(source, place):
    chunks = range(CHUNKS[source])
    if source == place:
        return [(place ^ turn, chunk) for turn in (0, 1, 2, 3) for chunk in chunks]
    return [(place ^ turn, chunk) for chunk in chunks for turn in (1, 2, 0, 3)]


def lane_index(width=LANES):
    return lax.broadcasted_iota(jnp.int32, (1, width), 1)


def turned(group, shift):
    shift = shift % LANES
    return pltpu.roll(group, shift, 1) if shift else group


def tiles_turned(field, shift):
    if shift % LANES == 0:
        return field
    tiles = [turned(field[:, t : t + LANES], shift) for t in range(0, field.shape[1], LANES)]
    return tiles[0] if len(tiles) == 1 else jnp.concatenate(tiles, axis=1)


def natural_tile(branch_level, container_ref):
    pixels = TH * TW >> 2 * branch_level
    channels = WIDTH << branch_level
    parts = []
    for part in range(1 << branch_level):
        at = part * pixels
        low = at // LANES * LANES
        piece = container_ref[:, low : low + max(pixels, LANES)]
        if at > low:
            piece = pltpu.roll(piece.astype(F32), LANES - at + low, 1).astype(BF16)
        parts.append(piece)
    held = lax.broadcasted_iota(jnp.int32, (1, channels), 1)
    part = sum((held >= WIDTH * turn).astype(jnp.int32) for turn in range(1, 1 << branch_level))
    home = ((held - WIDTH * part) << branch_level) + part
    order = jnp.where(lax.broadcasted_iota(jnp.int32, (channels, channels), 0) == home, 1.0, 0.0)
    return jnp.dot(
        order.astype(BF16), jnp.concatenate(parts, axis=0), preferred_element_type=F32
    ).astype(BF16)


def column_stack(branch_level, own, west, east):
    cols = TW >> branch_level
    col = lane_index(own.shape[1]) & (cols - 1)
    own32 = own.astype(F32)
    minus = tiles_turned(
        jnp.where(col == cols - 1, tiles_turned(west.astype(F32), -cols), own32), 1
    ).astype(BF16)
    plus = tiles_turned(
        jnp.where(col == 0, tiles_turned(east.astype(F32), cols), own32), -1
    ).astype(BF16)

    def zeros(rows):
        return jnp.zeros((rows, own.shape[1]), BF16)

    if branch_level == 0:
        pieces = [minus, own, zeros(32), plus, zeros(80)]
    elif branch_level == 3:
        pieces = [minus, own, plus]
    else:
        pad = zeros(-own.shape[0] % LANES)
        pieces = [minus, pad, own, pad, plus, pad]
    return jnp.concatenate(pieces, axis=0)


def taps(branch_level, weights, layer):
    channels = WIDTH << branch_level
    width = -(-channels // LANES) * LANES
    lines = []
    for dy in range(3):
        if branch_level == 0:
            first, middle, last = (weights[layer, dy, dx, 0:channels, 0:width] for dx in range(3))
            pair = jnp.where(
                lane_index() < channels,
                first.astype(F32),
                pltpu.roll(middle.astype(F32), channels, 1),
            )
            lines.append(jnp.concatenate([pair.astype(BF16), last], axis=1))
        else:
            lines.append(
                jnp.concatenate(
                    [weights[layer, dy, dx, 0:channels, 0:width] for dx in range(3)], axis=1
                )
            )
    return jnp.concatenate(lines, axis=0)


def row_sum(branch_level, products, first, count):
    channels = products.shape[0] // 3
    cols = TW >> branch_level
    above, here, below = (products[d * channels : (d + 1) * channels] for d in range(3))
    span = slice(first * LANES, (first + count) * LANES)
    if cols == LANES:
        return (
            above[:, (first - 1) * LANES : (first - 1 + count) * LANES]
            + here[:, span]
            + below[:, (first + 1) * LANES : (first + 1 + count) * LANES]
        )
    last = products.shape[1] // LANES - 1
    above, below = tiles_turned(above, cols), tiles_turned(below, -cols)
    lane = lane_index()

    def tile(field, t):
        t = min(max(t, 0), last)
        return field[:, t * LANES : (t + 1) * LANES]

    tiles = [
        jnp.where(lane < cols, tile(above, t - 1), tile(above, t))
        + tile(here, t)
        + jnp.where(lane >= LANES - cols, tile(below, t + 1), tile(below, t))
        for t in range(first, first + count)
    ]
    return tiles[0] if count == 1 else jnp.concatenate(tiles, axis=1)


def front_kernel(
    section, kernels, biases, join_weight, join_bias, out0, out1, out2, out3,
    held0, held1, held2, held3, mix, mix_bias, pool0, pool1, pool2,
    container, weights, bias, own0, own1, own2, own3, side0, side1, side2, side3,
    pack_send, pack_recv, hide0, hide1, hide2, hide3, hid0, hid1, hid2, hid3,
    settled0, settled1, settled2, settled3, relay0, relay1, relay2, relay3, load_sem,
    halo_send, halo_recv, hidden_send, hidden_recv, strip_send, strip_recv, relay_recv, own_sem,
):
    level = lax.axis_index("branch")
    place = lax.axis_index("row")
    col = lax.axis_index("col")
    row_count = lax.axis_size("row")
    col_count = lax.axis_size("col")

    def reach(dr, dc):
        there = jnp.bool_(True)
        if dr:
            there = (place + dr >= 0) & (place + dr < row_count)
        if dc:
            sideways = (col + dc >= 0) & (col + dc < col_count)
            there = there & sideways if dr else sideways
        device = (
            level,
            lax.rem(place + dr + row_count, row_count),
            lax.rem(col + dc + col_count, col_count),
        )
        return there, device

    barrier = pltpu.get_barrier_semaphore()
    expected = 0
    for dr, dc in WAYS:
        there, device = reach(dr, dc)
        expected = expected + there.astype(jnp.int32)

        @pl.when(there)
        def _():
            pl.semaphore_signal(barrier, inc=1, device_id=device, device_id_type=MESH)

    at_home = level == place
    for step in range(1, STRIPS):
        for device in (
            (level, lax.rem(place + step, STRIPS), col),
            (lax.rem(level + step, STRIPS), place, col),
        ):
            pl.semaphore_signal(barrier, inc=1, device_id=device, device_id_type=MESH)

    @pl.when((level > 0) & (place == STRIPS - 1 - level))
    def _():
        pl.semaphore_signal(barrier, inc=1, device_id=(0, level, col), device_id_type=MESH)

    for far in (2, 3):

        @pl.when(jnp.logical_not(at_home & (level == far)))
        def _():
            pl.semaphore_signal(barrier, inc=1, device_id=(far, level, col), device_id_type=MESH)

    expected = expected + 2 * (STRIPS - 1) + ((level == 0) & (place > 0)).astype(jnp.int32)
    expected = expected + jnp.where(level >= 2, STRIPS - at_home.astype(jnp.int32), 0)

    helds = (held0, held1, held2, held3)
    owns = (own0, own1, own2, own3)
    sides = (side0, side1, side2, side3)
    hides = (hide0, hide1, hide2, hide3)
    hids = (hid0, hid1, hid2, hid3)
    settleds = (settled0, settled1, settled2, settled3)
    relays = (relay0, relay1, relay2, relay3)

    mix_loads = [
        pltpu.make_async_copy(join_weight, mix, load_sem.at[4]),
        pltpu.make_async_copy(join_bias, mix_bias, load_sem.at[5]),
    ]

    def branch(b):
        channels = WIDTH << b
        width = -(-channels // LANES) * LANES
        pixels = TH * TW >> b
        cols, rows = TW >> b, TH >> b
        own, side, hide, hid = owns[b], sides[b], hides[b], hids[b]
        settled, held, relay = settleds[b], helds[b], relays[b]
        before, tiles = BEFORE[b], OWN_TILES[b]
        middle = slice(before * LANES, (before + tiles) * LANES)
        packed = b >= 2
        folds = channels // 96
        pair = 2 * cols
        chunks = CHUNKS[b]
        lane = lane_index()
        order = [way for way in WAYS if way[0]] + [way for way in WAYS if not way[0]]

        load = pltpu.make_async_copy(
            section.at[:, 0:pixels],
            own.at[:, middle] if b == 0 else container.at[:, 0:pixels],
            load_sem.at[0],
        )
        bias_load = pltpu.make_async_copy(biases, bias, load_sem.at[1])
        weight_loads = [
            pltpu.make_async_copy(
                kernels.at[layer, :, :, 0:channels, 0:width],
                weights.at[layer, :, :, 0:channels, 0:width],
                load_sem.at[2 + layer],
            )
            for layer in range(2)
        ]

        def begin():
            for copy in (load, bias_load, *weight_loads, *mix_loads):
                copy.start()

        def halo_region(dr, dc):
            if packed and dr:
                return pack_recv.at[WAYS.index((dr, dc))]
            target = own if dc == 0 else side.at[0 if dc == 1 else 1]
            if dr == 0:
                return target.at[:, middle]
            if dr == 1:
                return target.at[:, 0 : before * LANES]
            return target.at[:, (before + tiles) * LANES : (before + tiles + before) * LANES]

        def halo_source(dr):
            if dr == 0:
                return own.at[:, middle]
            if packed:
                return pack_send.at[0 if dr == -1 else 1]
            first = before if dr == -1 else tiles
            return own.at[:, first * LANES : (first + before) * LANES]

        def halo_copy(dr, dc):
            way = WAYS.index((dr, dc))
            return pltpu.make_async_remote_copy(
                src_ref=halo_source(dr),
                dst_ref=halo_region(dr, dc),
                send_sem=halo_send.at[way],
                recv_sem=halo_recv.at[way],
                device_id=reach(dr, dc)[1],
                device_id_type=MESH,
            )

        last = HIDDEN_TILES[b]
        if b < 2:
            hidden_parts = ((2, last - 2), (0, 2), (last - 2, last))
        else:
            hidden_parts = ((0, last),)

        def hidden_copy(dc, part):
            at = 0 if dc == 1 else 1
            low, high = hidden_parts[part]
            span = slice(low * LANES, high * LANES)
            return pltpu.make_async_remote_copy(
                src_ref=hid.at[:, span],
                dst_ref=hide.at[at, :, span],
                send_sem=hidden_send.at[at, part],
                recv_sem=hidden_recv.at[at, part],
                device_id=reach(0, dc)[1],
                device_id_type=MESH,
            )

        def hidden_start(*parts):
            for part in parts:
                for dc in (1, -1):
                    pl.when(reach(0, dc)[0])(hidden_copy(dc, part).start)

        def hidden_wait(*parts):
            for part in parts:
                for dc in (1, -1):
                    pl.when(reach(0, -dc)[0])(hidden_copy(dc, part).wait_recv)

        def bias_columns():
            bias_load.wait()
            return [
                jnp.broadcast_to(bias[layer : layer + 1, :], (8, bias.shape[1])).T[:channels, 0:1]
                for layer in range(2)
            ]

        def convolved(layer, fields, first, count):
            products = jnp.dot(
                taps(b, weights, layer), column_stack(b, *fields), preferred_element_type=F32
            )
            return row_sum(b, products, first, count)

        def settle_hidden(raw, offset, first):
            count = raw.shape[1] // LANES
            row = lax.shift_right_logical(lane_index(count * LANES), cols.bit_length() - 1)
            if b == 3:
                row = jnp.where(row >= 6, row - 8, row)
            else:
                row = row + (first + HIDDEN_START[b] - before) * (LANES // cols)
            low = jnp.where(place == 0, 0, -LANES)
            high = jnp.where(place == row_count - 1, rows, 2 * LANES)
            hidden = jnp.where((row >= low) & (row < high), jnp.maximum(raw + offset, 0.0), 0.0)
            hid[:, first * LANES : (first + count) * LANES] = hidden.astype(BF16)

        def hidden_tiles(offset, first, count):
            low = max(first + HIDDEN_START[b] - 1, 0)
            high = min(first + HIDDEN_START[b] + count + 1, FIELD_TILES[b])
            span = slice(low * LANES, high * LANES)
            fields = (own[:, span], side[0, :, span], side[1, :, span])
            start = first + HIDDEN_START[b] - low
            settle_hidden(convolved(0, fields, start, count), offset, first)

        def settled_tiles(offset, first, count):
            span = slice(first * LANES, (first + count + 2) * LANES)
            fields = (hid[:, span], hide[0, :, span], hide[1, :, span])
            after = convolved(1, fields, 1, count)
            kept = own[:, (before + first) * LANES : (before + first + count) * LANES]
            final = jnp.maximum(after + offset + kept.astype(F32), 0.0)
            settled[:, first * LANES : (first + count) * LANES] = final.astype(BF16)

        def ends(strip, chunk):
            if b == 3:
                return settled.at[strip], held
            if b == 2:
                size = channels // chunks
                span = slice(chunk * size, (chunk + 1) * size)
                tile = strip // 2
                return settled.at[span, tile * LANES : (tile + 1) * LANES], held.at[span]
            size = tiles * LANES // STRIPS // chunks
            at = (strip * chunks + chunk) * size
            return settled.at[:, at : at + size], held.at[:, chunk * size : (chunk + 1) * size]

        def exchange(here, strips=(), handing=False, closing=False):
            count = 0

            def send(source, target, arrived, device, act=True):
                nonlocal count
                copy = pltpu.make_async_remote_copy(
                    src_ref=source,
                    dst_ref=target,
                    send_sem=strip_send.at[count],
                    recv_sem=arrived,
                    device_id=device,
                    device_id_type=MESH,
                )
                count += 1
                if closing:
                    copy.wait_send()
                elif act:
                    copy.start()

            at_once = []
            for strip, chunk in own_pieces(b, here):
                source, target = ends(strip, chunk)
                act = strip in strips
                if here == b and strip == here:
                    copy = pltpu.make_async_copy(source, target, own_sem.at[chunk])
                    if act:
                        copy.start()
                    if handing:
                        at_once.append(copy)
                    continue
                via = route(b, here, strip, chunk)
                if via is None:
                    send(source, target, strip_recv.at[b], (here, strip, col), act)
                else:
                    slot = relayed(b, via).index((here, strip, chunk))
                    send(source, relay.at[slot], relay_recv.at[slot], (b, via, col), act)
            if not handing and not closing:
                return
            for slot, (tile, strip, chunk) in enumerate(relayed(b, here)):
                piece = relay.at[slot]
                if not closing:
                    pltpu.make_async_remote_copy(
                        src_ref=piece,
                        dst_ref=piece,
                        send_sem=strip_send.at[0],
                        recv_sem=relay_recv.at[slot],
                        device_id=(b, tile, col),
                        device_id_type=MESH,
                    ).wait_recv()
                send(piece, ends(strip, chunk)[1], strip_recv.at[b], (tile, strip, col))
            for copy in at_once:
                copy.wait()

        def open_halo():
            load.wait()
            if b:
                own[:, middle] = natural_tile(b, container)
            if packed:
                for end in range(2):
                    tile = before if end == 0 else before + tiles - 1
                    at = 0 if end == 0 else (rows - 2) * cols % LANES
                    edge = own[:, tile * LANES : (tile + 1) * LANES].astype(F32)
                    out = None
                    for g in range(folds):
                        part = turned(edge[g * 96 : (g + 1) * 96], pair * g - at)
                        out = part if g == 0 else jnp.where(lane < pair * g, out, part)
                    pack_send[end] = out.astype(BF16)

            pl.semaphore_wait(barrier, expected)
            for dr, dc in order:
                pl.when(reach(dr, dc)[0])(halo_copy(dr, dc).start)
            for dr, dc in order:

                @pl.when(jnp.logical_not(reach(-dr, -dc)[0]))
                def _():
                    region = halo_region(dr, dc)
                    region[...] = jnp.zeros(region.shape, BF16)

            for dc in (1, -1):

                @pl.when(jnp.logical_not(reach(0, -dc)[0]))
                def _():
                    at = 0 if dc == 1 else 1
                    hide[at] = jnp.zeros(hid.shape, BF16)

        def run():
            def halo_wait(ways):
                for dr, dc in ways:
                    pl.when(reach(-dr, -dc)[0])(halo_copy(dr, dc).wait_recv)

            def leave(early, **how):
                for here in range(STRIPS):
                    soon = [strip for strip in (1, 2) if strip != STRIPS - 1 - here]
                    strips = soon if early else [s for s in range(STRIPS) if s not in soon or packed]
                    pl.when(place == here)(partial(exchange, here, strips, **how))

            offsets = bias_columns()
            weight_loads[0].wait()
            if not packed:
                size = tiles // STRIPS
                halo_wait([way for way in order if not way[0]])
                hidden_tiles(offsets[0], 2, last - 4)
                hidden_start(0)
                halo_wait([way for way in order if way[0]])
                hidden_tiles(offsets[0], 0, 2)
                hidden_tiles(offsets[0], last - 2, 2)
                hidden_start(1, 2)
                weight_loads[1].wait()
                hidden_wait(0)
                settled_tiles(offsets[1], size, 2 * size)
                leave(True)
                hidden_wait(1)
                settled_tiles(offsets[1], 0, size)
                hidden_wait(2)
                settled_tiles(offsets[1], 3 * size, size)
                leave(False, handing=True)
                return

            halo_wait(order)
            fields = []
            for target, dc in ((own, 0), (side.at[0], 1), (side.at[1], -1)):
                upper = pack_recv[WAYS.index((1, dc))].astype(F32)
                lower = pack_recv[WAYS.index((-1, dc))].astype(F32)
                lines = []
                for g in range(folds):
                    here = target[g * 96 : (g + 1) * 96, middle]
                    above = turned(upper, LANES - pair - pair * g)
                    if b == 3:
                        ring = jnp.where(lane < 96, turned(lower, 64 - pair * g), above)
                        lines.append(jnp.where(lane < 64, here.astype(F32), ring).astype(BF16))
                    else:
                        below = turned(lower, -pair * g)
                        lines.append(
                            jnp.concatenate([above.astype(BF16), here, below.astype(BF16)], axis=1)
                        )
                fields.append(jnp.concatenate(lines, axis=0))
            settle_hidden(convolved(0, fields, 0, last), offsets[0], 0)
            hidden_start(0)
            weight_loads[1].wait()
            hidden_wait(0)
            after = convolved(1, (hid[...], hide[0], hide[1]), before, tiles)
            final = jnp.maximum(after + offsets[1] + own[:, middle].astype(F32), 0.0)
            if b < 3:
                settled[...] = final.astype(BF16)
            else:
                for strip in range(STRIPS):
                    out = None
                    for g in range(8):
                        part = turned(final[g * WIDTH : (g + 1) * WIDTH], 16 * g - 16 * strip)
                        out = part if g == 0 else jnp.where(lane < 16 * g, out, part)
                    settled[strip] = out.astype(BF16)

            leave(False, handing=True)

        def close():
            for here in range(STRIPS):
                pl.when(place == here)(partial(exchange, here, closing=True))
            for dr, dc in order:
                pl.when(reach(dr, dc)[0])(halo_copy(dr, dc).wait_send)
            for part in range(len(hidden_parts)):
                for dc in (1, -1):
                    pl.when(reach(0, dc)[0])(hidden_copy(dc, part).wait_send)

        return begin, open_halo, run, close

    branches = [branch(b) for b in range(STRIPS)]
    for b, (begin, _, _, _) in enumerate(branches):
        pl.when(level == b)(begin)
    for b, (_, open_halo, _, _) in enumerate(branches):
        pl.when(level == b)(open_halo)

    pool_refs = (pool0, pool1, pool2)
    for fine, pool in enumerate(pool_refs):
        pool[...] = pool_table(fine)

    for b, (_, _, run, _) in enumerate(branches):
        pl.when(level == b)(run)

    for copy in mix_loads:
        copy.wait()

    def arrived(source):
        arrival = pltpu.make_async_remote_copy(
            src_ref=helds[source],
            dst_ref=helds[source],
            send_sem=strip_send.at[0],
            recv_sem=strip_recv.at[source],
            device_id=(source, level, col),
            device_id_type=MESH,
        )
        pl.when(jnp.logical_not(at_home & (level == source)))(arrival.wait_recv)

    join(place, arrived, helds, mix, mix_bias, pool_refs, (out0, out1, out2, out3))

    for b, (_, _, _, close) in enumerate(branches):
        pl.when(level == b)(close)


def coarse_home(fine_level, coarse_level):
    fine_cols, coarse_cols = TW >> fine_level, TW >> coarse_level
    shift = coarse_level - fine_level
    pixel = lax.broadcasted_iota(jnp.int32, (strip_pixels(fine_level), 1), 0)
    row = lax.shift_right_logical(pixel, fine_cols.bit_length() - 1 + shift)
    return row * coarse_cols + lax.shift_right_logical(pixel & (fine_cols - 1), shift)


def strip_pixels(branch_level):
    return TH * TW // STRIPS >> 2 * branch_level


def pool_table(fine_level):
    at = 0
    hits = []
    for coarse_level in range(fine_level + 1, STRIPS):
        hits.append((at, at + coarse_home(fine_level, coarse_level)))
        at += strip_pixels(coarse_level)
    tiles = []
    for tile in range(-(-at // LANES)):
        target = lane_index() + tile * LANES
        hit = None
        for first, home in hits:
            same = home == target
            hit = same if hit is None else hit | same
        tiles.append(jnp.where(hit, 1.0, 0.0).astype(BF16))
    table = tiles[0] if len(tiles) == 1 else jnp.concatenate(tiles, axis=1)
    short = max(LANES - table.shape[0], 0)
    if short:
        table = jnp.concatenate([table, jnp.zeros((short, table.shape[1]), BF16)], axis=0)
    return table


def product(mix, rows, source, data):
    start = ((1 << source) - 1) * WIDTH
    stop = start + data.shape[0]
    low = start // LANES * LANES
    high = min(-(-stop // LANES) * LANES, mix.shape[1])
    pieces = [data]
    if start > low:
        pieces.insert(0, jnp.zeros((start - low, data.shape[1]), BF16))
    if high > stop:
        pieces.append(jnp.zeros((high - stop, data.shape[1]), BF16))
    stacked = jnp.concatenate(pieces, axis=0)
    return jnp.dot(
        mix[rows, low:high], stacked, preferred_element_type=F32
    ).astype(BF16).astype(F32)


def spread(term, pool):
    return lax.dot_general(
        term.astype(BF16), pool, (((1,), (1,)), ((), ())), preferred_element_type=F32
    )


def join(place, arrived, helds, mix, mix_bias, pools, outs):
    lane = lane_index()
    total = mix_bias.shape[0]
    line = jnp.concatenate([mix_bias[...][None, :], jnp.zeros((1, -total % LANES), F32)], axis=1)
    offset = jnp.broadcast_to(line, (8, line.shape[1])).T
    starts = [((1 << b) - 1) * WIDTH for b in range(STRIPS + 1)]
    offsets = [offset[starts[b] : starts[b + 1], 0:1] for b in range(STRIPS)]
    one, two, three = (slice(starts[b], starts[b + 1]) for b in range(1, STRIPS))

    arrived(3)
    folded = helds[3][...].astype(F32)
    last = jnp.concatenate([turned(folded, -16 * g) for g in range(8)], axis=0)
    from3 = product(mix, slice(0, starts[3]), 3, last.astype(BF16))

    arrived(2)
    pieces = helds[2][...].astype(F32)
    third = jnp.where(lax.rem(place, 2) == 1, turned(pieces, 64), pieces)
    third16 = third.astype(BF16)
    from2 = product(mix, slice(0, starts[2]), 2, third16)
    shrunk = jnp.dot(third16, pools[2][...], preferred_element_type=F32)
    total3 = last + offsets[3] + product(mix, three, 2, (shrunk * 0.25).astype(BF16))
    total2 = third + offsets[2] + spread(from3[two], pools[2][...])

    def side_by_side(near, far):
        return jnp.where(lane < 64, near, jnp.where(lane < 80, turned(far, 64), 0.0))

    arrived(1)
    second = helds[1][...]
    from1 = product(mix, slice(0, starts[1]), 1, second)
    shrunk = jnp.dot(second, pools[1][...], preferred_element_type=F32)
    shrunk = shrunk * jnp.where(lane < 64, 0.25, 0.0625)
    down1 = product(mix, slice(starts[2], total), 1, shrunk.astype(BF16))
    total2 = total2 + down1[: starts[3] - starts[2]]
    tail3 = down1[starts[3] - starts[2] :]
    total1 = second.astype(F32) + offsets[1]
    total1 = total1 + spread(side_by_side(from2[one], from3[one]), pools[1][...])
    first = slice(0, starts[1])
    total0 = offsets[0] + spread(
        jnp.concatenate([from1, side_by_side(from2[first], from3[first])], axis=1), pools[0][...]
    )

    arrived(0)
    maps = helds[0][...]
    shrunk = jnp.dot(maps, pools[0][...], preferred_element_type=F32)
    near = (shrunk[:, :256] * 0.25).astype(BF16)
    far = (shrunk[:, 256:] * jnp.where(lane < 64, 0.0625, 0.015625)).astype(BF16)
    total1 = total1 + product(mix, one, 0, near)
    down0 = product(mix, slice(starts[2], total), 0, far)
    total2 = total2 + down0[: starts[3] - starts[2]]
    total3 = total3 + turned(tail3 + down0[starts[3] - starts[2] :], -64)
    total0 = jnp.maximum(total0 + maps.astype(F32), 0.0)
    lines = [total0[:, at : at + LANES] for at in range(0, total0.shape[1], LANES)]
    outs[0][...] = jnp.stack(lines, axis=1).astype(BF16)
    for out, value in zip(outs[1:], (total1, total2, total3)):
        out[...] = jnp.maximum(value, 0.0).T[: out.shape[0]].astype(BF16)


HELD_SHAPES = ((48, 1024), (96, 256), (192, 128), (48, 128))


def front(section, kernels, biases, join_weight, join_bias):
    anywhere = pl.BlockSpec(memory_space=pl.ANY)
    vmem = pl.BlockSpec(memory_space=pltpu.VMEM)

    def field(b, tiles):
        return (WIDTH << b, tiles[b] * LANES)

    scratch = [pltpu.VMEM(shape, BF16) for shape in HELD_SHAPES]
    scratch += [pltpu.VMEM(join_weight.shape, BF16), pltpu.VMEM(join_bias.shape, F32)]
    scratch += [pltpu.VMEM(shape, BF16) for shape in ((1024, 384), (256, 128), (128, 128))]
    scratch += [
        pltpu.VMEM((WIDTH, TH * TW // 2), BF16),
        pltpu.VMEM(kernels.shape, BF16),
        pltpu.VMEM(biases.shape, F32),
    ]
    scratch += [pltpu.VMEM(field(b, FIELD_TILES), BF16) for b in range(4)]
    scratch += [pltpu.VMEM((2, *field(b, FIELD_TILES)), BF16) for b in range(4)]
    scratch += [pltpu.VMEM((2, 96, LANES), BF16), pltpu.VMEM((8, 96, LANES), BF16)]
    scratch += [pltpu.VMEM((2, *field(b, HIDDEN_TILES)), BF16) for b in range(4)]
    scratch += [pltpu.VMEM(field(b, HIDDEN_TILES), BF16) for b in range(4)]
    scratch += [pltpu.VMEM(field(b, OWN_TILES), BF16) for b in range(3)]
    scratch += [pltpu.VMEM((STRIPS, WIDTH, LANES), BF16)]
    pieces = ((48, 256), (96, 128), (96, 128), (48, 128))
    scratch += [pltpu.VMEM((RELAYS, *piece), BF16) for piece in pieces]
    counts = ((6,), (8,), (8,), (2, 3), (2, 3), (16 + RELAYS,), (4,), (RELAYS,), (4,))
    scratch += [pltpu.SemaphoreType.DMA(count) for count in counts]
    return pl.pallas_call(
        front_kernel,
        out_shape=[pltpu.VMEM(shape, BF16) for shape in OUT_SHAPES],
        in_specs=[anywhere] * 5,
        out_specs=[vmem] * 4,
        scratch_shapes=scratch,
        compiler_params=pltpu.CompilerParams(
            collective_id=0, has_side_effects=True, vmem_limit_bytes=VMEM_LIMIT
        ),
        name="front",
    )(
        *(
            pltpu.with_memory_space_constraint(array, pltpu.HBM)
            for array in (section, kernels, biases, join_weight, join_bias)
        )
    )


OUT_SHAPES = ((48, 8, 128), (256, 96), (64, 192), (16, 384))
VMEM_LIMIT = 48 << 20


def finish_kernel(*refs):
    sources, targets, sem = refs[:4], refs[4:8], refs[8]
    copies = [
        pltpu.make_async_copy(source, target, sem.at[at])
        for at, (source, target) in enumerate(zip(sources, targets))
    ]
    for copy in copies:
        copy.start()
    for copy in copies:
        copy.wait()


def finished(outs):
    return pl.pallas_call(
        finish_kernel,
        out_shape=[jax.ShapeDtypeStruct(out.shape, out.dtype) for out in outs],
        in_specs=[pl.BlockSpec(memory_space=pltpu.VMEM)] * 4,
        out_specs=[pl.BlockSpec(memory_space=pl.ANY)] * 4,
        scratch_shapes=[pltpu.SemaphoreType.DMA((4,))],
        compiler_params=pltpu.CompilerParams(vmem_limit_bytes=1 << 20),
        name="finish",
    )(*outs)


def local(section_in, conv_weight, conv_bias, join_weight, join_bias):
    outs = finished(
        front(section_in[0, 0, 0], conv_weight[0], conv_bias[0], join_weight, join_bias)
    )
    shapes = [(WIDTH << b, (TH >> b) // STRIPS, TW >> b) for b in range(4)]
    return tuple(
        out if out.ndim == 3 else out.reshape(*shape[1:], shape[0]).transpose(2, 0, 1)
        for out, shape in zip(outs, shapes)
    )


def solution(mesh):
    in_specs = (
        P("branch", "row", "col", None, None),
        P("branch", None, None, None, None, None),
        P("branch", None, None),
        P(),
        P(),
    )
    out_specs = (P(None, ("branch", "row"), "col"),) * 4
    return jax.shard_map(local, mesh=mesh, in_specs=in_specs, out_specs=out_specs, check_vma=False)
```

```python
from functools import partial

import jax
import jax.numpy as jnp
from jax import lax
from jax.experimental import pallas as pl
from jax.experimental.pallas import tpu as pltpu
from jax.sharding import PartitionSpec as P

WIDTH = 48
TH = 32
TW = 128
LANES = 128
STRIPS = 4
MESH = pl.DeviceIdType.MESH
WAYS = [(dr, dc) for dr in (-1, 0, 1) for dc in (-1, 0, 1) if dr or dc]
F32 = jnp.float32
BF16 = jnp.bfloat16

OWN_TILES = (32, 8, 2, 1)
BEFORE = (2, 1, 1, 0)
FIELD_TILES = (36, 10, 4, 1)
HIDDEN_TILES = (34, 10, 4, 1)
HIDDEN_START = (1, 0, 0, 0)


CHUNKS = (4, 2, 2, 1)
RELAYS = 12


def route(source, tile, strip, chunk):
    if tile == source or strip == tile or source == 3:
        return None
    if source == 0 and strip == 3 - tile and chunk % 2 == 0:
        return None
    return strip


def relayed(source, place):
    pieces = [
        (tile, strip, chunk)
        for chunk in range(CHUNKS[source])
        for tile in range(STRIPS)
        for strip in range(STRIPS)
        if tile != place and route(source, tile, strip, chunk) == place
    ]
    return sorted(
        pieces,
        key=lambda p: (
            source == 0 and halo_bound(*p[1:]),
            p[2],
            (p[0] ^ place).bit_count(),
            -abs(p[0] - source),
        ),
    )


def halo_bound(strip, chunk):
    return (strip, chunk) in ((0, 0), (STRIPS - 1, CHUNKS[0] - 1))


def own_pieces(source, place):
    chunks = range(CHUNKS[source])
    if source == place:
        return [(place ^ turn, chunk) for turn in (0, 1, 2, 3) for chunk in chunks]
    return [(place ^ turn, chunk) for chunk in chunks for turn in (1, 2, 0, 3)]


def lane_index(width=LANES):
    return lax.broadcasted_iota(jnp.int32, (1, width), 1)


def turned(group, shift):
    shift = shift % LANES
    return pltpu.roll(group, shift, 1) if shift else group


def tiles_turned(field, shift):
    if shift % LANES == 0:
        return field
    tiles = [turned(field[:, t : t + LANES], shift) for t in range(0, field.shape[1], LANES)]
    return tiles[0] if len(tiles) == 1 else jnp.concatenate(tiles, axis=1)


def natural_tile(branch_level, container_ref):
    pixels = TH * TW >> 2 * branch_level
    channels = WIDTH << branch_level
    parts = []
    for part in range(1 << branch_level):
        at = part * pixels
        low = at // LANES * LANES
        piece = container_ref[:, low : low + max(pixels, LANES)]
        if at > low:
            piece = pltpu.roll(piece.astype(F32), LANES - at + low, 1).astype(BF16)
        parts.append(piece)
    held = lax.broadcasted_iota(jnp.int32, (1, channels), 1)
    part = sum((held >= WIDTH * turn).astype(jnp.int32) for turn in range(1, 1 << branch_level))
    home = ((held - WIDTH * part) << branch_level) + part
    order = jnp.where(lax.broadcasted_iota(jnp.int32, (channels, channels), 0) == home, 1.0, 0.0)
    return jnp.dot(
        order.astype(BF16), jnp.concatenate(parts, axis=0), preferred_element_type=F32
    ).astype(BF16)


def column_stack(branch_level, own, west, east):
    cols = TW >> branch_level
    col = lane_index(own.shape[1]) & (cols - 1)
    own32 = own.astype(F32)
    minus = tiles_turned(
        jnp.where(col == cols - 1, tiles_turned(west.astype(F32), -cols), own32), 1
    ).astype(BF16)
    plus = tiles_turned(
        jnp.where(col == 0, tiles_turned(east.astype(F32), cols), own32), -1
    ).astype(BF16)

    def zeros(rows):
        return jnp.zeros((rows, own.shape[1]), BF16)

    if branch_level == 0:
        pieces = [minus, own, zeros(32), plus, zeros(80)]
    elif branch_level == 3:
        pieces = [minus, own, plus]
    else:
        pad = zeros(-own.shape[0] % LANES)
        pieces = [minus, pad, own, pad, plus, pad]
    return jnp.concatenate(pieces, axis=0)


def taps(branch_level, weights, layer):
    channels = WIDTH << branch_level
    width = -(-channels // LANES) * LANES
    lines = []
    for dy in range(3):
        if branch_level == 0:
            first, middle, last = (weights[layer, dy, dx, 0:channels, 0:width] for dx in range(3))
            pair = jnp.where(
                lane_index() < channels,
                first.astype(F32),
                pltpu.roll(middle.astype(F32), channels, 1),
            )
            lines.append(jnp.concatenate([pair.astype(BF16), last], axis=1))
        else:
            lines.append(
                jnp.concatenate(
                    [weights[layer, dy, dx, 0:channels, 0:width] for dx in range(3)], axis=1
                )
            )
    return jnp.concatenate(lines, axis=0)


def row_sum(branch_level, products, first, count):
    channels = products.shape[0] // 3
    cols = TW >> branch_level
    above, here, below = (products[d * channels : (d + 1) * channels] for d in range(3))
    span = slice(first * LANES, (first + count) * LANES)
    if cols == LANES:
        return (
            above[:, (first - 1) * LANES : (first - 1 + count) * LANES]
            + here[:, span]
            + below[:, (first + 1) * LANES : (first + 1 + count) * LANES]
        )
    last = products.shape[1] // LANES - 1
    above, below = tiles_turned(above, cols), tiles_turned(below, -cols)
    lane = lane_index()

    def tile(field, t):
        t = min(max(t, 0), last)
        return field[:, t * LANES : (t + 1) * LANES]

    tiles = [
        jnp.where(lane < cols, tile(above, t - 1), tile(above, t))
        + tile(here, t)
        + jnp.where(lane >= LANES - cols, tile(below, t + 1), tile(below, t))
        for t in range(first, first + count)
    ]
    return tiles[0] if count == 1 else jnp.concatenate(tiles, axis=1)


def front_kernel(
    section, kernels, biases, join_weight, join_bias, out0, out1, out2, out3,
    held0, held1, held2, held3, mix, mix_bias, pool0, pool1, pool2,
    container, weights, bias, own0, own1, own2, own3, side0, side1, side2, side3,
    pack_send, pack_recv, hide0, hide1, hide2, hide3, hid0, hid1, hid2, hid3,
    settled0, settled1, settled2, settled3, relay0, relay1, relay2, relay3, load_sem,
    halo_send, halo_recv, hidden_send, hidden_recv, strip_send, strip_recv, relay_recv, own_sem,
):
    level = lax.axis_index("branch")
    place = lax.axis_index("row")
    col = lax.axis_index("col")
    row_count = lax.axis_size("row")
    col_count = lax.axis_size("col")

    def reach(dr, dc):
        there = jnp.bool_(True)
        if dr:
            there = (place + dr >= 0) & (place + dr < row_count)
        if dc:
            sideways = (col + dc >= 0) & (col + dc < col_count)
            there = there & sideways if dr else sideways
        device = (
            level,
            lax.rem(place + dr + row_count, row_count),
            lax.rem(col + dc + col_count, col_count),
        )
        return there, device

    barrier = pltpu.get_barrier_semaphore()
    expected = 0
    for dr, dc in WAYS:
        there, device = reach(dr, dc)
        expected = expected + there.astype(jnp.int32)

        @pl.when(there)
        def _():
            pl.semaphore_signal(barrier, inc=1, device_id=device, device_id_type=MESH)

    at_home = level == place
    for step in range(1, STRIPS):
        for device in (
            (level, lax.rem(place + step, STRIPS), col),
            (lax.rem(level + step, STRIPS), place, col),
        ):
            pl.semaphore_signal(barrier, inc=1, device_id=device, device_id_type=MESH)

    @pl.when((level > 0) & (place == STRIPS - 1 - level))
    def _():
        pl.semaphore_signal(barrier, inc=1, device_id=(0, level, col), device_id_type=MESH)

    @pl.when(jnp.logical_not(at_home & (level == 3)))
    def _():
        pl.semaphore_signal(barrier, inc=1, device_id=(3, level, col), device_id_type=MESH)

    expected = expected + jnp.where(level == 3, STRIPS - at_home.astype(jnp.int32), 0)
    expected = expected + 2 * (STRIPS - 1) + ((level == 0) & (place > 0)).astype(jnp.int32)

    helds = (held0, held1, held2, held3)
    owns = (own0, own1, own2, own3)
    sides = (side0, side1, side2, side3)
    hides = (hide0, hide1, hide2, hide3)
    hids = (hid0, hid1, hid2, hid3)
    settleds = (settled0, settled1, settled2, settled3)
    relays = (relay0, relay1, relay2, relay3)

    mix_loads = [
        pltpu.make_async_copy(join_weight, mix, load_sem.at[4]),
        pltpu.make_async_copy(join_bias, mix_bias, load_sem.at[5]),
    ]

    def branch(b):
        channels = WIDTH << b
        width = -(-channels // LANES) * LANES
        pixels = TH * TW >> b
        cols, rows = TW >> b, TH >> b
        own, side, hide, hid = owns[b], sides[b], hides[b], hids[b]
        settled, held, relay = settleds[b], helds[b], relays[b]
        before, tiles = BEFORE[b], OWN_TILES[b]
        middle = slice(before * LANES, (before + tiles) * LANES)
        packed = b >= 2
        folds = channels // 96
        pair = 2 * cols
        chunks = CHUNKS[b]
        lane = lane_index()
        order = [way for way in WAYS if way[0]] + [way for way in WAYS if not way[0]]

        load = pltpu.make_async_copy(
            section.at[:, 0:pixels],
            own.at[:, middle] if b == 0 else container.at[:, 0:pixels],
            load_sem.at[0],
        )
        bias_load = pltpu.make_async_copy(biases, bias, load_sem.at[1])
        weight_loads = [
            pltpu.make_async_copy(
                kernels.at[layer, :, :, 0:channels, 0:width],
                weights.at[layer, :, :, 0:channels, 0:width],
                load_sem.at[2 + layer],
            )
            for layer in range(2)
        ]

        def begin():
            for copy in (load, bias_load, *weight_loads, *mix_loads):
                copy.start()

        def halo_region(dr, dc):
            if packed and dr:
                return pack_recv.at[WAYS.index((dr, dc))]
            target = own if dc == 0 else side.at[0 if dc == 1 else 1]
            if dr == 0:
                return target.at[:, middle]
            if dr == 1:
                return target.at[:, 0 : before * LANES]
            return target.at[:, (before + tiles) * LANES : (before + tiles + before) * LANES]

        def halo_source(dr):
            if dr == 0:
                return own.at[:, middle]
            if packed:
                return pack_send.at[0 if dr == -1 else 1]
            first = before if dr == -1 else tiles
            return own.at[:, first * LANES : (first + before) * LANES]

        def halo_copy(dr, dc):
            way = WAYS.index((dr, dc))
            return pltpu.make_async_remote_copy(
                src_ref=halo_source(dr),
                dst_ref=halo_region(dr, dc),
                send_sem=halo_send.at[way],
                recv_sem=halo_recv.at[way],
                device_id=reach(dr, dc)[1],
                device_id_type=MESH,
            )

        last = HIDDEN_TILES[b]
        if b < 2:
            hidden_parts = ((2, last - 2), (0, 2), (last - 2, last))
        else:
            hidden_parts = ((0, last),)

        def hidden_copy(dc, part):
            at = 0 if dc == 1 else 1
            low, high = hidden_parts[part]
            span = slice(low * LANES, high * LANES)
            return pltpu.make_async_remote_copy(
                src_ref=hid.at[:, span],
                dst_ref=hide.at[at, :, span],
                send_sem=hidden_send.at[at, part],
                recv_sem=hidden_recv.at[at, part],
                device_id=reach(0, dc)[1],
                device_id_type=MESH,
            )

        def hidden_start(*parts):
            for part in parts:
                for dc in (1, -1):
                    pl.when(reach(0, dc)[0])(hidden_copy(dc, part).start)

        def hidden_wait(*parts):
            for part in parts:
                for dc in (1, -1):
                    pl.when(reach(0, -dc)[0])(hidden_copy(dc, part).wait_recv)

        def bias_columns():
            bias_load.wait()
            return [
                jnp.broadcast_to(bias[layer : layer + 1, :], (8, bias.shape[1])).T[:channels, 0:1]
                for layer in range(2)
            ]

        def convolved(layer, fields, first, count):
            products = jnp.dot(
                taps(b, weights, layer), column_stack(b, *fields), preferred_element_type=F32
            )
            return row_sum(b, products, first, count)

        def settle_hidden(raw, offset, first):
            count = raw.shape[1] // LANES
            row = lax.shift_right_logical(lane_index(count * LANES), cols.bit_length() - 1)
            if b == 3:
                row = jnp.where(row >= 6, row - 8, row)
            else:
                row = row + (first + HIDDEN_START[b] - before) * (LANES // cols)
            low = jnp.where(place == 0, 0, -LANES)
            high = jnp.where(place == row_count - 1, rows, 2 * LANES)
            hidden = jnp.where((row >= low) & (row < high), jnp.maximum(raw + offset, 0.0), 0.0)
            hid[:, first * LANES : (first + count) * LANES] = hidden.astype(BF16)

        def hidden_tiles(offset, first, count):
            low = max(first + HIDDEN_START[b] - 1, 0)
            high = min(first + HIDDEN_START[b] + count + 1, FIELD_TILES[b])
            span = slice(low * LANES, high * LANES)
            fields = (own[:, span], side[0, :, span], side[1, :, span])
            start = first + HIDDEN_START[b] - low
            settle_hidden(convolved(0, fields, start, count), offset, first)

        def settled_tiles(offset, first, count):
            span = slice(first * LANES, (first + count + 2) * LANES)
            fields = (hid[:, span], hide[0, :, span], hide[1, :, span])
            after = convolved(1, fields, 1, count)
            kept = own[:, (before + first) * LANES : (before + first + count) * LANES]
            final = jnp.maximum(after + offset + kept.astype(F32), 0.0)
            settled[:, first * LANES : (first + count) * LANES] = final.astype(BF16)

        def ends(strip, chunk):
            if b == 3:
                return settled.at[strip], held
            if b == 2:
                size = channels // chunks
                span = slice(chunk * size, (chunk + 1) * size)
                tile = strip // 2
                return settled.at[span, tile * LANES : (tile + 1) * LANES], held.at[span]
            size = tiles * LANES // STRIPS // chunks
            at = (strip * chunks + chunk) * size
            return settled.at[:, at : at + size], held.at[:, chunk * size : (chunk + 1) * size]

        def exchange(here, wanted=None, handing=False, closing=False):
            count = 0

            def send(source, target, arrived, device, act=True):
                nonlocal count
                copy = pltpu.make_async_remote_copy(
                    src_ref=source,
                    dst_ref=target,
                    send_sem=strip_send.at[count],
                    recv_sem=arrived,
                    device_id=device,
                    device_id_type=MESH,
                )
                count += 1
                if closing:
                    copy.wait_send()
                elif act:
                    copy.start()

            at_once = []
            for strip, chunk in own_pieces(b, here):
                source, target = ends(strip, chunk)
                act = not closing and wanted(strip, chunk)
                if here == b and strip == here:
                    copy = pltpu.make_async_copy(source, target, own_sem.at[chunk])
                    if act:
                        copy.start()
                    if handing:
                        at_once.append(copy)
                    continue
                via = route(b, here, strip, chunk)
                if via is None:
                    send(source, target, strip_recv.at[b], (here, strip, col), act)
                else:
                    slot = relayed(b, via).index((here, strip, chunk))
                    send(source, relay.at[slot], relay_recv.at[slot], (b, via, col), act)
            if not handing and not closing:
                return
            for slot, (tile, strip, chunk) in enumerate(relayed(b, here)):
                piece = relay.at[slot]
                if not closing:
                    pltpu.make_async_remote_copy(
                        src_ref=piece,
                        dst_ref=piece,
                        send_sem=strip_send.at[0],
                        recv_sem=relay_recv.at[slot],
                        device_id=(b, tile, col),
                        device_id_type=MESH,
                    ).wait_recv()
                send(piece, ends(strip, chunk)[1], strip_recv.at[b], (tile, strip, col))
            for copy in at_once:
                copy.wait()

        def open_halo():
            load.wait()
            if b:
                own[:, middle] = natural_tile(b, container)
            if packed:
                for end in range(2):
                    tile = before if end == 0 else before + tiles - 1
                    at = 0 if end == 0 else (rows - 2) * cols % LANES
                    edge = own[:, tile * LANES : (tile + 1) * LANES].astype(F32)
                    out = None
                    for g in range(folds):
                        part = turned(edge[g * 96 : (g + 1) * 96], pair * g - at)
                        out = part if g == 0 else jnp.where(lane < pair * g, out, part)
                    pack_send[end] = out.astype(BF16)

            pl.semaphore_wait(barrier, expected)
            for dr, dc in order:
                pl.when(reach(dr, dc)[0])(halo_copy(dr, dc).start)
            for dr, dc in order:

                @pl.when(jnp.logical_not(reach(-dr, -dc)[0]))
                def _():
                    region = halo_region(dr, dc)
                    region[...] = jnp.zeros(region.shape, BF16)

            for dc in (1, -1):

                @pl.when(jnp.logical_not(reach(0, -dc)[0]))
                def _():
                    at = 0 if dc == 1 else 1
                    hide[at] = jnp.zeros(hid.shape, BF16)

        def run():
            def halo_wait(ways):
                for dr, dc in ways:
                    pl.when(reach(-dr, -dc)[0])(halo_copy(dr, dc).wait_recv)

            def leave(wanted, **how):
                for here in range(STRIPS):
                    pl.when(place == here)(partial(exchange, here, wanted, **how))

            offsets = bias_columns()
            weight_loads[0].wait()
            def anything(strip, chunk):
                return True

            if not packed:
                halo_wait([way for way in order if not way[0]])
                hidden_tiles(offsets[0], 2, last - 4)
                hidden_start(0)
                if b == 0:
                    weight_loads[1].wait()
                    hidden_wait(0)
                    settled_tiles(offsets[1], 2, tiles - 4)
                    leave(lambda strip, chunk: not halo_bound(strip, chunk))
                halo_wait([way for way in order if way[0]])
                hidden_tiles(offsets[0], 0, 2)
                hidden_tiles(offsets[0], last - 2, 2)
                hidden_start(1, 2)
                if b == 0:
                    hidden_wait(1, 2)
                    settled_tiles(offsets[1], 0, 2)
                    settled_tiles(offsets[1], tiles - 2, 2)
                    leave(halo_bound, handing=True)
                else:
                    weight_loads[1].wait()
                    hidden_wait(0, 1, 2)
                    settled_tiles(offsets[1], 0, tiles)
                    leave(anything, handing=True)
                return

            halo_wait(order)
            fields = []
            for target, dc in ((own, 0), (side.at[0], 1), (side.at[1], -1)):
                upper = pack_recv[WAYS.index((1, dc))].astype(F32)
                lower = pack_recv[WAYS.index((-1, dc))].astype(F32)
                lines = []
                for g in range(folds):
                    here = target[g * 96 : (g + 1) * 96, middle]
                    above = turned(upper, LANES - pair - pair * g)
                    if b == 3:
                        ring = jnp.where(lane < 96, turned(lower, 64 - pair * g), above)
                        lines.append(jnp.where(lane < 64, here.astype(F32), ring).astype(BF16))
                    else:
                        below = turned(lower, -pair * g)
                        lines.append(
                            jnp.concatenate([above.astype(BF16), here, below.astype(BF16)], axis=1)
                        )
                fields.append(jnp.concatenate(lines, axis=0))
            settle_hidden(convolved(0, fields, 0, last), offsets[0], 0)
            hidden_start(0)
            weight_loads[1].wait()
            hidden_wait(0)
            after = convolved(1, (hid[...], hide[0], hide[1]), before, tiles)
            final = jnp.maximum(after + offsets[1] + own[:, middle].astype(F32), 0.0)
            if b < 3:
                settled[...] = final.astype(BF16)
            else:
                for strip in range(STRIPS):
                    out = None
                    for g in range(8):
                        part = turned(final[g * WIDTH : (g + 1) * WIDTH], 16 * g - 16 * strip)
                        out = part if g == 0 else jnp.where(lane < 16 * g, out, part)
                    settled[strip] = out.astype(BF16)

            leave(anything, handing=True)

        def close():
            for here in range(STRIPS):
                pl.when(place == here)(partial(exchange, here, closing=True))
            for dr, dc in order:
                pl.when(reach(dr, dc)[0])(halo_copy(dr, dc).wait_send)
            for part in range(len(hidden_parts)):
                for dc in (1, -1):
                    pl.when(reach(0, dc)[0])(hidden_copy(dc, part).wait_send)

        return begin, open_halo, run, close

    branches = [branch(b) for b in range(STRIPS)]
    for b, (begin, _, _, _) in enumerate(branches):
        pl.when(level == b)(begin)
    for b, (_, open_halo, _, _) in enumerate(branches):
        pl.when(level == b)(open_halo)

    pool_refs = (pool0, pool1, pool2)
    for fine, pool in enumerate(pool_refs):
        pool[...] = pool_table(fine)

    for b, (_, _, run, _) in enumerate(branches):
        pl.when(level == b)(run)

    for copy in mix_loads:
        copy.wait()

    def arrived(source):
        arrival = pltpu.make_async_remote_copy(
            src_ref=helds[source],
            dst_ref=helds[source],
            send_sem=strip_send.at[0],
            recv_sem=strip_recv.at[source],
            device_id=(source, level, col),
            device_id_type=MESH,
        )
        pl.when(jnp.logical_not(at_home & (level == source)))(arrival.wait_recv)

    for late3 in (True, False):

        @pl.when((level < 2) if late3 else (level >= 2))
        def _():
            outs = (out0, out1, out2, out3)
            join(late3, place, arrived, helds, mix, mix_bias, pool_refs, outs)

    for b, (_, _, _, close) in enumerate(branches):
        pl.when(level == b)(close)


def coarse_home(fine_level, coarse_level):
    fine_cols, coarse_cols = TW >> fine_level, TW >> coarse_level
    shift = coarse_level - fine_level
    pixel = lax.broadcasted_iota(jnp.int32, (strip_pixels(fine_level), 1), 0)
    row = lax.shift_right_logical(pixel, fine_cols.bit_length() - 1 + shift)
    return row * coarse_cols + lax.shift_right_logical(pixel & (fine_cols - 1), shift)


def strip_pixels(branch_level):
    return TH * TW // STRIPS >> 2 * branch_level


def pool_table(fine_level):
    at = 0
    hits = []
    for coarse_level in range(fine_level + 1, STRIPS):
        hits.append((at, at + coarse_home(fine_level, coarse_level)))
        at += strip_pixels(coarse_level)
    tiles = []
    for tile in range(-(-at // LANES)):
        target = lane_index() + tile * LANES
        hit = None
        for first, home in hits:
            same = home == target
            hit = same if hit is None else hit | same
        tiles.append(jnp.where(hit, 1.0, 0.0).astype(BF16))
    table = tiles[0] if len(tiles) == 1 else jnp.concatenate(tiles, axis=1)
    short = max(LANES - table.shape[0], 0)
    if short:
        table = jnp.concatenate([table, jnp.zeros((short, table.shape[1]), BF16)], axis=0)
    return table


def product(mix, rows, source, data):
    start = ((1 << source) - 1) * WIDTH
    stop = start + data.shape[0]
    low = start // LANES * LANES
    high = min(-(-stop // LANES) * LANES, mix.shape[1])
    pieces = [data]
    if start > low:
        pieces.insert(0, jnp.zeros((start - low, data.shape[1]), BF16))
    if high > stop:
        pieces.append(jnp.zeros((high - stop, data.shape[1]), BF16))
    stacked = jnp.concatenate(pieces, axis=0)
    return jnp.dot(
        mix[rows, low:high], stacked, preferred_element_type=F32
    ).astype(BF16).astype(F32)


def spread(term, pool):
    return lax.dot_general(
        term.astype(BF16), pool, (((1,), (1,)), ((), ())), preferred_element_type=F32
    )


def join(late3, place, arrived, helds, mix, mix_bias, pools, outs):
    lane = lane_index()
    total = mix_bias.shape[0]
    line = jnp.concatenate([mix_bias[...][None, :], jnp.zeros((1, -total % LANES), F32)], axis=1)
    offset = jnp.broadcast_to(line, (8, line.shape[1])).T
    starts = [((1 << b) - 1) * WIDTH for b in range(STRIPS + 1)]
    offsets = [offset[starts[b] : starts[b + 1], 0:1] for b in range(STRIPS)]
    one, two, three = (slice(starts[b], starts[b + 1]) for b in range(1, STRIPS))

    def side_by_side(near, far):
        return jnp.where(lane < 64, near, jnp.where(lane < 80, turned(far, 64), 0.0))

    def take3():
        arrived(3)
        folded = helds[3][...].astype(F32)
        last = jnp.concatenate([turned(folded, -16 * g) for g in range(8)], axis=0)
        return last, product(mix, slice(0, starts[3]), 3, last.astype(BF16))

    first = slice(0, starts[1])
    if not late3:
        last, from3 = take3()

    arrived(2)
    pieces = helds[2][...].astype(F32)
    third = jnp.where(lax.rem(place, 2) == 1, turned(pieces, 64), pieces)
    third16 = third.astype(BF16)
    from2 = product(mix, slice(0, starts[2]), 2, third16)
    shrunk = jnp.dot(third16, pools[2][...], preferred_element_type=F32)
    total3 = offsets[3] + product(mix, three, 2, (shrunk * 0.25).astype(BF16))
    total2 = third + offsets[2]

    arrived(1)
    second = helds[1][...]
    from1 = product(mix, slice(0, starts[1]), 1, second)
    shrunk = jnp.dot(second, pools[1][...], preferred_element_type=F32)
    shrunk = shrunk * jnp.where(lane < 64, 0.25, 0.0625)
    down1 = product(mix, slice(starts[2], total), 1, shrunk.astype(BF16))
    total2 = total2 + down1[: starts[3] - starts[2]]
    tail3 = down1[starts[3] - starts[2] :]
    total1 = second.astype(F32) + offsets[1]

    def add3(total0, total1, total2, total3, far0, far1):
        return (
            total0 + spread(far0, pools[0][...]),
            total1 + spread(far1, pools[1][...]),
            total2 + spread(from3[two], pools[2][...]),
            total3 + last,
        )

    if late3:
        nothing = jnp.zeros((1, LANES), F32)
        near0 = jnp.concatenate([from1, side_by_side(from2[first], nothing)], axis=1)
        total0 = offsets[0] + spread(near0, pools[0][...])
        total1 = total1 + spread(side_by_side(from2[one], nothing), pools[1][...])
    else:
        far0 = jnp.concatenate([from1, side_by_side(from2[first], from3[first])], axis=1)
        far1 = side_by_side(from2[one], from3[one])
        total0, total1, total2, total3 = add3(offsets[0], total1, total2, total3, far0, far1)

    arrived(0)
    maps = helds[0][...]
    shrunk = jnp.dot(maps, pools[0][...], preferred_element_type=F32)
    near = (shrunk[:, :256] * 0.25).astype(BF16)
    far = (shrunk[:, 256:] * jnp.where(lane < 64, 0.0625, 0.015625)).astype(BF16)
    total1 = total1 + product(mix, one, 0, near)
    down0 = product(mix, slice(starts[2], total), 0, far)
    total2 = total2 + down0[: starts[3] - starts[2]]
    total3 = total3 + turned(tail3 + down0[starts[3] - starts[2] :], -64)
    if late3:
        last, from3 = take3()
        apart = jnp.where((lane >= 64) & (lane < 80), turned(from3[: starts[2]], 64), 0.0)
        total0 = total0 + spread(apart[first], pools[0][:, 256:])
        total1 = total1 + spread(apart[one], pools[1][...])
        total2 = total2 + spread(from3[two], pools[2][...])
        total3 = total3 + last
    total0 = jnp.maximum(total0 + maps.astype(F32), 0.0)
    lines = [total0[:, at : at + LANES] for at in range(0, total0.shape[1], LANES)]
    outs[0][...] = jnp.stack(lines, axis=1).astype(BF16)
    for out, value in zip(outs[1:], (total1, total2, total3)):
        out[...] = jnp.maximum(value, 0.0).T[: out.shape[0]].astype(BF16)


HELD_SHAPES = ((48, 1024), (96, 256), (192, 128), (48, 128))


def front(section, kernels, biases, join_weight, join_bias):
    anywhere = pl.BlockSpec(memory_space=pl.ANY)
    vmem = pl.BlockSpec(memory_space=pltpu.VMEM)

    def field(b, tiles):
        return (WIDTH << b, tiles[b] * LANES)

    scratch = [pltpu.VMEM(shape, BF16) for shape in HELD_SHAPES]
    scratch += [pltpu.VMEM(join_weight.shape, BF16), pltpu.VMEM(join_bias.shape, F32)]
    scratch += [pltpu.VMEM(shape, BF16) for shape in ((1024, 384), (256, 128), (128, 128))]
    scratch += [
        pltpu.VMEM((WIDTH, TH * TW // 2), BF16),
        pltpu.VMEM(kernels.shape, BF16),
        pltpu.VMEM(biases.shape, F32),
    ]
    scratch += [pltpu.VMEM(field(b, FIELD_TILES), BF16) for b in range(4)]
    scratch += [pltpu.VMEM((2, *field(b, FIELD_TILES)), BF16) for b in range(4)]
    scratch += [pltpu.VMEM((2, 96, LANES), BF16), pltpu.VMEM((8, 96, LANES), BF16)]
    scratch += [pltpu.VMEM((2, *field(b, HIDDEN_TILES)), BF16) for b in range(4)]
    scratch += [pltpu.VMEM(field(b, HIDDEN_TILES), BF16) for b in range(4)]
    scratch += [pltpu.VMEM(field(b, OWN_TILES), BF16) for b in range(3)]
    scratch += [pltpu.VMEM((STRIPS, WIDTH, LANES), BF16)]
    pieces = ((48, 256), (96, 128), (96, 128), (48, 128))
    scratch += [pltpu.VMEM((RELAYS, *piece), BF16) for piece in pieces]
    counts = ((6,), (8,), (8,), (2, 3), (2, 3), (16 + RELAYS,), (4,), (RELAYS,), (4,))
    scratch += [pltpu.SemaphoreType.DMA(count) for count in counts]
    return pl.pallas_call(
        front_kernel,
        out_shape=[pltpu.VMEM(shape, BF16) for shape in OUT_SHAPES],
        in_specs=[anywhere] * 5,
        out_specs=[vmem] * 4,
        scratch_shapes=scratch,
        compiler_params=pltpu.CompilerParams(
            collective_id=0, has_side_effects=True, vmem_limit_bytes=VMEM_LIMIT
        ),
        name="front",
    )(
        *(
            pltpu.with_memory_space_constraint(array, pltpu.HBM)
            for array in (section, kernels, biases, join_weight, join_bias)
        )
    )


OUT_SHAPES = ((48, 8, 128), (256, 96), (64, 192), (16, 384))
VMEM_LIMIT = 48 << 20


def finish_kernel(*refs):
    sources, targets, sem = refs[:4], refs[4:8], refs[8]
    copies = [
        pltpu.make_async_copy(source, target, sem.at[at])
        for at, (source, target) in enumerate(zip(sources, targets))
    ]
    for copy in copies:
        copy.start()
    for copy in copies:
        copy.wait()


def finished(outs):
    return pl.pallas_call(
        finish_kernel,
        out_shape=[jax.ShapeDtypeStruct(out.shape, out.dtype) for out in outs],
        in_specs=[pl.BlockSpec(memory_space=pltpu.VMEM)] * 4,
        out_specs=[pl.BlockSpec(memory_space=pl.ANY)] * 4,
        scratch_shapes=[pltpu.SemaphoreType.DMA((4,))],
        compiler_params=pltpu.CompilerParams(vmem_limit_bytes=1 << 20),
        name="finish",
    )(*outs)


def local(section_in, conv_weight, conv_bias, join_weight, join_bias):
    outs = finished(
        front(section_in[0, 0, 0], conv_weight[0], conv_bias[0], join_weight, join_bias)
    )
    shapes = [(WIDTH << b, (TH >> b) // STRIPS, TW >> b) for b in range(4)]
    return tuple(
        out if out.ndim == 3 else out.reshape(*shape[1:], shape[0]).transpose(2, 0, 1)
        for out, shape in zip(outs, shapes)
    )


def solution(mesh):
    in_specs = (
        P("branch", "row", "col", None, None),
        P("branch", None, None, None, None, None),
        P("branch", None, None),
        P(),
        P(),
    )
    out_specs = (P(None, ("branch", "row"), "col"),) * 4
    return jax.shard_map(local, mesh=mesh, in_specs=in_specs, out_specs=out_specs, check_vma=False)
```

```python
from functools import partial

import jax
import jax.numpy as jnp
from jax import lax
from jax.experimental import pallas as pl
from jax.experimental.pallas import tpu as pltpu
from jax.sharding import PartitionSpec as P

WIDTH = 48
TH = 32
TW = 128
LANES = 128
STRIPS = 4
MESH = pl.DeviceIdType.MESH
WAYS = [(dr, dc) for dr in (-1, 0, 1) for dc in (-1, 0, 1) if dr or dc]
F32 = jnp.float32
BF16 = jnp.bfloat16

OWN_TILES = (32, 8, 2, 1)
BEFORE = (2, 1, 1, 0)
FIELD_TILES = (36, 10, 4, 1)
HIDDEN_TILES = (34, 10, 4, 1)
HIDDEN_START = (1, 0, 0, 0)


CHUNKS = (4, 2, 1, 1)
RELAYS = 12


def route(source, tile, strip, chunk):
    if tile == source or strip == tile or source == 3:
        return None
    if source == 0 and strip == 3 - tile and (chunk % 2 == 0 or strip == 0):
        return None
    return strip


def relayed(source, place):
    pieces = [
        (tile, strip, chunk)
        for chunk in range(CHUNKS[source])
        for tile in range(STRIPS)
        for strip in range(STRIPS)
        if tile != place and route(source, tile, strip, chunk) == place
    ]
    return sorted(
        pieces,
        key=lambda p: (
            source == 0 and halo_bound(*p[1:]),
            p[2],
            (p[0] ^ place).bit_count(),
            -abs(p[0] - source),
        ),
    )


def halo_bound(strip, chunk):
    return (strip, chunk) in ((0, 0), (STRIPS - 1, CHUNKS[0] - 1))


def own_pieces(source, place):
    chunks = range(CHUNKS[source])
    if source == place:
        return [(place ^ turn, chunk) for turn in (0, 1, 2, 3) for chunk in chunks]
    return [(place ^ turn, chunk) for chunk in chunks for turn in (1, 2, 0, 3)]


def lane_index(width=LANES):
    return lax.broadcasted_iota(jnp.int32, (1, width), 1)


def turned(group, shift):
    shift = shift % LANES
    return pltpu.roll(group, shift, 1) if shift else group


def tiles_turned(field, shift):
    if shift % LANES == 0:
        return field
    tiles = [turned(field[:, t : t + LANES], shift) for t in range(0, field.shape[1], LANES)]
    return tiles[0] if len(tiles) == 1 else jnp.concatenate(tiles, axis=1)


def natural_tile(branch_level, container_ref):
    pixels = TH * TW >> 2 * branch_level
    channels = WIDTH << branch_level
    parts = []
    for part in range(1 << branch_level):
        at = part * pixels
        low = at // LANES * LANES
        piece = container_ref[:, low : low + max(pixels, LANES)]
        if at > low:
            piece = pltpu.roll(piece.astype(F32), LANES - at + low, 1).astype(BF16)
        parts.append(piece)
    held = lax.broadcasted_iota(jnp.int32, (1, channels), 1)
    part = sum((held >= WIDTH * turn).astype(jnp.int32) for turn in range(1, 1 << branch_level))
    home = ((held - WIDTH * part) << branch_level) + part
    order = jnp.where(lax.broadcasted_iota(jnp.int32, (channels, channels), 0) == home, 1.0, 0.0)
    return jnp.dot(
        order.astype(BF16), jnp.concatenate(parts, axis=0), preferred_element_type=F32
    ).astype(BF16)


def column_stack(branch_level, own, west, east):
    cols = TW >> branch_level
    col = lane_index(own.shape[1]) & (cols - 1)
    own32 = own.astype(F32)
    minus = tiles_turned(
        jnp.where(col == cols - 1, tiles_turned(west.astype(F32), -cols), own32), 1
    ).astype(BF16)
    plus = tiles_turned(
        jnp.where(col == 0, tiles_turned(east.astype(F32), cols), own32), -1
    ).astype(BF16)

    def zeros(rows):
        return jnp.zeros((rows, own.shape[1]), BF16)

    if branch_level == 0:
        pieces = [minus, own, zeros(32), plus, zeros(80)]
    elif branch_level == 3:
        pieces = [minus, own, plus]
    else:
        pad = zeros(-own.shape[0] % LANES)
        pieces = [minus, pad, own, pad, plus, pad]
    return jnp.concatenate(pieces, axis=0)


def taps(branch_level, weights, layer):
    channels = WIDTH << branch_level
    width = -(-channels // LANES) * LANES
    lines = []
    for dy in range(3):
        if branch_level == 0:
            first, middle, last = (weights[layer, dy, dx, 0:channels, 0:width] for dx in range(3))
            pair = jnp.where(
                lane_index() < channels,
                first.astype(F32),
                pltpu.roll(middle.astype(F32), channels, 1),
            )
            lines.append(jnp.concatenate([pair.astype(BF16), last], axis=1))
        else:
            lines.append(
                jnp.concatenate(
                    [weights[layer, dy, dx, 0:channels, 0:width] for dx in range(3)], axis=1
                )
            )
    return jnp.concatenate(lines, axis=0)


def row_sum(branch_level, products, first, count):
    channels = products.shape[0] // 3
    cols = TW >> branch_level
    above, here, below = (products[d * channels : (d + 1) * channels] for d in range(3))
    span = slice(first * LANES, (first + count) * LANES)
    if cols == LANES:
        return (
            above[:, (first - 1) * LANES : (first - 1 + count) * LANES]
            + here[:, span]
            + below[:, (first + 1) * LANES : (first + 1 + count) * LANES]
        )
    last = products.shape[1] // LANES - 1
    above, below = tiles_turned(above, cols), tiles_turned(below, -cols)
    lane = lane_index()

    def tile(field, t):
        t = min(max(t, 0), last)
        return field[:, t * LANES : (t + 1) * LANES]

    tiles = [
        jnp.where(lane < cols, tile(above, t - 1), tile(above, t))
        + tile(here, t)
        + jnp.where(lane >= LANES - cols, tile(below, t + 1), tile(below, t))
        for t in range(first, first + count)
    ]
    return tiles[0] if count == 1 else jnp.concatenate(tiles, axis=1)


def front_kernel(
    section, kernels, biases, join_weight, join_bias, out0, out1, out2, out3,
    held0, held1, held2, held3, mix, mix_bias, pool0, pool1, pool2,
    container, weights, bias, own0, own1, own2, own3, side0, side1, side2, side3,
    pack_send, pack_recv, hide0, hide1, hide2, hide3, hid0, hid1, hid2, hid3,
    settled0, settled1, settled2, settled3, relay0, relay1, relay2, relay3, load_sem,
    halo_send, halo_recv, hidden_send, hidden_recv, strip_send, strip_recv, relay_recv, own_sem,
):
    level = lax.axis_index("branch")
    place = lax.axis_index("row")
    col = lax.axis_index("col")
    row_count = lax.axis_size("row")
    col_count = lax.axis_size("col")

    def reach(dr, dc):
        there = jnp.bool_(True)
        if dr:
            there = (place + dr >= 0) & (place + dr < row_count)
        if dc:
            sideways = (col + dc >= 0) & (col + dc < col_count)
            there = there & sideways if dr else sideways
        device = (
            level,
            lax.rem(place + dr + row_count, row_count),
            lax.rem(col + dc + col_count, col_count),
        )
        return there, device

    barrier = pltpu.get_barrier_semaphore()
    expected = 0
    for dr, dc in WAYS:
        there, device = reach(dr, dc)
        expected = expected + there.astype(jnp.int32)

        @pl.when(there)
        def _():
            pl.semaphore_signal(barrier, inc=1, device_id=device, device_id_type=MESH)

    at_home = level == place
    for step in range(1, STRIPS):
        for device in (
            (level, lax.rem(place + step, STRIPS), col),
            (lax.rem(level + step, STRIPS), place, col),
        ):
            pl.semaphore_signal(barrier, inc=1, device_id=device, device_id_type=MESH)

    @pl.when((level > 0) & (place == STRIPS - 1 - level))
    def _():
        pl.semaphore_signal(barrier, inc=1, device_id=(0, level, col), device_id_type=MESH)

    @pl.when(jnp.logical_not(at_home & (level == 3)))
    def _():
        pl.semaphore_signal(barrier, inc=1, device_id=(3, level, col), device_id_type=MESH)

    expected = expected + jnp.where(level == 3, STRIPS - at_home.astype(jnp.int32), 0)
    expected = expected + 2 * (STRIPS - 1) + ((level == 0) & (place > 0)).astype(jnp.int32)

    helds = (held0, held1, held2, held3)
    owns = (own0, own1, own2, own3)
    sides = (side0, side1, side2, side3)
    hides = (hide0, hide1, hide2, hide3)
    hids = (hid0, hid1, hid2, hid3)
    settleds = (settled0, settled1, settled2, settled3)
    relays = (relay0, relay1, relay2, relay3)

    mix_loads = [
        pltpu.make_async_copy(join_weight, mix, load_sem.at[4]),
        pltpu.make_async_copy(join_bias, mix_bias, load_sem.at[5]),
    ]

    def branch(b):
        channels = WIDTH << b
        width = -(-channels // LANES) * LANES
        pixels = TH * TW >> b
        cols, rows = TW >> b, TH >> b
        own, side, hide, hid = owns[b], sides[b], hides[b], hids[b]
        settled, held, relay = settleds[b], helds[b], relays[b]
        before, tiles = BEFORE[b], OWN_TILES[b]
        middle = slice(before * LANES, (before + tiles) * LANES)
        packed = b >= 2
        folds = channels // 96
        pair = 2 * cols
        chunks = CHUNKS[b]
        lane = lane_index()
        order = [way for way in WAYS if way[0]] + [way for way in WAYS if not way[0]]

        load = pltpu.make_async_copy(
            section.at[:, 0:pixels],
            own.at[:, middle] if b == 0 else container.at[:, 0:pixels],
            load_sem.at[0],
        )
        bias_load = pltpu.make_async_copy(biases, bias, load_sem.at[1])
        weight_loads = [
            pltpu.make_async_copy(
                kernels.at[layer, :, :, 0:channels, 0:width],
                weights.at[layer, :, :, 0:channels, 0:width],
                load_sem.at[2 + layer],
            )
            for layer in range(2)
        ]

        def begin():
            for copy in (load, bias_load, *weight_loads, *mix_loads):
                copy.start()

        def halo_region(dr, dc):
            if packed and dr:
                return pack_recv.at[WAYS.index((dr, dc))]
            target = own if dc == 0 else side.at[0 if dc == 1 else 1]
            if dr == 0:
                return target.at[:, middle]
            if dr == 1:
                return target.at[:, 0 : before * LANES]
            return target.at[:, (before + tiles) * LANES : (before + tiles + before) * LANES]

        def halo_source(dr):
            if dr == 0:
                return own.at[:, middle]
            if packed:
                return pack_send.at[0 if dr == -1 else 1]
            first = before if dr == -1 else tiles
            return own.at[:, first * LANES : (first + before) * LANES]

        def halo_copy(dr, dc):
            way = WAYS.index((dr, dc))
            return pltpu.make_async_remote_copy(
                src_ref=halo_source(dr),
                dst_ref=halo_region(dr, dc),
                send_sem=halo_send.at[way],
                recv_sem=halo_recv.at[way],
                device_id=reach(dr, dc)[1],
                device_id_type=MESH,
            )

        last = HIDDEN_TILES[b]
        if b < 2:
            hidden_parts = ((2, last - 2), (0, 2), (last - 2, last))
        else:
            hidden_parts = ((0, last),)

        def hidden_copy(dc, part):
            at = 0 if dc == 1 else 1
            low, high = hidden_parts[part]
            span = slice(low * LANES, high * LANES)
            return pltpu.make_async_remote_copy(
                src_ref=hid.at[:, span],
                dst_ref=hide.at[at, :, span],
                send_sem=hidden_send.at[at, part],
                recv_sem=hidden_recv.at[at, part],
                device_id=reach(0, dc)[1],
                device_id_type=MESH,
            )

        def hidden_start(*parts):
            for part in parts:
                for dc in (1, -1):
                    pl.when(reach(0, dc)[0])(hidden_copy(dc, part).start)

        def hidden_wait(*parts):
            for part in parts:
                for dc in (1, -1):
                    pl.when(reach(0, -dc)[0])(hidden_copy(dc, part).wait_recv)

        def bias_columns():
            bias_load.wait()
            return [
                jnp.broadcast_to(bias[layer : layer + 1, :], (8, bias.shape[1])).T[:channels, 0:1]
                for layer in range(2)
            ]

        def convolved(layer, fields, first, count):
            products = jnp.dot(
                taps(b, weights, layer), column_stack(b, *fields), preferred_element_type=F32
            )
            return row_sum(b, products, first, count)

        def settle_hidden(raw, offset, first):
            count = raw.shape[1] // LANES
            row = lax.shift_right_logical(lane_index(count * LANES), cols.bit_length() - 1)
            if b == 3:
                row = jnp.where(row >= 6, row - 8, row)
            else:
                row = row + (first + HIDDEN_START[b] - before) * (LANES // cols)
            low = jnp.where(place == 0, 0, -LANES)
            high = jnp.where(place == row_count - 1, rows, 2 * LANES)
            hidden = jnp.where((row >= low) & (row < high), jnp.maximum(raw + offset, 0.0), 0.0)
            hid[:, first * LANES : (first + count) * LANES] = hidden.astype(BF16)

        def hidden_tiles(offset, first, count):
            low = max(first + HIDDEN_START[b] - 1, 0)
            high = min(first + HIDDEN_START[b] + count + 1, FIELD_TILES[b])
            span = slice(low * LANES, high * LANES)
            fields = (own[:, span], side[0, :, span], side[1, :, span])
            start = first + HIDDEN_START[b] - low
            settle_hidden(convolved(0, fields, start, count), offset, first)

        def settled_tiles(offset, first, count):
            span = slice(first * LANES, (first + count + 2) * LANES)
            fields = (hid[:, span], hide[0, :, span], hide[1, :, span])
            after = convolved(1, fields, 1, count)
            kept = own[:, (before + first) * LANES : (before + first + count) * LANES]
            final = jnp.maximum(after + offset + kept.astype(F32), 0.0)
            settled[:, first * LANES : (first + count) * LANES] = final.astype(BF16)

        def ends(strip, chunk):
            if packed:
                return settled.at[strip], held
            size = tiles * LANES // STRIPS // chunks
            at = (strip * chunks + chunk) * size
            return settled.at[:, at : at + size], held.at[:, chunk * size : (chunk + 1) * size]

        def exchange(here, wanted=None, handing=False, closing=False):
            count = 0

            def send(source, target, arrived, device, act=True):
                nonlocal count
                copy = pltpu.make_async_remote_copy(
                    src_ref=source,
                    dst_ref=target,
                    send_sem=strip_send.at[count],
                    recv_sem=arrived,
                    device_id=device,
                    device_id_type=MESH,
                )
                count += 1
                if closing:
                    copy.wait_send()
                elif act:
                    copy.start()

            at_once = []
            for strip, chunk in own_pieces(b, here):
                source, target = ends(strip, chunk)
                act = not closing and wanted(strip, chunk)
                if here == b and strip == here:
                    copy = pltpu.make_async_copy(source, target, own_sem.at[chunk])
                    if act:
                        copy.start()
                    if handing:
                        at_once.append(copy)
                    continue
                via = route(b, here, strip, chunk)
                if via is None:
                    send(source, target, strip_recv.at[b], (here, strip, col), act)
                else:
                    slot = relayed(b, via).index((here, strip, chunk))
                    send(source, relay.at[slot], relay_recv.at[slot], (b, via, col), act)
            if not handing and not closing:
                return
            for slot, (tile, strip, chunk) in enumerate(relayed(b, here)):
                piece = relay.at[slot]
                if not closing:
                    pltpu.make_async_remote_copy(
                        src_ref=piece,
                        dst_ref=piece,
                        send_sem=strip_send.at[0],
                        recv_sem=relay_recv.at[slot],
                        device_id=(b, tile, col),
                        device_id_type=MESH,
                    ).wait_recv()
                send(piece, ends(strip, chunk)[1], strip_recv.at[b], (tile, strip, col))
            for copy in at_once:
                copy.wait()

        def open_halo():
            load.wait()
            if b:
                own[:, middle] = natural_tile(b, container)
            if packed:
                for end in range(2):
                    tile = before if end == 0 else before + tiles - 1
                    at = 0 if end == 0 else (rows - 2) * cols % LANES
                    edge = own[:, tile * LANES : (tile + 1) * LANES].astype(F32)
                    out = None
                    for g in range(folds):
                        part = turned(edge[g * 96 : (g + 1) * 96], pair * g - at)
                        out = part if g == 0 else jnp.where(lane < pair * g, out, part)
                    pack_send[end] = out.astype(BF16)

            pl.semaphore_wait(barrier, expected)
            for dr, dc in order:
                pl.when(reach(dr, dc)[0])(halo_copy(dr, dc).start)
            for dr, dc in order:

                @pl.when(jnp.logical_not(reach(-dr, -dc)[0]))
                def _():
                    region = halo_region(dr, dc)
                    region[...] = jnp.zeros(region.shape, BF16)

            for dc in (1, -1):

                @pl.when(jnp.logical_not(reach(0, -dc)[0]))
                def _():
                    at = 0 if dc == 1 else 1
                    hide[at] = jnp.zeros(hid.shape, BF16)

        def run():
            def halo_wait(ways):
                for dr, dc in ways:
                    pl.when(reach(-dr, -dc)[0])(halo_copy(dr, dc).wait_recv)

            def leave(wanted, **how):
                for here in range(STRIPS):
                    pl.when(place == here)(partial(exchange, here, wanted, **how))

            offsets = bias_columns()
            weight_loads[0].wait()
            def anything(strip, chunk):
                return True

            if not packed:
                halo_wait([way for way in order if not way[0]])
                hidden_tiles(offsets[0], 2, last - 4)
                hidden_start(0)
                if b == 0:
                    weight_loads[1].wait()
                    hidden_wait(0)
                    settled_tiles(offsets[1], 2, tiles - 4)
                    leave(lambda strip, chunk: not halo_bound(strip, chunk))
                halo_wait([way for way in order if way[0]])
                hidden_tiles(offsets[0], 0, 2)
                hidden_tiles(offsets[0], last - 2, 2)
                hidden_start(1, 2)
                if b == 0:
                    hidden_wait(1, 2)
                    settled_tiles(offsets[1], 0, 2)
                    settled_tiles(offsets[1], tiles - 2, 2)
                    leave(halo_bound, handing=True)
                else:
                    weight_loads[1].wait()
                    hidden_wait(0, 1, 2)
                    settled_tiles(offsets[1], 0, tiles)
                    leave(anything, handing=True)
                return

            halo_wait(order)
            fields = []
            for target, dc in ((own, 0), (side.at[0], 1), (side.at[1], -1)):
                upper = pack_recv[WAYS.index((1, dc))].astype(F32)
                lower = pack_recv[WAYS.index((-1, dc))].astype(F32)
                lines = []
                for g in range(folds):
                    here = target[g * 96 : (g + 1) * 96, middle]
                    above = turned(upper, LANES - pair - pair * g)
                    if b == 3:
                        ring = jnp.where(lane < 96, turned(lower, 64 - pair * g), above)
                        lines.append(jnp.where(lane < 64, here.astype(F32), ring).astype(BF16))
                    else:
                        below = turned(lower, -pair * g)
                        lines.append(
                            jnp.concatenate([above.astype(BF16), here, below.astype(BF16)], axis=1)
                        )
                fields.append(jnp.concatenate(lines, axis=0))
            settle_hidden(convolved(0, fields, 0, last), offsets[0], 0)
            hidden_start(0)
            weight_loads[1].wait()
            hidden_wait(0)
            after = convolved(1, (hid[...], hide[0], hide[1]), before, tiles)
            final = jnp.maximum(after + offsets[1] + own[:, middle].astype(F32), 0.0)
            size = settled.shape[1]
            pixels = strip_pixels(b)
            for strip in range(STRIPS):
                tile, at = divmod(strip * pixels, LANES)
                strip_tile = final[:, tile * LANES : (tile + 1) * LANES]
                out = None
                for g in range(LANES // pixels):
                    part = turned(strip_tile[g * size : (g + 1) * size], pixels * g - at)
                    out = part if g == 0 else jnp.where(lane < pixels * g, out, part)
                settled[strip] = out.astype(BF16)

            leave(anything, handing=True)

        def close():
            for here in range(STRIPS):
                pl.when(place == here)(partial(exchange, here, closing=True))
            for dr, dc in order:
                pl.when(reach(dr, dc)[0])(halo_copy(dr, dc).wait_send)
            for part in range(len(hidden_parts)):
                for dc in (1, -1):
                    pl.when(reach(0, dc)[0])(hidden_copy(dc, part).wait_send)

        return begin, open_halo, run, close

    branches = [branch(b) for b in range(STRIPS)]
    for b, (begin, _, _, _) in enumerate(branches):
        pl.when(level == b)(begin)
    for b, (_, open_halo, _, _) in enumerate(branches):
        pl.when(level == b)(open_halo)

    pool_refs = (pool0, pool1, pool2)
    for fine, pool in enumerate(pool_refs):
        pool[...] = pool_table(fine)

    for b, (_, _, run, _) in enumerate(branches):
        pl.when(level == b)(run)

    for copy in mix_loads:
        copy.wait()

    def arrived(source):
        arrival = pltpu.make_async_remote_copy(
            src_ref=helds[source],
            dst_ref=helds[source],
            send_sem=strip_send.at[0],
            recv_sem=strip_recv.at[source],
            device_id=(source, level, col),
            device_id_type=MESH,
        )
        pl.when(jnp.logical_not(at_home & (level == source)))(arrival.wait_recv)

    for late3 in (True, False):

        @pl.when((level < 2) if late3 else (level >= 2))
        def _():
            outs = (out0, out1, out2, out3)
            join(late3, place, arrived, helds, mix, mix_bias, pool_refs, outs)

    for b, (_, _, _, close) in enumerate(branches):
        pl.when(level == b)(close)


def coarse_home(fine_level, coarse_level):
    fine_cols, coarse_cols = TW >> fine_level, TW >> coarse_level
    shift = coarse_level - fine_level
    pixel = lax.broadcasted_iota(jnp.int32, (strip_pixels(fine_level), 1), 0)
    row = lax.shift_right_logical(pixel, fine_cols.bit_length() - 1 + shift)
    return row * coarse_cols + lax.shift_right_logical(pixel & (fine_cols - 1), shift)


def strip_pixels(branch_level):
    return TH * TW // STRIPS >> 2 * branch_level


def pool_table(fine_level):
    at = 0
    hits = []
    for coarse_level in range(fine_level + 1, STRIPS):
        hits.append((at, at + coarse_home(fine_level, coarse_level)))
        at += strip_pixels(coarse_level)
    tiles = []
    for tile in range(-(-at // LANES)):
        target = lane_index() + tile * LANES
        hit = None
        for first, home in hits:
            same = home == target
            hit = same if hit is None else hit | same
        tiles.append(jnp.where(hit, 1.0, 0.0).astype(BF16))
    table = tiles[0] if len(tiles) == 1 else jnp.concatenate(tiles, axis=1)
    short = max(LANES - table.shape[0], 0)
    if short:
        table = jnp.concatenate([table, jnp.zeros((short, table.shape[1]), BF16)], axis=0)
    return table


def product(mix, rows, source, data):
    start = ((1 << source) - 1) * WIDTH
    stop = start + data.shape[0]
    low = start // LANES * LANES
    high = min(-(-stop // LANES) * LANES, mix.shape[1])
    pieces = [data]
    if start > low:
        pieces.insert(0, jnp.zeros((start - low, data.shape[1]), BF16))
    if high > stop:
        pieces.append(jnp.zeros((high - stop, data.shape[1]), BF16))
    stacked = jnp.concatenate(pieces, axis=0)
    return jnp.dot(
        mix[rows, low:high], stacked, preferred_element_type=F32
    ).astype(BF16).astype(F32)


def spread(term, pool):
    return lax.dot_general(
        term.astype(BF16), pool, (((1,), (1,)), ((), ())), preferred_element_type=F32
    )


def join(late3, place, arrived, helds, mix, mix_bias, pools, outs):
    lane = lane_index()
    total = mix_bias.shape[0]
    line = jnp.concatenate([mix_bias[...][None, :], jnp.zeros((1, -total % LANES), F32)], axis=1)
    offset = jnp.broadcast_to(line, (8, line.shape[1])).T
    starts = [((1 << b) - 1) * WIDTH for b in range(STRIPS + 1)]
    offsets = [offset[starts[b] : starts[b + 1], 0:1] for b in range(STRIPS)]
    one, two, three = (slice(starts[b], starts[b + 1]) for b in range(1, STRIPS))

    def side_by_side(near, far):
        return jnp.where(lane < 64, near, jnp.where(lane < 80, turned(far, 64), 0.0))

    def take3():
        arrived(3)
        folded = helds[3][...].astype(F32)
        last = jnp.concatenate([turned(folded, -16 * g) for g in range(8)], axis=0)
        return last, product(mix, slice(0, starts[3]), 3, last.astype(BF16))

    first = slice(0, starts[1])
    if not late3:
        last, from3 = take3()

    arrived(2)
    pieces = helds[2][...].astype(F32)
    third = jnp.concatenate([pieces, turned(pieces, -64)], axis=0)
    third16 = third.astype(BF16)
    from2 = product(mix, slice(0, starts[2]), 2, third16)
    shrunk = jnp.dot(third16, pools[2][...], preferred_element_type=F32)
    total3 = offsets[3] + product(mix, three, 2, (shrunk * 0.25).astype(BF16))
    total2 = third + offsets[2]

    arrived(1)
    second = helds[1][...]
    from1 = product(mix, slice(0, starts[1]), 1, second)
    shrunk = jnp.dot(second, pools[1][...], preferred_element_type=F32)
    shrunk = shrunk * jnp.where(lane < 64, 0.25, 0.0625)
    down1 = product(mix, slice(starts[2], total), 1, shrunk.astype(BF16))
    total2 = total2 + down1[: starts[3] - starts[2]]
    tail3 = down1[starts[3] - starts[2] :]
    total1 = second.astype(F32) + offsets[1]

    def add3(total0, total1, total2, total3, far0, far1):
        return (
            total0 + spread(far0, pools[0][...]),
            total1 + spread(far1, pools[1][...]),
            total2 + spread(from3[two], pools[2][...]),
            total3 + last,
        )

    if late3:
        nothing = jnp.zeros((1, LANES), F32)
        near0 = jnp.concatenate([from1, side_by_side(from2[first], nothing)], axis=1)
        total0 = offsets[0] + spread(near0, pools[0][...])
        total1 = total1 + spread(side_by_side(from2[one], nothing), pools[1][...])
    else:
        far0 = jnp.concatenate([from1, side_by_side(from2[first], from3[first])], axis=1)
        far1 = side_by_side(from2[one], from3[one])
        total0, total1, total2, total3 = add3(offsets[0], total1, total2, total3, far0, far1)

    arrived(0)
    maps = helds[0][...]
    shrunk = jnp.dot(maps, pools[0][...], preferred_element_type=F32)
    near = (shrunk[:, :256] * 0.25).astype(BF16)
    far = (shrunk[:, 256:] * jnp.where(lane < 64, 0.0625, 0.015625)).astype(BF16)
    total1 = total1 + product(mix, one, 0, near)
    down0 = product(mix, slice(starts[2], total), 0, far)
    total2 = total2 + down0[: starts[3] - starts[2]]
    total3 = total3 + turned(tail3 + down0[starts[3] - starts[2] :], -64)
    if late3:
        last, from3 = take3()
        apart = jnp.where((lane >= 64) & (lane < 80), turned(from3[: starts[2]], 64), 0.0)
        total0 = total0 + spread(apart[first], pools[0][:, 256:])
        total1 = total1 + spread(apart[one], pools[1][...])
        total2 = total2 + spread(from3[two], pools[2][...])
        total3 = total3 + last
    total0 = jnp.maximum(total0 + maps.astype(F32), 0.0)
    lines = [total0[:, at : at + LANES] for at in range(0, total0.shape[1], LANES)]
    outs[0][...] = jnp.stack(lines, axis=1).astype(BF16)
    for out, value in zip(outs[1:], (total1, total2, total3)):
        out[...] = jnp.maximum(value, 0.0).T[: out.shape[0]].astype(BF16)


HELD_SHAPES = ((48, 1024), (96, 256), (96, 128), (48, 128))


def front(section, kernels, biases, join_weight, join_bias):
    anywhere = pl.BlockSpec(memory_space=pl.ANY)
    vmem = pl.BlockSpec(memory_space=pltpu.VMEM)

    def field(b, tiles):
        return (WIDTH << b, tiles[b] * LANES)

    scratch = [pltpu.VMEM(shape, BF16) for shape in HELD_SHAPES]
    scratch += [pltpu.VMEM(join_weight.shape, BF16), pltpu.VMEM(join_bias.shape, F32)]
    scratch += [pltpu.VMEM(shape, BF16) for shape in ((1024, 384), (256, 128), (128, 128))]
    scratch += [
        pltpu.VMEM((WIDTH, TH * TW // 2), BF16),
        pltpu.VMEM(kernels.shape, BF16),
        pltpu.VMEM(biases.shape, F32),
    ]
    scratch += [pltpu.VMEM(field(b, FIELD_TILES), BF16) for b in range(4)]
    scratch += [pltpu.VMEM((2, *field(b, FIELD_TILES)), BF16) for b in range(4)]
    scratch += [pltpu.VMEM((2, 96, LANES), BF16), pltpu.VMEM((8, 96, LANES), BF16)]
    scratch += [pltpu.VMEM((2, *field(b, HIDDEN_TILES)), BF16) for b in range(4)]
    scratch += [pltpu.VMEM(field(b, HIDDEN_TILES), BF16) for b in range(4)]
    scratch += [pltpu.VMEM(field(b, OWN_TILES), BF16) for b in range(2)]
    scratch += [pltpu.VMEM((STRIPS, size, LANES), BF16) for size in (2 * WIDTH, WIDTH)]
    pieces = ((48, 256), (96, 128), (96, 128), (48, 128))
    scratch += [pltpu.VMEM((RELAYS, *piece), BF16) for piece in pieces]
    counts = ((6,), (8,), (8,), (2, 3), (2, 3), (16 + RELAYS,), (4,), (RELAYS,), (4,))
    scratch += [pltpu.SemaphoreType.DMA(count) for count in counts]
    return pl.pallas_call(
        front_kernel,
        out_shape=[pltpu.VMEM(shape, BF16) for shape in OUT_SHAPES],
        in_specs=[anywhere] * 5,
        out_specs=[vmem] * 4,
        scratch_shapes=scratch,
        compiler_params=pltpu.CompilerParams(
            collective_id=0, has_side_effects=True, vmem_limit_bytes=VMEM_LIMIT
        ),
        name="front",
    )(
        *(
            pltpu.with_memory_space_constraint(array, pltpu.HBM)
            for array in (section, kernels, biases, join_weight, join_bias)
        )
    )


OUT_SHAPES = ((48, 8, 128), (256, 96), (64, 192), (16, 384))
VMEM_LIMIT = 48 << 20


def finish_kernel(*refs):
    sources, targets, sem = refs[:4], refs[4:8], refs[8]
    copies = [
        pltpu.make_async_copy(source, target, sem.at[at])
        for at, (source, target) in enumerate(zip(sources, targets))
    ]
    for copy in copies:
        copy.start()
    for copy in copies:
        copy.wait()


def finished(outs):
    return pl.pallas_call(
        finish_kernel,
        out_shape=[jax.ShapeDtypeStruct(out.shape, out.dtype) for out in outs],
        in_specs=[pl.BlockSpec(memory_space=pltpu.VMEM)] * 4,
        out_specs=[pl.BlockSpec(memory_space=pl.ANY)] * 4,
        scratch_shapes=[pltpu.SemaphoreType.DMA((4,))],
        compiler_params=pltpu.CompilerParams(vmem_limit_bytes=1 << 20),
        name="finish",
    )(*outs)


def local(section_in, conv_weight, conv_bias, join_weight, join_bias):
    outs = finished(
        front(section_in[0, 0, 0], conv_weight[0], conv_bias[0], join_weight, join_bias)
    )
    shapes = [(WIDTH << b, (TH >> b) // STRIPS, TW >> b) for b in range(4)]
    return tuple(
        out if out.ndim == 3 else out.reshape(*shape[1:], shape[0]).transpose(2, 0, 1)
        for out, shape in zip(outs, shapes)
    )


def solution(mesh):
    in_specs = (
        P("branch", "row", "col", None, None),
        P("branch", None, None, None, None, None),
        P("branch", None, None),
        P(),
        P(),
    )
    out_specs = (P(None, ("branch", "row"), "col"),) * 4
    return jax.shard_map(local, mesh=mesh, in_specs=in_specs, out_specs=out_specs, check_vma=False)
```

```python
from functools import partial

import jax
import jax.numpy as jnp
from jax import lax
from jax.experimental import pallas as pl
from jax.experimental.pallas import tpu as pltpu
from jax.sharding import PartitionSpec as P

WIDTH = 48
TH = 32
TW = 128
LANES = 128
STRIPS = 4
MESH = pl.DeviceIdType.MESH
WAYS = [(dr, dc) for dr in (-1, 0, 1) for dc in (-1, 0, 1) if dr or dc]
F32 = jnp.float32
BF16 = jnp.bfloat16

OWN_TILES = (32, 8, 2, 1)
BEFORE = (2, 1, 1, 0)
FIELD_TILES = (36, 10, 4, 1)
HIDDEN_TILES = (34, 10, 4, 1)
HIDDEN_START = (1, 0, 0, 0)


CHUNKS = (4, 2, 1, 1)
RELAYS = 12


def route(source, tile, strip, chunk):
    if tile == source or strip == tile or source == 3:
        return None
    if source == 0 and strip == 3 - tile:
        return None
    return strip


def relayed(source, place):
    pieces = [
        (tile, strip, chunk)
        for chunk in range(CHUNKS[source])
        for tile in range(STRIPS)
        for strip in range(STRIPS)
        if tile != place and route(source, tile, strip, chunk) == place
    ]
    return sorted(
        pieces,
        key=lambda p: (
            source == 0 and halo_bound(*p[1:]),
            p[2],
            (p[0] ^ place).bit_count(),
            -abs(p[0] - source),
        ),
    )


def halo_bound(strip, chunk):
    return (strip, chunk) in ((0, 0), (STRIPS - 1, CHUNKS[0] - 1))


def own_pieces(source, place):
    chunks = range(CHUNKS[source])
    if source == place:
        return [(place ^ turn, chunk) for turn in (0, 1, 2, 3) for chunk in chunks]
    return [(place ^ turn, chunk) for chunk in chunks for turn in (1, 2, 0, 3)]


def lane_index(width=LANES):
    return lax.broadcasted_iota(jnp.int32, (1, width), 1)


def turned(group, shift):
    shift = shift % LANES
    return pltpu.roll(group, shift, 1) if shift else group


def tiles_turned(field, shift):
    if shift % LANES == 0:
        return field
    tiles = [turned(field[:, t : t + LANES], shift) for t in range(0, field.shape[1], LANES)]
    return tiles[0] if len(tiles) == 1 else jnp.concatenate(tiles, axis=1)


def natural_tile(branch_level, container_ref):
    pixels = TH * TW >> 2 * branch_level
    channels = WIDTH << branch_level
    parts = []
    for part in range(1 << branch_level):
        at = part * pixels
        low = at // LANES * LANES
        piece = container_ref[:, low : low + max(pixels, LANES)]
        if at > low:
            piece = pltpu.roll(piece.astype(F32), LANES - at + low, 1).astype(BF16)
        parts.append(piece)
    held = lax.broadcasted_iota(jnp.int32, (1, channels), 1)
    part = sum((held >= WIDTH * turn).astype(jnp.int32) for turn in range(1, 1 << branch_level))
    home = ((held - WIDTH * part) << branch_level) + part
    order = jnp.where(lax.broadcasted_iota(jnp.int32, (channels, channels), 0) == home, 1.0, 0.0)
    return jnp.dot(
        order.astype(BF16), jnp.concatenate(parts, axis=0), preferred_element_type=F32
    ).astype(BF16)


def column_stack(branch_level, own, west, east):
    cols = TW >> branch_level
    col = lane_index(own.shape[1]) & (cols - 1)
    own32 = own.astype(F32)
    minus = tiles_turned(
        jnp.where(col == cols - 1, tiles_turned(west.astype(F32), -cols), own32), 1
    ).astype(BF16)
    plus = tiles_turned(
        jnp.where(col == 0, tiles_turned(east.astype(F32), cols), own32), -1
    ).astype(BF16)

    def zeros(rows):
        return jnp.zeros((rows, own.shape[1]), BF16)

    if branch_level == 0:
        pieces = [minus, own, zeros(32), plus, zeros(80)]
    elif branch_level == 3:
        pieces = [minus, own, plus]
    else:
        pad = zeros(-own.shape[0] % LANES)
        pieces = [minus, pad, own, pad, plus, pad]
    return jnp.concatenate(pieces, axis=0)


def taps(branch_level, weights, layer):
    channels = WIDTH << branch_level
    width = -(-channels // LANES) * LANES
    lines = []
    for dy in range(3):
        if branch_level == 0:
            first, middle, last = (weights[layer, dy, dx, 0:channels, 0:width] for dx in range(3))
            pair = jnp.where(
                lane_index() < channels,
                first.astype(F32),
                pltpu.roll(middle.astype(F32), channels, 1),
            )
            lines.append(jnp.concatenate([pair.astype(BF16), last], axis=1))
        else:
            lines.append(
                jnp.concatenate(
                    [weights[layer, dy, dx, 0:channels, 0:width] for dx in range(3)], axis=1
                )
            )
    return jnp.concatenate(lines, axis=0)


def row_sum(branch_level, products, first, count):
    channels = products.shape[0] // 3
    cols = TW >> branch_level
    above, here, below = (products[d * channels : (d + 1) * channels] for d in range(3))
    span = slice(first * LANES, (first + count) * LANES)
    if cols == LANES:
        return (
            above[:, (first - 1) * LANES : (first - 1 + count) * LANES]
            + here[:, span]
            + below[:, (first + 1) * LANES : (first + 1 + count) * LANES]
        )
    last = products.shape[1] // LANES - 1
    above, below = tiles_turned(above, cols), tiles_turned(below, -cols)
    lane = lane_index()

    def tile(field, t):
        t = min(max(t, 0), last)
        return field[:, t * LANES : (t + 1) * LANES]

    tiles = [
        jnp.where(lane < cols, tile(above, t - 1), tile(above, t))
        + tile(here, t)
        + jnp.where(lane >= LANES - cols, tile(below, t + 1), tile(below, t))
        for t in range(first, first + count)
    ]
    return tiles[0] if count == 1 else jnp.concatenate(tiles, axis=1)


def front_kernel(
    section, kernels, biases, join_weight, join_bias, out0, out1, out2, out3,
    held0, held1, held2, held3, mix, mix_bias, pool0, pool1, pool2,
    container, weights, bias, own0, own1, own2, own3, side0, side1, side2, side3,
    pack_send, pack_recv, hide0, hide1, hide2, hide3, hid0, hid1, hid2, hid3,
    settled0, settled1, settled2, settled3, relay0, relay1, relay2, relay3, load_sem,
    halo_send, halo_recv, hidden_send, hidden_recv, strip_send, strip_recv, relay_recv, own_sem,
):
    level = lax.axis_index("branch")
    place = lax.axis_index("row")
    col = lax.axis_index("col")
    row_count = lax.axis_size("row")
    col_count = lax.axis_size("col")

    def reach(dr, dc):
        there = jnp.bool_(True)
        if dr:
            there = (place + dr >= 0) & (place + dr < row_count)
        if dc:
            sideways = (col + dc >= 0) & (col + dc < col_count)
            there = there & sideways if dr else sideways
        device = (
            level,
            lax.rem(place + dr + row_count, row_count),
            lax.rem(col + dc + col_count, col_count),
        )
        return there, device

    barrier = pltpu.get_barrier_semaphore()
    expected = 0
    for dr, dc in WAYS:
        there, device = reach(dr, dc)
        expected = expected + there.astype(jnp.int32)

        @pl.when(there)
        def _():
            pl.semaphore_signal(barrier, inc=1, device_id=device, device_id_type=MESH)

    at_home = level == place
    for step in range(1, STRIPS):
        for device in (
            (level, lax.rem(place + step, STRIPS), col),
            (lax.rem(level + step, STRIPS), place, col),
        ):
            pl.semaphore_signal(barrier, inc=1, device_id=device, device_id_type=MESH)

    @pl.when((level > 0) & (place == STRIPS - 1 - level))
    def _():
        pl.semaphore_signal(barrier, inc=1, device_id=(0, level, col), device_id_type=MESH)

    @pl.when(jnp.logical_not(at_home & (level == 3)))
    def _():
        pl.semaphore_signal(barrier, inc=1, device_id=(3, level, col), device_id_type=MESH)

    expected = expected + jnp.where(level == 3, STRIPS - at_home.astype(jnp.int32), 0)
    expected = expected + 2 * (STRIPS - 1) + ((level == 0) & (place > 0)).astype(jnp.int32)

    helds = (held0, held1, held2, held3)
    owns = (own0, own1, own2, own3)
    sides = (side0, side1, side2, side3)
    hides = (hide0, hide1, hide2, hide3)
    hids = (hid0, hid1, hid2, hid3)
    settleds = (settled0, settled1, settled2, settled3)
    relays = (relay0, relay1, relay2, relay3)

    mix_loads = [
        pltpu.make_async_copy(join_weight, mix, load_sem.at[4]),
        pltpu.make_async_copy(join_bias, mix_bias, load_sem.at[5]),
    ]

    def branch(b):
        channels = WIDTH << b
        width = -(-channels // LANES) * LANES
        pixels = TH * TW >> b
        cols, rows = TW >> b, TH >> b
        own, side, hide, hid = owns[b], sides[b], hides[b], hids[b]
        settled, held, relay = settleds[b], helds[b], relays[b]
        before, tiles = BEFORE[b], OWN_TILES[b]
        middle = slice(before * LANES, (before + tiles) * LANES)
        packed = b >= 2
        folds = channels // 96
        pair = 2 * cols
        chunks = CHUNKS[b]
        lane = lane_index()
        order = [way for way in WAYS if way[0]] + [way for way in WAYS if not way[0]]

        load = pltpu.make_async_copy(
            section.at[:, 0:pixels],
            own.at[:, middle] if b == 0 else container.at[:, 0:pixels],
            load_sem.at[0],
        )
        bias_load = pltpu.make_async_copy(biases, bias, load_sem.at[1])
        weight_loads = [
            pltpu.make_async_copy(
                kernels.at[layer, :, :, 0:channels, 0:width],
                weights.at[layer, :, :, 0:channels, 0:width],
                load_sem.at[2 + layer],
            )
            for layer in range(2)
        ]

        def begin():
            for copy in (load, bias_load, *weight_loads, *mix_loads):
                copy.start()

        def halo_region(dr, dc):
            if packed and dr:
                return pack_recv.at[WAYS.index((dr, dc))]
            target = own if dc == 0 else side.at[0 if dc == 1 else 1]
            if dr == 0:
                return target.at[:, middle]
            if dr == 1:
                return target.at[:, 0 : before * LANES]
            return target.at[:, (before + tiles) * LANES : (before + tiles + before) * LANES]

        def halo_source(dr):
            if dr == 0:
                return own.at[:, middle]
            if packed:
                return pack_send.at[0 if dr == -1 else 1]
            first = before if dr == -1 else tiles
            return own.at[:, first * LANES : (first + before) * LANES]

        def halo_copy(dr, dc):
            way = WAYS.index((dr, dc))
            return pltpu.make_async_remote_copy(
                src_ref=halo_source(dr),
                dst_ref=halo_region(dr, dc),
                send_sem=halo_send.at[way],
                recv_sem=halo_recv.at[way],
                device_id=reach(dr, dc)[1],
                device_id_type=MESH,
            )

        last = HIDDEN_TILES[b]
        if b < 2:
            hidden_parts = ((2, last - 2), (0, 2), (last - 2, last))
        else:
            hidden_parts = ((0, last),)

        def hidden_copy(dc, part):
            at = 0 if dc == 1 else 1
            low, high = hidden_parts[part]
            span = slice(low * LANES, high * LANES)
            return pltpu.make_async_remote_copy(
                src_ref=hid.at[:, span],
                dst_ref=hide.at[at, :, span],
                send_sem=hidden_send.at[at, part],
                recv_sem=hidden_recv.at[at, part],
                device_id=reach(0, dc)[1],
                device_id_type=MESH,
            )

        def hidden_start(*parts):
            for part in parts:
                for dc in (1, -1):
                    pl.when(reach(0, dc)[0])(hidden_copy(dc, part).start)

        def hidden_wait(*parts):
            for part in parts:
                for dc in (1, -1):
                    pl.when(reach(0, -dc)[0])(hidden_copy(dc, part).wait_recv)

        def bias_columns():
            bias_load.wait()
            return [
                jnp.broadcast_to(bias[layer : layer + 1, :], (8, bias.shape[1])).T[:channels, 0:1]
                for layer in range(2)
            ]

        def convolved(layer, fields, first, count):
            products = jnp.dot(
                taps(b, weights, layer), column_stack(b, *fields), preferred_element_type=F32
            )
            return row_sum(b, products, first, count)

        def settle_hidden(raw, offset, first):
            count = raw.shape[1] // LANES
            row = lax.shift_right_logical(lane_index(count * LANES), cols.bit_length() - 1)
            if b == 3:
                row = jnp.where(row >= 6, row - 8, row)
            else:
                row = row + (first + HIDDEN_START[b] - before) * (LANES // cols)
            low = jnp.where(place == 0, 0, -LANES)
            high = jnp.where(place == row_count - 1, rows, 2 * LANES)
            hidden = jnp.where((row >= low) & (row < high), jnp.maximum(raw + offset, 0.0), 0.0)
            hid[:, first * LANES : (first + count) * LANES] = hidden.astype(BF16)

        def hidden_tiles(offset, first, count):
            low = max(first + HIDDEN_START[b] - 1, 0)
            high = min(first + HIDDEN_START[b] + count + 1, FIELD_TILES[b])
            span = slice(low * LANES, high * LANES)
            fields = (own[:, span], side[0, :, span], side[1, :, span])
            start = first + HIDDEN_START[b] - low
            settle_hidden(convolved(0, fields, start, count), offset, first)

        def settled_tiles(offset, first, count):
            span = slice(first * LANES, (first + count + 2) * LANES)
            fields = (hid[:, span], hide[0, :, span], hide[1, :, span])
            after = convolved(1, fields, 1, count)
            kept = own[:, (before + first) * LANES : (before + first + count) * LANES]
            final = jnp.maximum(after + offset + kept.astype(F32), 0.0)
            settled[:, first * LANES : (first + count) * LANES] = final.astype(BF16)

        def ends(strip, chunk):
            if packed:
                return settled.at[strip], held
            size = tiles * LANES // STRIPS // chunks
            at = (strip * chunks + chunk) * size
            return settled.at[:, at : at + size], held.at[:, chunk * size : (chunk + 1) * size]

        def exchange(here, wanted=None, handing=False, closing=False):
            count = 0

            def send(source, target, arrived, device, act=True):
                nonlocal count
                copy = pltpu.make_async_remote_copy(
                    src_ref=source,
                    dst_ref=target,
                    send_sem=strip_send.at[count],
                    recv_sem=arrived,
                    device_id=device,
                    device_id_type=MESH,
                )
                count += 1
                if closing:
                    copy.wait_send()
                elif act:
                    copy.start()

            at_once = []
            for strip, chunk in own_pieces(b, here):
                source, target = ends(strip, chunk)
                act = not closing and wanted(strip, chunk)
                if here == b and strip == here:
                    copy = pltpu.make_async_copy(source, target, own_sem.at[chunk])
                    if act:
                        copy.start()
                    if handing:
                        at_once.append(copy)
                    continue
                via = route(b, here, strip, chunk)
                if via is None:
                    send(source, target, strip_recv.at[b], (here, strip, col), act)
                else:
                    slot = relayed(b, via).index((here, strip, chunk))
                    send(source, relay.at[slot], relay_recv.at[slot], (b, via, col), act)
            if not handing and not closing:
                return
            for slot, (tile, strip, chunk) in enumerate(relayed(b, here)):
                piece = relay.at[slot]
                if not closing:
                    pltpu.make_async_remote_copy(
                        src_ref=piece,
                        dst_ref=piece,
                        send_sem=strip_send.at[0],
                        recv_sem=relay_recv.at[slot],
                        device_id=(b, tile, col),
                        device_id_type=MESH,
                    ).wait_recv()
                send(piece, ends(strip, chunk)[1], strip_recv.at[b], (tile, strip, col))
            for copy in at_once:
                copy.wait()

        def open_halo():
            load.wait()
            if b:
                own[:, middle] = natural_tile(b, container)
            if packed:
                for end in range(2):
                    tile = before if end == 0 else before + tiles - 1
                    at = 0 if end == 0 else (rows - 2) * cols % LANES
                    edge = own[:, tile * LANES : (tile + 1) * LANES].astype(F32)
                    out = None
                    for g in range(folds):
                        part = turned(edge[g * 96 : (g + 1) * 96], pair * g - at)
                        out = part if g == 0 else jnp.where(lane < pair * g, out, part)
                    pack_send[end] = out.astype(BF16)

            pl.semaphore_wait(barrier, expected)
            for dr, dc in sorted(order, key=lambda way: way[0] != 0):
                pl.when(reach(dr, dc)[0])(halo_copy(dr, dc).start)
            for dr, dc in order:

                @pl.when(jnp.logical_not(reach(-dr, -dc)[0]))
                def _():
                    region = halo_region(dr, dc)
                    region[...] = jnp.zeros(region.shape, BF16)

            for dc in (1, -1):

                @pl.when(jnp.logical_not(reach(0, -dc)[0]))
                def _():
                    at = 0 if dc == 1 else 1
                    hide[at] = jnp.zeros(hid.shape, BF16)

        def run():
            def halo_wait(ways):
                for dr, dc in ways:
                    pl.when(reach(-dr, -dc)[0])(halo_copy(dr, dc).wait_recv)

            def leave(wanted, **how):
                for here in range(STRIPS):
                    pl.when(place == here)(partial(exchange, here, wanted, **how))

            offsets = bias_columns()
            weight_loads[0].wait()
            def anything(strip, chunk):
                return True

            if not packed:
                halo_wait([way for way in order if not way[0]])
                hidden_tiles(offsets[0], 2, last - 4)
                hidden_start(0)
                if b == 0:
                    weight_loads[1].wait()
                    hidden_wait(0)
                    settled_tiles(offsets[1], 2, tiles - 4)
                    leave(lambda strip, chunk: not halo_bound(strip, chunk))
                halo_wait([way for way in order if way[0]])
                hidden_tiles(offsets[0], 0, 2)
                hidden_tiles(offsets[0], last - 2, 2)
                hidden_start(1, 2)
                if b == 0:
                    hidden_wait(1, 2)
                    settled_tiles(offsets[1], 0, 2)
                    settled_tiles(offsets[1], tiles - 2, 2)
                    leave(halo_bound, handing=True)
                else:
                    weight_loads[1].wait()
                    hidden_wait(0, 1, 2)
                    settled_tiles(offsets[1], 0, tiles)
                    leave(anything, handing=True)
                return

            halo_wait(order)
            fields = []
            for target, dc in ((own, 0), (side.at[0], 1), (side.at[1], -1)):
                upper = pack_recv[WAYS.index((1, dc))].astype(F32)
                lower = pack_recv[WAYS.index((-1, dc))].astype(F32)
                lines = []
                for g in range(folds):
                    here = target[g * 96 : (g + 1) * 96, middle]
                    above = turned(upper, LANES - pair - pair * g)
                    if b == 3:
                        ring = jnp.where(lane < 96, turned(lower, 64 - pair * g), above)
                        lines.append(jnp.where(lane < 64, here.astype(F32), ring).astype(BF16))
                    else:
                        below = turned(lower, -pair * g)
                        lines.append(
                            jnp.concatenate([above.astype(BF16), here, below.astype(BF16)], axis=1)
                        )
                fields.append(jnp.concatenate(lines, axis=0))
            settle_hidden(convolved(0, fields, 0, last), offsets[0], 0)
            hidden_start(0)
            weight_loads[1].wait()
            hidden_wait(0)
            after = convolved(1, (hid[...], hide[0], hide[1]), before, tiles)
            final = jnp.maximum(after + offsets[1] + own[:, middle].astype(F32), 0.0)
            size = settled.shape[1]
            pixels = strip_pixels(b)
            for strip in range(STRIPS):
                tile, at = divmod(strip * pixels, LANES)
                strip_tile = final[:, tile * LANES : (tile + 1) * LANES]
                out = None
                for g in range(LANES // pixels):
                    part = turned(strip_tile[g * size : (g + 1) * size], pixels * g - at)
                    out = part if g == 0 else jnp.where(lane < pixels * g, out, part)
                settled[strip] = out.astype(BF16)

            leave(anything, handing=True)

        def close():
            for here in range(STRIPS):
                pl.when(place == here)(partial(exchange, here, closing=True))
            for dr, dc in order:
                pl.when(reach(dr, dc)[0])(halo_copy(dr, dc).wait_send)
            for part in range(len(hidden_parts)):
                for dc in (1, -1):
                    pl.when(reach(0, dc)[0])(hidden_copy(dc, part).wait_send)

        return begin, open_halo, run, close

    branches = [branch(b) for b in range(STRIPS)]
    for b, (begin, _, _, _) in enumerate(branches):
        pl.when(level == b)(begin)
    for b, (_, open_halo, _, _) in enumerate(branches):
        pl.when(level == b)(open_halo)

    pool_refs = (pool0, pool1, pool2)
    for fine, pool in enumerate(pool_refs):
        pool[...] = pool_table(fine)

    for b, (_, _, run, _) in enumerate(branches):
        pl.when(level == b)(run)

    for copy in mix_loads:
        copy.wait()

    def arrived(source):
        arrival = pltpu.make_async_remote_copy(
            src_ref=helds[source],
            dst_ref=helds[source],
            send_sem=strip_send.at[0],
            recv_sem=strip_recv.at[source],
            device_id=(source, level, col),
            device_id_type=MESH,
        )
        pl.when(jnp.logical_not(at_home & (level == source)))(arrival.wait_recv)

    for late3 in (True, False):

        @pl.when((level < 2) if late3 else (level >= 2))
        def _():
            outs = (out0, out1, out2, out3)
            join(late3, place, arrived, helds, mix, mix_bias, pool_refs, outs)

    for b, (_, _, _, close) in enumerate(branches):
        pl.when(level == b)(close)


def coarse_home(fine_level, coarse_level):
    fine_cols, coarse_cols = TW >> fine_level, TW >> coarse_level
    shift = coarse_level - fine_level
    pixel = lax.broadcasted_iota(jnp.int32, (strip_pixels(fine_level), 1), 0)
    row = lax.shift_right_logical(pixel, fine_cols.bit_length() - 1 + shift)
    return row * coarse_cols + lax.shift_right_logical(pixel & (fine_cols - 1), shift)


def strip_pixels(branch_level):
    return TH * TW // STRIPS >> 2 * branch_level


def pool_table(fine_level):
    at = 0
    hits = []
    for coarse_level in range(fine_level + 1, STRIPS):
        hits.append((at, at + coarse_home(fine_level, coarse_level)))
        at += strip_pixels(coarse_level)
    tiles = []
    for tile in range(-(-at // LANES)):
        target = lane_index() + tile * LANES
        hit = None
        for first, home in hits:
            same = home == target
            hit = same if hit is None else hit | same
        tiles.append(jnp.where(hit, 1.0, 0.0).astype(BF16))
    table = tiles[0] if len(tiles) == 1 else jnp.concatenate(tiles, axis=1)
    short = max(LANES - table.shape[0], 0)
    if short:
        table = jnp.concatenate([table, jnp.zeros((short, table.shape[1]), BF16)], axis=0)
    return table


def product(mix, rows, source, data):
    start = ((1 << source) - 1) * WIDTH
    stop = start + data.shape[0]
    low = start // LANES * LANES
    high = min(-(-stop // LANES) * LANES, mix.shape[1])
    pieces = [data]
    if start > low:
        pieces.insert(0, jnp.zeros((start - low, data.shape[1]), BF16))
    if high > stop:
        pieces.append(jnp.zeros((high - stop, data.shape[1]), BF16))
    stacked = jnp.concatenate(pieces, axis=0)
    return jnp.dot(
        mix[rows, low:high], stacked, preferred_element_type=F32
    ).astype(BF16).astype(F32)


def spread(term, pool):
    return lax.dot_general(
        term.astype(BF16), pool, (((1,), (1,)), ((), ())), preferred_element_type=F32
    )


def join(late3, place, arrived, helds, mix, mix_bias, pools, outs):
    lane = lane_index()
    total = mix_bias.shape[0]
    line = jnp.concatenate([mix_bias[...][None, :], jnp.zeros((1, -total % LANES), F32)], axis=1)
    offset = jnp.broadcast_to(line, (8, line.shape[1])).T
    starts = [((1 << b) - 1) * WIDTH for b in range(STRIPS + 1)]
    offsets = [offset[starts[b] : starts[b + 1], 0:1] for b in range(STRIPS)]
    one, two, three = (slice(starts[b], starts[b + 1]) for b in range(1, STRIPS))

    def side_by_side(near, far):
        return jnp.where(lane < 64, near, jnp.where(lane < 80, turned(far, 64), 0.0))

    def take3():
        arrived(3)
        folded = helds[3][...].astype(F32)
        last = jnp.concatenate([turned(folded, -16 * g) for g in range(8)], axis=0)
        return last, product(mix, slice(0, starts[3]), 3, last.astype(BF16))

    first = slice(0, starts[1])
    if not late3:
        last, from3 = take3()

    arrived(2)
    pieces = helds[2][...].astype(F32)
    third = jnp.concatenate([pieces, turned(pieces, -64)], axis=0)
    third16 = third.astype(BF16)
    from2 = product(mix, slice(0, starts[2]), 2, third16)
    shrunk = jnp.dot(third16, pools[2][...], preferred_element_type=F32)
    total3 = offsets[3] + product(mix, three, 2, (shrunk * 0.25).astype(BF16))
    total2 = third + offsets[2]

    arrived(1)
    second = helds[1][...]
    from1 = product(mix, slice(0, starts[1]), 1, second)
    shrunk = jnp.dot(second, pools[1][...], preferred_element_type=F32)
    shrunk = shrunk * jnp.where(lane < 64, 0.25, 0.0625)
    down1 = product(mix, slice(starts[2], total), 1, shrunk.astype(BF16))
    total2 = total2 + down1[: starts[3] - starts[2]]
    tail3 = down1[starts[3] - starts[2] :]
    total1 = second.astype(F32) + offsets[1]

    def add3(total0, total1, total2, total3, far0, far1):
        return (
            total0 + spread(far0, pools[0][...]),
            total1 + spread(far1, pools[1][...]),
            total2 + spread(from3[two], pools[2][...]),
            total3 + last,
        )

    if late3:
        nothing = jnp.zeros((1, LANES), F32)
        near0 = jnp.concatenate([from1, side_by_side(from2[first], nothing)], axis=1)
        total0 = offsets[0] + spread(near0, pools[0][...])
        total1 = total1 + spread(side_by_side(from2[one], nothing), pools[1][...])
    else:
        far0 = jnp.concatenate([from1, side_by_side(from2[first], from3[first])], axis=1)
        far1 = side_by_side(from2[one], from3[one])
        total0, total1, total2, total3 = add3(offsets[0], total1, total2, total3, far0, far1)

    arrived(0)
    maps = helds[0][...]
    shrunk = jnp.dot(maps, pools[0][...], preferred_element_type=F32)
    near = (shrunk[:, :256] * 0.25).astype(BF16)
    far = (shrunk[:, 256:] * jnp.where(lane < 64, 0.0625, 0.015625)).astype(BF16)
    total1 = total1 + product(mix, one, 0, near)
    down0 = product(mix, slice(starts[2], total), 0, far)
    total2 = total2 + down0[: starts[3] - starts[2]]
    total3 = total3 + turned(tail3 + down0[starts[3] - starts[2] :], -64)
    if late3:
        last, from3 = take3()
        apart = jnp.where((lane >= 64) & (lane < 80), turned(from3[: starts[2]], 64), 0.0)
        total0 = total0 + spread(apart[first], pools[0][:, 256:])
        total1 = total1 + spread(apart[one], pools[1][...])
        total2 = total2 + spread(from3[two], pools[2][...])
        total3 = total3 + last
    total0 = jnp.maximum(total0 + maps.astype(F32), 0.0)
    lines = [total0[:, at : at + LANES] for at in range(0, total0.shape[1], LANES)]
    outs[0][...] = jnp.stack(lines, axis=1).astype(BF16)
    for out, value in zip(outs[1:], (total1, total2, total3)):
        out[...] = jnp.maximum(value, 0.0).T[: out.shape[0]].astype(BF16)


HELD_SHAPES = ((48, 1024), (96, 256), (96, 128), (48, 128))


def front(section, kernels, biases, join_weight, join_bias):
    anywhere = pl.BlockSpec(memory_space=pl.ANY)
    vmem = pl.BlockSpec(memory_space=pltpu.VMEM)

    def field(b, tiles):
        return (WIDTH << b, tiles[b] * LANES)

    scratch = [pltpu.VMEM(shape, BF16) for shape in HELD_SHAPES]
    scratch += [pltpu.VMEM(join_weight.shape, BF16), pltpu.VMEM(join_bias.shape, F32)]
    scratch += [pltpu.VMEM(shape, BF16) for shape in ((1024, 384), (256, 128), (128, 128))]
    scratch += [
        pltpu.VMEM((WIDTH, TH * TW // 2), BF16),
        pltpu.VMEM(kernels.shape, BF16),
        pltpu.VMEM(biases.shape, F32),
    ]
    scratch += [pltpu.VMEM(field(b, FIELD_TILES), BF16) for b in range(4)]
    scratch += [pltpu.VMEM((2, *field(b, FIELD_TILES)), BF16) for b in range(4)]
    scratch += [pltpu.VMEM((2, 96, LANES), BF16), pltpu.VMEM((8, 96, LANES), BF16)]
    scratch += [pltpu.VMEM((2, *field(b, HIDDEN_TILES)), BF16) for b in range(4)]
    scratch += [pltpu.VMEM(field(b, HIDDEN_TILES), BF16) for b in range(4)]
    scratch += [pltpu.VMEM(field(b, OWN_TILES), BF16) for b in range(2)]
    scratch += [pltpu.VMEM((STRIPS, size, LANES), BF16) for size in (2 * WIDTH, WIDTH)]
    pieces = ((48, 256), (96, 128), (96, 128), (48, 128))
    scratch += [pltpu.VMEM((RELAYS, *piece), BF16) for piece in pieces]
    counts = ((6,), (8,), (8,), (2, 3), (2, 3), (16 + RELAYS,), (4,), (RELAYS,), (4,))
    scratch += [pltpu.SemaphoreType.DMA(count) for count in counts]
    return pl.pallas_call(
        front_kernel,
        out_shape=[pltpu.VMEM(shape, BF16) for shape in OUT_SHAPES],
        in_specs=[anywhere] * 5,
        out_specs=[vmem] * 4,
        scratch_shapes=scratch,
        compiler_params=pltpu.CompilerParams(
            collective_id=0, has_side_effects=True, vmem_limit_bytes=VMEM_LIMIT
        ),
        name="front",
    )(
        *(
            pltpu.with_memory_space_constraint(array, pltpu.HBM)
            for array in (section, kernels, biases, join_weight, join_bias)
        )
    )


OUT_SHAPES = ((48, 8, 128), (256, 96), (64, 192), (16, 384))
VMEM_LIMIT = 48 << 20


def finish_kernel(*refs):
    sources, targets, sem = refs[:4], refs[4:8], refs[8]
    copies = [
        pltpu.make_async_copy(source, target, sem.at[at])
        for at, (source, target) in enumerate(zip(sources, targets))
    ]
    for copy in copies:
        copy.start()
    for copy in copies:
        copy.wait()


def finished(outs):
    return pl.pallas_call(
        finish_kernel,
        out_shape=[jax.ShapeDtypeStruct(out.shape, out.dtype) for out in outs],
        in_specs=[pl.BlockSpec(memory_space=pltpu.VMEM)] * 4,
        out_specs=[pl.BlockSpec(memory_space=pl.ANY)] * 4,
        scratch_shapes=[pltpu.SemaphoreType.DMA((4,))],
        compiler_params=pltpu.CompilerParams(vmem_limit_bytes=1 << 20),
        name="finish",
    )(*outs)


def local(section_in, conv_weight, conv_bias, join_weight, join_bias):
    outs = finished(
        front(section_in[0, 0, 0], conv_weight[0], conv_bias[0], join_weight, join_bias)
    )
    shapes = [(WIDTH << b, (TH >> b) // STRIPS, TW >> b) for b in range(4)]
    return tuple(
        out if out.ndim == 3 else out.reshape(*shape[1:], shape[0]).transpose(2, 0, 1)
        for out, shape in zip(outs, shapes)
    )


def solution(mesh):
    in_specs = (
        P("branch", "row", "col", None, None),
        P("branch", None, None, None, None, None),
        P("branch", None, None),
        P(),
        P(),
    )
    out_specs = (P(None, ("branch", "row"), "col"),) * 4
    return jax.shard_map(local, mesh=mesh, in_specs=in_specs, out_specs=out_specs, check_vma=False)
```
